128 devices in a mesh: dp: 32 (over x_hi, z, y), head: 4 (over x_lo, core).
Axes of the slice: x: 4 (x_hi: 2, x_lo: 2; x = x_hi * 2 + x_lo), y: 4, z: 4, core: 2. Of those that a mesh axis runs over, the one named last changes fastest.
Arguments:
- q_latent: bfloat16 [4096, 1536], P('dp'), may hold values from -1000 to 1000
- kv_latent: bfloat16 [4096, 576], P('dp'), may hold values from -6 to 6
- kv_gain: float32 [512], replicated, may hold values from 0.1 to 1.9
- w_q_b: bfloat16 [1536, 12288], P(None, 'head'), may hold values from -0.15625 to 0.15625
- w_kv_b: bfloat16 [512, 16384], P(None, 'head'), may hold values from -0.25 to 0.25
- w_o: bfloat16 [8192, 7168], P('head', 'dp'), may hold values from -0.5 to 0.5
- prompt_len: int32 [1], replicated, may hold values from 1 to 1023
- response_mask: int32 [4096], replicated, may hold values 0 or 1
Outputs:
- mixed: bfloat16 [4096, 7168], P('dp', 'head')
The draws below stay inside these ranges and needn't reach their ends.
All inputs are finite; a program needn't handle non-finite values.
Results may differ from the reference program's by a relative error of at most 0.013.
The reference program's roundings to bfloat16 on the way (of `keys`, `queries`, `query_rope`, `absorbed`, `weights`, `context` and `attended`) count: a program that leaves them out, or rounds other values in their place, can miss the bound.
Values may be sent and summed in bfloat16 or wider, within the bound.
A program may use at most 192 MiB of HBM per device.

```python
import math
import jax
import jax.numpy as jnp
from jax import lax

D = 7168
HEADS = 64
QR = 1536
KVR = 512
ROPE = 64
NOPE = 128
VD = 128
TOKENS = 4096


def draw_q_latent(key, part):
    values = jax.random.truncated_normal(jax.random.fold_in(key, 11), -3.0, 3.0, (TOKENS, QR), jnp.float32) * 2.0
    return values.astype(jnp.bfloat16)


def plant(array, own_key, low, largest):
    longest = array.shape.index(max(array.shape))
    spots = []
    for shift in (0, 1):
        where = [jax.random.randint(jax.random.fold_in(own_key, axis), (), 0, length) for axis, length in enumerate(array.shape)]
        where[longest] = (where[longest] + shift) % array.shape[longest]
        spots.append(tuple(where))
    return array.at[spots[0]].set(low).at[spots[1]].set(largest)


def raised(drawn, own_key, source, target, blocks, factor):
    def block_of(position):
        return (jnp.arange(drawn.shape[position]) // (drawn.shape[position] // blocks)).reshape((-1,) + (1,) * (drawn.ndim - 1 - position))

    one_side = jax.random.permutation(own_key, blocks)[block_of(target)]
    far = (block_of(target) + blocks // 2) % blocks
    return jnp.where((block_of(source) == one_side) | (block_of(source) == far), factor * drawn, drawn)


def shard_levels(key, shape, cuts, low, high):
    def one(axis_at, blocks):
        draws = jax.random.uniform(jax.random.fold_in(jax.random.fold_in(key, 6), axis_at), (blocks,), jnp.float32, low / len(cuts), high / len(cuts))
        return jnp.repeat(jnp.exp(draws), shape[axis_at] // blocks).reshape((-1,) + (1,) * (len(shape) - axis_at - 1))

    loudness = one(*cuts[0])
    for cut in cuts[1:]:
        loudness = loudness * one(*cut)
    return loudness


def bell_draw(key, shape, spread, reach, split=(), kind=jnp.bfloat16):
    level = shard_levels(key, shape, split, -0.22, 0.18) if split else 1.0
    values = jax.random.normal(key, shape, jnp.float32) * spread * level
    return jnp.minimum(jnp.maximum(values, -reach), reach).astype(kind)


def noise_with(stream_key, shape, width, limit, split, heavy, kind=jnp.bfloat16):
    array = width * jax.random.normal(stream_key, shape, jnp.float32)
    if split:
        array = array * shard_levels(stream_key, shape, split, -0.22, 0.18)
    return jnp.clip(raised(array, jax.random.fold_in(stream_key, 3), *heavy), -limit, limit).astype(kind)


def setup_inputs(seed: int = 0) -> dict:
    seeds = jax.random.split(jax.random.key(seed), 9)
    return {
        "q_latent": draw_q_latent(jax.random.fold_in(seeds[8], 71), 0),
        "kv_latent": bell_draw(seeds[1], (TOKENS, KVR + ROPE), 1.0, 6.0, ((0, 32),)),
        "kv_gain": jnp.clip(1.0 + 0.18 * jax.random.normal(seeds[2], (KVR,), jnp.float32), 0.1, 1.9),
        "w_q_b": bell_draw(seeds[3], (QR, HEADS * (NOPE + ROPE)), QR ** -0.5, 0.15625, ((1, 4),)),
        "w_kv_b": bell_draw(seeds[4], (KVR, HEADS * (NOPE + VD)), KVR ** -0.5, 0.25, ((1, 4),)),
        "w_o": noise_with(seeds[5], (HEADS * VD, D), (VD * 4) ** -0.5, 0.5, ((0, 4), (1, 32)), (0, 1, 32, 2.75)),
        "prompt_len": jax.random.randint(seeds[6], (1,), 1, TOKENS // 4).astype(jnp.int32),
        "response_mask": plant((jax.random.randint(seeds[7], (TOKENS,), 0, 2) < 1).astype(jnp.int32), jax.random.fold_in(seeds[7], 1), 0, 1),
    }


epsilon = 1e-06

def tables(positions):
    half_width = ROPE // 2
    frequency = 10000.0 ** (-jnp.arange(half_width, dtype=jnp.float32) * 2.0 / ROPE)
    angles = positions.astype(jnp.float32)[:, None] * frequency[None, :]
    return (jnp.cos(angles), jnp.sin(angles))

def rotate(values, cosine, sine_table):
    half_width = values.shape[-1] // 2
    leading = values[..., :half_width]
    trailing = values[..., half_width:]
    return jnp.concatenate([leading * cosine - trailing * sine_table, trailing * cosine + leading * sine_table], axis=-1)

def reference(q_latent, kv_latent, kv_gain, w_q_b, w_kv_b, w_o, prompt_len, response_mask):
    positions = jnp.arange(TOKENS, dtype=jnp.int32)
    cosine, sine_table = tables(positions)
    latent = kv_latent[:, :KVR].astype(jnp.float32)
    normed = latent * lax.rsqrt(lax.optimization_barrier(jnp.mean(latent * latent, axis=-1, keepdims=True)) + epsilon) * kv_gain
    key_rope = rotate(kv_latent[:, KVR:].astype(jnp.float32), cosine, sine_table)
    keys = jnp.concatenate([normed, key_rope], axis=1).astype(jnp.bfloat16)
    queries = jnp.dot(q_latent, w_q_b, preferred_element_type=jnp.float32).astype(jnp.bfloat16)
    queries = queries.reshape(TOKENS, HEADS, NOPE + ROPE)
    query_rope = rotate(queries[:, :, NOPE:].astype(jnp.float32), cosine[:, None, :], sine_table[:, None, :]).astype(jnp.bfloat16)
    w_heads = w_kv_b.reshape(KVR, HEADS, NOPE + VD)
    absorbed = jnp.einsum('thn,khn->thk', queries[:, :, :NOPE].astype(jnp.float32), w_heads[:, :, :NOPE].astype(jnp.float32)).astype(jnp.bfloat16)
    full_query = jnp.concatenate([absorbed, query_rope], axis=-1)
    usable = (positions < prompt_len[0]) | (response_mask == 1)
    allowed = (positions[None, :] <= positions[:, None]) & usable[None, :]
    keys_wide = keys.astype(jnp.float32)
    latent_values = keys_wide[:, :KVR]
    scale = 1.0 / math.sqrt(NOPE + ROPE)
    group_size = math.gcd(HEADS, 4)
    groups = HEADS // group_size
    grouped = full_query.reshape(TOKENS, groups, group_size, KVR + ROPE).transpose(1, 0, 2, 3)
    value_blocks = w_heads[:, :, NOPE:].reshape(KVR, groups, group_size, VD).transpose(1, 0, 2, 3)

    def one_group(operands):
        chosen, w_group = operands
        scores = jnp.einsum('tgc,sc->tgs', chosen.astype(jnp.float32), keys_wide) * scale
        scores = jnp.where(allowed[:, None, :], scores, -1e+30)
        row_max = lax.optimization_barrier(jnp.max(scores, axis=-1, keepdims=True))
        lifted = jnp.exp(scores - row_max)
        weights = (lifted / lax.optimization_barrier(jnp.sum(lifted, axis=-1, keepdims=True))).astype(jnp.bfloat16)
        context = jnp.einsum('tgs,sc->tgc', weights.astype(jnp.float32), latent_values).astype(jnp.bfloat16)
        return jnp.einsum('tgc,cgv->tgv', context.astype(jnp.float32), w_group.astype(jnp.float32)).astype(jnp.bfloat16)
    outputs = lax.map(one_group, (grouped, value_blocks))
    attended = outputs.transpose(1, 0, 2, 3).reshape(TOKENS, HEADS * VD)
    return jnp.dot(attended, w_o, preferred_element_type=jnp.float32).astype(jnp.bfloat16)
```

```python
import functools
import math

import jax
import jax.numpy as jnp
from jax import lax
from jax.experimental import pallas as pl
from jax.experimental.pallas import tpu as pltpu
from jax.sharding import Mesh
from jax.sharding import PartitionSpec as P

KVR = 512
ROPE = 64
NOPE = 128
VD = 128
WIDE = KVR + ROPE
AXES = ("xh", "z", "y", "xl", "c")
DP = ("xh", "z", "y")
HEAD = ("xl", "c")
MESH = pl.DeviceIdType.MESH

HEADS = 16
CHUNKS = 4
PER = HEADS // CHUNKS
HALF = 64
BLOCK = 512
LOG2E = 1.4426950408889634
EPS = 1e-06

CROSS = 0
SWAP = 1
D1 = 2
D1H = 6
D2 = 10
D2H = 26
PAIR = 42
WFULL = 74
WHALF = 78
WPAIR = 80
ABASE = 84
APAIR, AX, AZ, AZH = 0, 1, 2, 6
ASTRIDE = 10
OUT = ABASE + ASTRIDE * CHUNKS
NSEM = OUT + 4


def turn(values, cosine, sine):
    swapped = jnp.concatenate([values[:, ROPE // 2 :], values[:, : ROPE // 2]], axis=1)
    return values * cosine + swapped * sine


def body(
    q_lat,
    kv_lat,
    gain,
    cos_tab,
    sin_tab,
    bias,
    wq_hbm,
    wkv_hbm,
    wo_hbm,
    out_ref,
    out_sem,
    in_sem,
    local_sem,
    qx,
    wq,
    wkv,
    keys,
    qs,
    ctx,
    astage,
    ag,
    wg,
    part,
    outgoing,
    landed,
    m_ref,
    l_ref,
    acc_ref,
):
    xh, z, y, xl, c = (lax.axis_index(a) for a in AXES)
    d1 = y + c * (z - y)
    d2 = z + c * (y - z)

    def place(t, o1, o2):
        a = lax.rem(d1 + o1 + 4, 4)
        b = lax.rem(d2 + o2 + 4, 4)
        zz = b + c * (a - b)
        yy = a + c * (b - a)
        xx = xh + t - 2 * xh * t
        return xx, zz, yy

    def unit(t, o1, o2):
        xx, zz, yy = place(t, o1, o2)
        return xx * 16 + zz * 4 + yy

    def near(o1, o2):
        _, zz, yy = place(0, o1, o2)
        return (xh, zz, yy, xl, c)

    def copy(src, dst, number, device, leaving=None):
        return pltpu.make_async_remote_copy(
            src_ref=src,
            dst_ref=dst,
            send_sem=out_sem.at[number if leaving is None else leaving],
            recv_sem=in_sem.at[number],
            device_id=device,
            device_id_type=MESH,
        )

    me = unit(0, 0, 0)
    partner = (xh, z, y, xl, 1 - c)
    cross = (1 - xh, z, y, 1 - xl, c)
    swap_peer = (1 - xh, 3 - z, y, 1 - xl, c)
    across = (1 - xh, z, y, xl, c)
    up_y = (xh, z, lax.rem(y + 1, 4), xl, c)
    down_y = (xh, z, lax.rem(y + 3, 4), xl, c)
    up_z = (xh, lax.rem(z + 1, 4), y, xl, c)
    down_z = (xh, lax.rem(z + 3, 4), y, xl, c)
    owners = [(c, k, y, xh, z // 2) for k in range(4)]
    makers = [(xl, 2 * c + k // 2, y, k % 2, xh) for k in range(4)]
    same = lambda u, v: 1 - jnp.minimum((u - v) * (u - v), 1)
    mine = same(c, xh) * same(xl, xh) * same(z // 2, c)

    for j in range(8):
        pltpu.make_async_copy(wq_hbm.at[:, pl.ds(j * 384, 384)], wq.at[j], local_sem.at[j]).start()
    pltpu.make_async_copy(wkv_hbm, wkv, local_sem.at[8]).start()
    pltpu.make_async_copy(wo_hbm, wg.at[y, c], local_sem.at[9]).start()

    barrier = pltpu.get_barrier_semaphore()
    for peer in (partner, cross, swap_peer, across, up_y, down_y, up_z, down_z):
        pl.semaphore_signal(barrier, inc=1, device_id=peer, device_id_type=MESH)
    for k in range(4):

        @pl.when((mine == 0) | (z != k))
        def _(k=k):
            pl.semaphore_signal(barrier, inc=1, device_id=owners[k], device_id_type=MESH)

    for k in range(4):
        maker = makers[k]

        @pl.when((mine == 0) | (maker[1] != z) | (maker[3] != xl))
        def _(maker=maker):
            pl.semaphore_signal(barrier, inc=1, device_id=maker, device_id_type=MESH)

    rows = kv_lat[pl.ds(pl.multiple_of(c * HALF, HALF), HALF), :].astype(jnp.float32)
    latent = rows[:, :KVR]
    inverse = lax.rsqrt(jnp.mean(latent * latent, axis=-1, keepdims=True) + EPS)
    keys[me, c, :, :KVR] = (latent * inverse * gain[...]).astype(jnp.bfloat16)
    keys[me, c, :, KVR:] = turn(
        rows[:, KVR:], cos_tab[: HALF, :], sin_tab[: HALF, :]
    ).astype(jnp.bfloat16)
    qx[xh] = q_lat[xh]

    pl.semaphore_wait(barrier, 16 - 2 * mine)

    def key(t, o1, o2, which=None):
        ref = keys.at[unit(t, o1, o2), c]
        if which is None:
            return ref
        return ref.at[pl.ds(32 * which, 32)]

    def key_copy(number, t, o1, o2, device, which=None):
        ref = key(t, o1, o2, which)
        return copy(ref, ref, number, device)

    offsets = (0, 1, 3, 2)

    def spread(k):
        t, o = k % 2, offsets[k // 2]
        key_copy(D2 + 2 * k, t, o, 0, near(0, 1)).start()
        key_copy(D2 + 2 * k + 1, t, o, 0, near(0, -1)).start()
        key_copy(PAIR + k, t, o, 0, partner).start()

    key_copy(CROSS, 0, 0, 0, cross).start()
    swap = copy(q_lat.at[1 - xh], qx.at[xh], SWAP, swap_peer)
    swap_in = copy(q_lat.at[1 - xh], qx.at[1 - xh], SWAP, swap_peer)
    key_copy(D1, 0, 0, 0, near(1, 0)).start()
    key_copy(D1 + 1, 0, 0, 0, near(-1, 0)).start()
    swap.start()
    spread(0)
    key_copy(CROSS, 1, 0, 0, cross).wait_recv()
    key_copy(D1 + 2, 1, 0, 0, near(1, 0)).start()
    key_copy(D1 + 3, 1, 0, 0, near(-1, 0)).start()
    spread(1)
    for t in range(2):
        key_copy(D1 + 2 * t, t, -1, 0, near(1, 0)).wait_recv()
        key_copy(D1H + 2 * t, t, -1, 0, near(1, 0), 0).start()
        spread(4 + t)
        key_copy(D1 + 2 * t + 1, t, 1, 0, near(-1, 0)).wait_recv()
        key_copy(D1H + 2 * t + 1, t, 1, 0, near(-1, 0), 1).start()
        spread(2 + t)
    swap_in.wait_recv()
    pltpu.make_async_copy(wkv_hbm, wkv, local_sem.at[8]).wait()

    def project(j):
        pltpu.make_async_copy(
            wq_hbm.at[:, pl.ds(0, 384)], wq.at[j], local_sem.at[j]
        ).wait()
        both = jnp.dot(
            qx[...].reshape(2 * HALF, -1), wq[j], preferred_element_type=jnp.float32
        ).astype(jnp.bfloat16)
        for e in range(2):
            h = 2 * j + e
            plain = both[:, e * 192 : e * 192 + NOPE]
            roped = both[:, e * 192 + NOPE : (e + 1) * 192].astype(jnp.float32)
            w_key = wkv[:, pl.ds(pl.multiple_of(h * 256, 256), NOPE)]
            absorbed = lax.dot_general(
                plain, w_key, (((1,), (1,)), ((), ())), preferred_element_type=jnp.float32
            ).astype(jnp.bfloat16)
            turned = turn(roped, cos_tab[HALF:, :], sin_tab[HALF:, :]).astype(jnp.bfloat16)
            for half in range(2):
                qs[half, h, :, :KVR] = absorbed[half * HALF : (half + 1) * HALF]
                qs[half, h, :, KVR:] = turned[half * HALF : (half + 1) * HALF]

    def relay(k):
        t = lax.rem(k, 2)
        q = k // 2
        o = q + q // 2 - 2 * (q // 3)
        key_copy(D2 + 2 * k, t, o, -1, near(0, 1)).wait_recv()
        key_copy(D2H + 2 * k, t, o, -1, near(0, 1), 0).start()
        key_copy(PAIR + 8 + k, t, o, -1, partner).start()
        key_copy(D2 + 2 * k + 1, t, o, 1, near(0, -1)).wait_recv()
        key_copy(D2H + 2 * k + 1, t, o, 1, near(0, -1), 1).start()
        key_copy(PAIR + 16 + k, t, o, 1, partner).start()

    project(0)
    for t in range(2):
        key_copy(D1H + 2 * t, t, 2, 0, near(1, 0), 0).wait_recv()
        key_copy(D1H + 2 * t + 1, t, 2, 0, near(-1, 0), 1).wait_recv()
        spread(6 + t)

    w_mine = wg.at[y, c]
    pltpu.make_async_copy(wo_hbm, w_mine, local_sem.at[9]).wait()
    span = wo_hbm.shape[0] // 2

    def w_copy(number, row, device, which):
        ref = wg.at[row, c, pl.ds(which * span, span)]
        return copy(ref, ref, number, device)

    def project_step(k, carry):
        relay(k - 1)
        project(k)
        return carry

    lax.fori_loop(1, 8, project_step, 0)
    relay(7)
    for which in range(2):
        w_copy(WFULL + which, y, up_y, which).start()
        w_copy(WFULL + 3 - which, y, down_y, 1 - which).start()

    def w_pair(row, number):
        return copy(wg.at[row, c], wg.at[row, c], WPAIR + number, partner)

    def w_pair_in(row, number):
        return copy(wg.at[row, 1 - c], wg.at[row, 1 - c], WPAIR + number, partner)

    w_pair(y, 0).start()

    def last_in(k, carry):
        t = lax.rem(k, 2)
        q = k // 2
        o = q + q // 2 - 2 * (q // 3)
        key_copy(D2H + 2 * k, t, o, 2, near(0, 1), 0).wait_recv()
        key_copy(D2H + 2 * k + 1, t, o, 2, near(0, -1), 1).wait_recv()
        key_copy(PAIR + 24 + k, t, o, 2, partner).start()
        return carry

    lax.fori_loop(0, 8, last_in, 0)

    def pair_in(n, carry):
        ref = keys.at[0, 1 - c]
        copy(ref, ref, PAIR + n, partner).wait_recv()
        return carry

    lax.fori_loop(0, 32, pair_in, 0)

    z_low = z + xh * (3 - 2 * z)
    shard = (z_low * 4 + y, 16 + (3 - z_low) * 4 + y)
    scale = LOG2E / math.sqrt(NOPE + ROPE)
    tile_rows = PER * HALF
    reach = BLOCK // 128

    def attend(half, g):
        where = shard[half]
        blocks = where // reach
        m_ref[...] = jnp.full_like(m_ref, -1e30)
        l_ref[...] = jnp.zeros_like(l_ref)
        acc_ref[...] = jnp.zeros_like(acc_ref)
        query = qs[half, pl.ds(g * PER, PER)].reshape(tile_rows, WIDE)

        def step(b, causal):
            block = keys[pl.ds(b * reach, reach)].reshape(BLOCK, WIDE)
            scores = lax.dot_general(
                query, block, (((1,), (1,)), ((), ())), preferred_element_type=jnp.float32
            )
            scores = scores * scale + bias[pl.ds(b, 1), :]
            if causal is not None:
                scores = (scores.reshape(PER, HALF, BLOCK) + causal[None]).reshape(
                    tile_rows, BLOCK
                )
            before = m_ref[...]
            m_new = jnp.maximum(before, jnp.max(scores, axis=1, keepdims=True))
            alpha = jnp.exp2(before - m_new)
            lifted = jnp.exp2(scores - jnp.concatenate([m_new] * (BLOCK // 128), axis=1))
            total = l_ref[...] * alpha
            for k in range(BLOCK // 128):
                total = total + lifted[:, k * 128 : (k + 1) * 128]
            l_ref[...] = total
            m_ref[...] = m_new
            acc_ref[...] = acc_ref[...] * jnp.concatenate([alpha] * (KVR // 128), axis=1) + jnp.dot(
                lifted.astype(jnp.bfloat16), block[:, :KVR], preferred_element_type=jnp.float32
            )

        def open_step(b, carry):
            step(b, None)
            return carry

        lax.fori_loop(0, blocks, open_step, 0)
        token = where * 128 + xh * HALF + lax.broadcasted_iota(jnp.int32, (HALF, BLOCK), 0)
        position = blocks * BLOCK + lax.broadcasted_iota(jnp.int32, (HALF, BLOCK), 1)
        step(blocks, jnp.where(position <= token, 0.0, -1e30))
        total = jnp.sum(l_ref[...], axis=1, keepdims=True)
        ctx[half] = (acc_ref[...] / total).astype(jnp.bfloat16).reshape(PER, HALF, KVR)

    here = xh * 4 + z

    def values(g):
        for n in range(PER):
            h = g * PER + n
            context = jnp.concatenate([ctx[0, n], ctx[1, n]], axis=0)
            w_value = wkv[:, pl.ds(pl.multiple_of(h * 256 + NOPE, NOPE), VD)]
            attended = jnp.dot(context, w_value, preferred_element_type=jnp.float32).astype(
                jnp.bfloat16
            )
            astage[g, 0, :, n * VD : (n + 1) * VD] = attended[:HALF]
            astage[g, 1, :, n * VD : (n + 1) * VD] = attended[HALF:]
        ag[here, g, c] = astage[g, c]

    def a_copy(g, number, t, o, device, which=None):
        slot = (xh + t - 2 * xh * t) * 4 + lax.rem(z + o + 4, 4)
        ref = ag.at[slot, g]
        if which is not None:
            ref = ref.at[which]
        return copy(ref, ref, ABASE + ASTRIDE * g + number, device)

    def pair_copy(g):
        return copy(
            astage.at[g, 1 - c], ag.at[here, g, c], ABASE + ASTRIDE * g + APAIR, partner
        )

    def pair_copy_in(g):
        ref = ag.at[here, g, 1 - c]
        return copy(ref, ref, ABASE + ASTRIDE * g + APAIR, partner)

    def stage1(g):
        pair_copy_in(g).wait_recv()
        a_copy(g, AX, 0, 0, across).start()
        a_copy(g, AZ, 0, 0, up_z).start()
        a_copy(g, AZ + 1, 0, 0, down_z).start()

    def stage2(g):
        a_copy(g, AX, 1, 0, across).wait_recv()
        a_copy(g, AZ + 2, 1, 0, up_z).start()
        a_copy(g, AZ + 3, 1, 0, down_z).start()
        for t in range(1):
            a_copy(g, AZ + 2 * t, t, -1, up_z).wait_recv()
            a_copy(g, AZH + 2 * t, t, -1, up_z, 0).start()
            a_copy(g, AZ + 2 * t + 1, t, 1, down_z).wait_recv()
            a_copy(g, AZH + 2 * t + 1, t, 1, down_z, 1).start()

    def stage3(g):
        t = 1
        a_copy(g, AZ + 2 * t, t, -1, up_z).wait_recv()
        a_copy(g, AZH + 2 * t, t, -1, up_z, 0).start()
        a_copy(g, AZ + 2 * t + 1, t, 1, down_z).wait_recv()
        a_copy(g, AZH + 2 * t + 1, t, 1, down_z, 1).start()

    def stage4(g):
        for t in range(2):
            a_copy(g, AZH + 2 * t, t, 2, up_z, 0).wait_recv()
            a_copy(g, AZH + 2 * t + 1, t, 2, down_z, 1).wait_recv()

    def w_relay(which):
        if which == 0:
            w_copy(WFULL, lax.rem(y + 3, 4), up_y, 0).wait_recv()
            w_copy(WHALF, lax.rem(y + 3, 4), up_y, 0).start()
        else:
            w_copy(WFULL + 3, lax.rem(y + 1, 4), down_y, 1).wait_recv()
            w_copy(WHALF + 1, lax.rem(y + 1, 4), down_y, 1).start()

    def chunk(g, first):
        attend(0, g)
        if not first:
            stage1(g - 1)
        attend(1, g)
        values(g)
        pair_copy(g).start()

    chunk(0, True)
    chunk(1, False)
    w_relay(0)
    w_relay(1)
    chunk(2, False)
    stage2(0)
    chunk(3, False)
    stage3(0)
    stage2(1)
    stage1(3)
    w_copy(WFULL + 1, lax.rem(y + 3, 4), up_y, 1).wait_recv()
    w_pair(lax.rem(y + 3, 4), 1).start()
    w_copy(WFULL + 2, lax.rem(y + 1, 4), down_y, 0).wait_recv()
    w_pair(lax.rem(y + 1, 4), 2).start()
    stage3(1)
    stage2(2)
    w_copy(WHALF, lax.rem(y + 2, 4), up_y, 0).wait_recv()
    w_copy(WHALF + 1, lax.rem(y + 2, 4), down_y, 1).wait_recv()
    w_pair(lax.rem(y + 2, 4), 3).start()
    for k, o in enumerate((0, 3, 1, 2)):
        w_pair_in(lax.rem(y + o, 4), k).wait_recv()

    depth = PER * VD

    def multiply(g):
        def columns(k, carry):
            total = jnp.zeros((8 * HALF, 224), jnp.float32) if g == 0 else part[k]
            for core in range(2):
                total = total + jnp.dot(
                    ag[:, g, core].reshape(8 * HALF, depth),
                    wg[k, core, g * depth : (g + 1) * depth, :],
                    preferred_element_type=jnp.float32,
                )
            if g < CHUNKS - 1:
                part[k] = total
            else:
                rounded = total.astype(jnp.bfloat16)
                for xs in range(2):
                    for zs in range(4):
                        alike = 1 - (xs + c - 2 * xs * c)
                        to = (3 - zs) + alike * (2 * zs - 3)
                        s = xs * 4 + zs
                        outgoing[to, xs, k] = rounded[s * HALF : (s + 1) * HALF]
            return carry

        lax.fori_loop(0, 4, columns, 0)

    stage4(0)
    multiply(0)
    stage3(2)
    stage2(3)
    stage4(1)
    multiply(1)
    stage3(3)
    stage4(2)
    multiply(2)
    stage4(3)
    multiply(3)

    slot = lax.rem(z, 2) * 2 + xl
    for k in range(4):

        @pl.when((mine == 0) | (z != k))
        def _(k=k):
            copy(outgoing.at[k], landed.at[slot], OUT + slot, owners[k], OUT + k).start()

        @pl.when((mine == 1) & (z == k))
        def _(k=k):
            landed[slot] = outgoing[k]

    for k in range(4):
        maker = makers[k]

        @pl.when((mine == 0) | (maker[1] != z) | (maker[3] != xl))
        def _(k=k):
            copy(outgoing.at[k], landed.at[k], OUT + k, owners[k]).wait_recv()

    for zz in range(2):
        for xs in range(2):
            for k in range(4):
                total = landed[2 * zz, xs, k].astype(jnp.float32) + landed[
                    2 * zz + 1, xs, k
                ].astype(jnp.float32)
                out_ref[zz * 4 + k, xs * HALF : (xs + 1) * HALF, :] = total.astype(jnp.bfloat16)

    full = keys.at[0, 0]
    part_key = keys.at[0, 0, pl.ds(0, 32)]

    def sent(ref, number):
        copy(ref, ref, number, partner).wait_send()

    def drain(ref, first, count):
        def one(n, carry):
            sent(ref, first + n)
            return carry

        lax.fori_loop(0, count, one, 0)

    sent(full, CROSS)
    sent(qx.at[0], SWAP)
    drain(full, D1, 4)
    drain(part_key, D1H, 4)
    drain(full, D2, 16)
    drain(part_key, D2H, 16)
    drain(full, PAIR, 32)
    drain(wg.at[0, 0, pl.ds(0, span)], WFULL, 4)
    drain(wg.at[0, 0, pl.ds(0, span)], WHALF, 2)
    drain(wg.at[0, 0], WPAIR, 4)
    for g in range(CHUNKS):
        at = ABASE + ASTRIDE * g
        sent(astage.at[g, 0], at + APAIR)
        sent(ag.at[0, 0], at + AX)
        drain(ag.at[0, 0], at + AZ, 4)
        drain(ag.at[0, 0, 0], at + AZH, 4)
    for k in range(4):

        @pl.when((mine == 0) | (z != k))
        def _(k=k):
            sent(outgoing.at[0], OUT + k)


def local(q_latent, kv_latent, kv_gain, w_q_b, w_kv_b, w_o, prompt_len, response_mask):
    xh, z, y, _, c = (lax.axis_index(a) for a in AXES)
    z_low = z + xh * (3 - 2 * z)
    row = jnp.arange(HALF, dtype=jnp.int32)
    me = xh * 16 + z * 4 + y
    positions = jnp.concatenate(
        [
            me * 128 + c * HALF + row,
            (z_low * 4 + y) * 128 + xh * HALF + row,
            (16 + (3 - z_low) * 4 + y) * 128 + xh * HALF + row,
        ]
    ).astype(jnp.float32)
    lane = jnp.arange(ROPE, dtype=jnp.int32)
    frequency = 10000.0 ** (-(lane % (ROPE // 2)).astype(jnp.float32) * 2.0 / ROPE)
    angles = positions[:, None] * frequency[None, :]
    cos_tab = jnp.cos(angles)
    sin_tab = jnp.sin(angles) * jnp.where(lane < ROPE // 2, -1.0, 1.0)[None, :]
    everywhere = jnp.arange(response_mask.shape[0], dtype=jnp.int32)
    usable = (everywhere < prompt_len[0]) | (response_mask == 1)
    bias = jnp.where(usable, 0.0, -1e30).astype(jnp.float32).reshape(-1, BLOCK)
    vmem = pl.BlockSpec(memory_space=pltpu.VMEM)
    hbm = pl.BlockSpec(memory_space=pl.ANY)
    bf16 = jnp.bfloat16
    depth = PER * VD
    result = pl.pallas_call(
        body,
        out_shape=jax.ShapeDtypeStruct((8, 128, 224), bf16),
        in_specs=[vmem] * 6 + [hbm] * 3,
        out_specs=vmem,
        scratch_shapes=[
            pltpu.SemaphoreType.DMA((NSEM,)),
            pltpu.SemaphoreType.DMA((NSEM,)),
            pltpu.SemaphoreType.DMA((10,)),
            pltpu.VMEM((2, HALF, 1536), bf16),
            pltpu.VMEM((8, 1536, 384), bf16),
            pltpu.VMEM((512, 4096), bf16),
            pltpu.VMEM((32, 2, HALF, WIDE), bf16),
            pltpu.VMEM((2, HEADS, HALF, WIDE), bf16),
            pltpu.VMEM((2, PER, HALF, KVR), bf16),
            pltpu.VMEM((CHUNKS, 2, HALF, depth), bf16),
            pltpu.VMEM((8, CHUNKS, 2, HALF, depth), bf16),
            pltpu.VMEM((4, 2, 2048, 224), bf16),
            pltpu.VMEM((4, 8 * HALF, 224), jnp.float32),
            pltpu.VMEM((4, 2, 4, HALF, 224), bf16),
            pltpu.VMEM((4, 2, 4, HALF, 224), bf16),
            pltpu.VMEM((PER * HALF, 128), jnp.float32),
            pltpu.VMEM((PER * HALF, 128), jnp.float32),
            pltpu.VMEM((PER * HALF, KVR), jnp.float32),
        ],
        compiler_params=pltpu.CompilerParams(
            collective_id=0, has_side_effects=True, vmem_limit_bytes=67000000
        ),
        cost_estimate=pl.CostEstimate(
            flops=20_000_000_000, bytes_accessed=16_000_000, transcendentals=0
        ),
        name="layer",
    )(
        q_latent.reshape(2, HALF, -1),
        kv_latent,
        kv_gain.reshape(1, -1),
        cos_tab,
        sin_tab,
        bias,
        w_q_b,
        w_kv_b,
        w_o,
    )
    return result.transpose(1, 0, 2).reshape(128, -1)


def solution(mesh):
    finer = Mesh(mesh.devices.reshape(2, 4, 4, 2, 2), AXES)
    placed = (
        P(DP, None),
        P(DP, None),
        P(),
        P(None, HEAD),
        P(None, HEAD),
        P(HEAD, DP),
        P(),
        P(),
    )
    return jax.shard_map(
        local, mesh=finer, in_specs=placed, out_specs=P(DP, HEAD), check_vma=False
    )
```

```python
import functools
import math

import jax
import jax.numpy as jnp
import numpy as np
from jax import lax
from jax.experimental import pallas as pl
from jax.experimental.pallas import tpu as pltpu
from jax.sharding import Mesh
from jax.sharding import PartitionSpec as P

KVR = 512
ROPE = 64
NOPE = 128
VD = 128
WIDE = KVR + ROPE
AXES = ("xh", "z", "y", "xl", "c")
DP = ("xh", "z", "y")
HEAD = ("xl", "c")
MESH = pl.DeviceIdType.MESH

HEADS = 16
CHUNKS = 4
PER = HEADS // CHUNKS
SUB = 2
PART = PER // SUB
HALF = 64
BLOCK = 512
LOG2E = 1.4426950408889634
EPS = 1e-06

CROSS = 0
SWAP = 1
D1 = 2
D1H = 6
D2 = 10
D2H = 26
PAIR = 42
WFULL = 74
WHALF = 78
WPAIR = 80
ABASE = 84
APAIR, AX, AZ, AZH = 0, 1, 2, 6
ASTRIDE = 10
OUT = ABASE + ASTRIDE * CHUNKS
XSUM = OUT + 4
NSEM = XSUM + 4


def turn(values, cosine, sine):
    swapped = jnp.concatenate([values[:, ROPE // 2 :], values[:, : ROPE // 2]], axis=1)
    return values * cosine + swapped * sine


def body(
    q_lat,
    kv_lat,
    gain,
    table,
    live,
    prompt,
    wq_hbm,
    wkv_hbm,
    wo_hbm,
    out_ref,
    out_sem,
    in_sem,
    local_sem,
    qx,
    wq,
    wkv,
    keys,
    qs,
    ctx,
    astage,
    ag,
    wg,
    part,
    outgoing,
    summand,
    landed,
    bias,
    m_ref,
    l_ref,
    acc_ref,
):
    xh, z, y, xl, c = (lax.axis_index(a) for a in AXES)
    d1 = y + c * (z - y)
    d2 = z + c * (y - z)

    def place(t, o1, o2):
        a = lax.rem(d1 + o1 + 4, 4)
        b = lax.rem(d2 + o2 + 4, 4)
        zz = b + c * (a - b)
        yy = a + c * (b - a)
        xx = xh + t - 2 * xh * t
        return xx, zz, yy

    def unit(t, o1, o2):
        xx, zz, yy = place(t, o1, o2)
        return xx * 16 + zz * 4 + yy

    def near(o1, o2):
        _, zz, yy = place(0, o1, o2)
        return (xh, zz, yy, xl, c)

    def copy(src, dst, number, device, leaving=None):
        return pltpu.make_async_remote_copy(
            src_ref=src,
            dst_ref=dst,
            send_sem=out_sem.at[number if leaving is None else leaving],
            recv_sem=in_sem.at[number],
            device_id=device,
            device_id_type=MESH,
        )

    me = unit(0, 0, 0)
    partner = (xh, z, y, xl, 1 - c)
    cross = (1 - xh, z, y, 1 - xl, c)
    swap_peer = (1 - xh, 3 - z, y, 1 - xl, c)
    across = (1 - xh, z, y, xl, c)
    up_y = (xh, z, lax.rem(y + 1, 4), xl, c)
    down_y = (xh, z, lax.rem(y + 3, 4), xl, c)
    up_z = (xh, lax.rem(z + 1, 4), y, xl, c)
    down_z = (xh, lax.rem(z + 3, 4), y, xl, c)
    owners = [(c, k, y, xh, z // 2) for k in range(4)]
    makers = [(xl, 2 * c + k, y, xh, xh) for k in range(2)]
    beside = (xh, z, y, 1 - xl, c)
    same = lambda u, v: 1 - jnp.minimum((u - v) * (u - v), 1)
    sums = same(xl, c)
    mine = same(c, xh) * same(xl, xh) * same(z // 2, c)
    z_low = z + xh * (3 - 2 * z)
    shard = (z_low * 4 + y, 16 + (3 - z_low) * 4 + y)

    with jax.named_scope("start"):
        for j in range(8):
            pltpu.make_async_copy(wq_hbm.at[:, pl.ds(j * 384, 384)], wq.at[j], local_sem.at[j]).start()
        pltpu.make_async_copy(wkv_hbm, wkv, local_sem.at[8]).start()
        pltpu.make_async_copy(wo_hbm, wg.at[c, y], local_sem.at[9]).start()

    barrier = pltpu.get_barrier_semaphore()
    for peer in (partner, cross, swap_peer, across, beside, up_y, down_y, up_z, down_z):
        pl.semaphore_signal(barrier, inc=1, device_id=peer, device_id_type=MESH)
    for k in range(2):

        @pl.when((mine == 0) | (2 * c + k != z))
        def _(k=k):
            pl.semaphore_signal(barrier, inc=1, device_id=makers[k], device_id_type=MESH)

    with jax.named_scope("norm"):
        lane = lax.broadcasted_iota(jnp.int32, (1, ROPE), 1)
        sign = jnp.where(lane < ROPE // 2, -1.0, 1.0)

        def angles(m):
            cos_a, sin_a = table[2, pl.ds(m, 1), :], table[3, pl.ds(m, 1), :]
            cos_b, sin_b = table[0], table[1]
            return cos_a * cos_b - sin_a * sin_b, (sin_a * cos_b + cos_a * sin_b) * sign

        turned_rows = kv_lat[...].astype(jnp.float32).T
        rows = jnp.where(c == 0, turned_rows[:HALF], turned_rows[HALF:])
        latent = rows[:, :KVR]
        inverse = lax.rsqrt(jnp.mean(latent * latent, axis=-1, keepdims=True) + EPS)
        keys[me, c, :, :KVR] = (latent * inverse * gain[...]).astype(jnp.bfloat16)
        keys[me, c, :, KVR:] = turn(rows[:, KVR:], *angles(me * 2 + c)).astype(jnp.bfloat16)
        qx[xh] = q_lat[xh]
        spot = lax.broadcasted_iota(jnp.int32, (32, 128), 0) * 128 + lax.broadcasted_iota(
            jnp.int32, (32, 128), 1
        )
        usable = (spot < prompt[0]) | (live[...] == 1)
        masked = jnp.where(usable, 0.0, -1e30)
        for r in range(32):
            b, at = r // (BLOCK // 128), r % (BLOCK // 128)
            bias[b : b + 1, at * 128 : (at + 1) * 128] = masked[r : r + 1]

    with jax.named_scope("barrier"):
        pl.semaphore_wait(barrier, 9 + sums * (4 - mine))

    def key(t, o1, o2, which=None):
        ref = keys.at[unit(t, o1, o2), c]
        if which is None:
            return ref
        return ref.at[pl.ds(32 * which, 32)]

    def key_copy(number, t, o1, o2, device, which=None):
        ref = key(t, o1, o2, which)
        return copy(ref, ref, number, device)

    offsets = (0, 1, 3, 2)

    def spread(k):
        t, o = k % 2, offsets[k // 2]
        key_copy(D2 + 2 * k, t, o, 0, near(0, 1)).start()
        key_copy(D2 + 2 * k + 1, t, o, 0, near(0, -1)).start()
        key_copy(PAIR + k, t, o, 0, partner).start()

    with jax.named_scope("spread"):
        key_copy(CROSS, 0, 0, 0, cross).start()
        swap = copy(q_lat.at[1 - xh], qx.at[xh], SWAP, swap_peer)
        swap_in = copy(q_lat.at[1 - xh], qx.at[1 - xh], SWAP, swap_peer)
        key_copy(D1, 0, 0, 0, near(1, 0)).start()
        key_copy(D1 + 1, 0, 0, 0, near(-1, 0)).start()
        swap.start()
        spread(0)
        with jax.named_scope('cross'):
            key_copy(CROSS, 1, 0, 0, cross).wait_recv()
        key_copy(D1 + 2, 1, 0, 0, near(1, 0)).start()
        key_copy(D1 + 3, 1, 0, 0, near(-1, 0)).start()
        spread(1)
        for t in range(2):
            key_copy(D1 + 2 * t, t, -1, 0, near(1, 0)).wait_recv()
            key_copy(D1H + 2 * t, t, -1, 0, near(1, 0), 0).start()
            spread(4 + t)
            key_copy(D1 + 2 * t + 1, t, 1, 0, near(-1, 0)).wait_recv()
            key_copy(D1H + 2 * t + 1, t, 1, 0, near(-1, 0), 1).start()
            spread(2 + t)
        with jax.named_scope('swap'):
            swap_in.wait_recv()
        with jax.named_scope('wkv'):
            pltpu.make_async_copy(wkv_hbm, wkv, local_sem.at[8]).wait()

    tables = [angles(2 * where + xh) for where in shard]

    def project(j):
        pltpu.make_async_copy(
            wq_hbm.at[:, pl.ds(0, 384)], wq.at[j], local_sem.at[j]
        ).wait()
        both = jnp.dot(
            qx[...].reshape(2 * HALF, -1), wq[j], preferred_element_type=jnp.float32
        ).astype(jnp.bfloat16)
        for e in range(2):
            h = 2 * j + e
            plain = both[:, e * 192 : e * 192 + NOPE]
            roped = both[:, e * 192 + NOPE : (e + 1) * 192].astype(jnp.float32)
            w_key = wkv[:, pl.ds(pl.multiple_of(h * 256, 256), NOPE)]
            absorbed = lax.dot_general(
                plain, w_key, (((1,), (1,)), ((), ())), preferred_element_type=jnp.float32
            ).astype(jnp.bfloat16)
            for half in range(2):
                mine_rows = slice(half * HALF, (half + 1) * HALF)
                qs[half, h, :, :KVR] = absorbed[mine_rows]
                qs[half, h, :, KVR:] = turn(roped[mine_rows], *tables[half]).astype(jnp.bfloat16)

    def relay(k):
        t = lax.rem(k, 2)
        q = k // 2
        o = q + q // 2 - 2 * (q // 3)
        key_copy(D2 + 2 * k, t, o, -1, near(0, 1)).wait_recv()
        key_copy(D2H + 2 * k, t, o, -1, near(0, 1), 0).start()
        key_copy(PAIR + 8 + k, t, o, -1, partner).start()
        key_copy(D2 + 2 * k + 1, t, o, 1, near(0, -1)).wait_recv()
        key_copy(D2H + 2 * k + 1, t, o, 1, near(0, -1), 1).start()
        key_copy(PAIR + 16 + k, t, o, 1, partner).start()

    with jax.named_scope("project"):
        project(0)
    with jax.named_scope("ring1"):
        for t in range(2):
            key_copy(D1H + 2 * t, t, 2, 0, near(1, 0), 0).wait_recv()
            key_copy(D1H + 2 * t + 1, t, 2, 0, near(-1, 0), 1).wait_recv()
            spread(6 + t)

    w_mine = wg.at[c, y]
    pltpu.make_async_copy(wo_hbm, w_mine, local_sem.at[9]).wait()
    span = wo_hbm.shape[0] // 2

    def w_copy(number, row, device, which):
        ref = wg.at[c, row, pl.ds(which * span, span)]
        return copy(ref, ref, number, device)

    def project_step(k, carry):
        with jax.named_scope("relay"):
            relay(k - 1)
        with jax.named_scope("project"):
            project(k)
        return carry

    lax.fori_loop(1, 8, project_step, 0)
    relay(7)
    for which in range(2):
        w_copy(WFULL + which, y, up_y, which).start()
        w_copy(WFULL + 3 - which, y, down_y, 1 - which).start()

    def w_pair(row, number):
        return copy(wg.at[c, row], wg.at[c, row], WPAIR + number, partner)

    def w_pair_in(row, number):
        return copy(wg.at[1 - c, row], wg.at[1 - c, row], WPAIR + number, partner)

    w_pair(y, 0).start()

    def last_in(k, carry):
        t = lax.rem(k, 2)
        q = k // 2
        o = q + q // 2 - 2 * (q // 3)
        key_copy(D2H + 2 * k, t, o, 2, near(0, 1), 0).wait_recv()
        key_copy(D2H + 2 * k + 1, t, o, 2, near(0, -1), 1).wait_recv()
        key_copy(PAIR + 24 + k, t, o, 2, partner).start()
        return carry

    with jax.named_scope("last_in"):
        lax.fori_loop(0, 8, last_in, 0)

    def pair_in(n, carry):
        ref = keys.at[0, 1 - c]
        copy(ref, ref, PAIR + n, partner).wait_recv()
        return carry

    with jax.named_scope("pair_in"):
        lax.fori_loop(0, 32, pair_in, 0)

    scale = LOG2E / math.sqrt(NOPE + ROPE)
    tile_rows = PART * HALF
    reach = BLOCK // 128

    def attend(half, g):
        where = shard[half]
        blocks = where // reach
        m_ref[...] = jnp.full_like(m_ref, -1e30)
        l_ref[...] = jnp.zeros_like(l_ref)
        acc_ref[...] = jnp.zeros_like(acc_ref)

        def step(b, causal):
            block = keys[pl.ds(b * reach, reach)].reshape(BLOCK, WIDE)
            hidden = bias[pl.ds(b, 1), :]
            for n in range(SUB):
                query = qs[half, pl.ds(g * PER + n * PART, PART)].reshape(tile_rows, WIDE)
                scores = lax.dot_general(
                    query, block, (((1,), (1,)), ((), ())), preferred_element_type=jnp.float32
                )
                scores = scores * scale + hidden
                if causal is not None:
                    scores = (scores.reshape(PART, HALF, BLOCK) + causal[None]).reshape(
                        tile_rows, BLOCK
                    )
                before = m_ref[n]
                m_new = jnp.maximum(before, jnp.max(scores, axis=1, keepdims=True))
                alpha = jnp.exp2(before - m_new)
                lifted = jnp.exp2(scores - jnp.concatenate([m_new] * (BLOCK // 128), axis=1))
                total = l_ref[n] * alpha
                for k in range(BLOCK // 128):
                    total = total + lifted[:, k * 128 : (k + 1) * 128]
                l_ref[n] = total
                m_ref[n] = m_new
                acc_ref[n] = acc_ref[n] * jnp.concatenate([alpha] * (KVR // 128), axis=1) + jnp.dot(
                    lifted.astype(jnp.bfloat16), block[:, :KVR], preferred_element_type=jnp.float32
                )

        def open_step(b, carry):
            step(b, None)
            return carry

        lax.fori_loop(0, blocks, open_step, 0)
        token = where * 128 + xh * HALF + lax.broadcasted_iota(jnp.int32, (HALF, BLOCK), 0)
        position = blocks * BLOCK + lax.broadcasted_iota(jnp.int32, (HALF, BLOCK), 1)
        step(blocks, jnp.where(position <= token, 0.0, -1e30))
        for n in range(SUB):
            total = jnp.sum(l_ref[n], axis=1, keepdims=True)
            ctx[half, n * PART : (n + 1) * PART] = (
                (acc_ref[n] / total).astype(jnp.bfloat16).reshape(PART, HALF, KVR)
            )

    here = xh * 4 + z

    def values(g):
        for n in range(PER):
            h = g * PER + n
            context = jnp.concatenate([ctx[0, n], ctx[1, n]], axis=0)
            w_value = wkv[:, pl.ds(pl.multiple_of(h * 256 + NOPE, NOPE), VD)]
            attended = jnp.dot(context, w_value, preferred_element_type=jnp.float32).astype(
                jnp.bfloat16
            )
            astage[g, 0, :, n * VD : (n + 1) * VD] = attended[:HALF]
            astage[g, 1, :, n * VD : (n + 1) * VD] = attended[HALF:]
        ag[here, g, c] = astage[g, c]

    def a_copy(g, number, t, o, device, which=None):
        slot = (xh + t - 2 * xh * t) * 4 + lax.rem(z + o + 4, 4)
        ref = ag.at[slot, g]
        if which is not None:
            ref = ref.at[which]
        return copy(ref, ref, ABASE + ASTRIDE * g + number, device)

    def pair_copy(g):
        return copy(
            astage.at[g, 1 - c], ag.at[here, g, c], ABASE + ASTRIDE * g + APAIR, partner
        )

    def pair_copy_in(g):
        ref = ag.at[here, g, 1 - c]
        return copy(ref, ref, ABASE + ASTRIDE * g + APAIR, partner)

    def stage1(g):
        pair_copy_in(g).wait_recv()
        a_copy(g, AX, 0, 0, across).start()
        a_copy(g, AZ, 0, 0, up_z).start()
        a_copy(g, AZ + 1, 0, 0, down_z).start()

    def stage2(g):
        a_copy(g, AX, 1, 0, across).wait_recv()
        a_copy(g, AZ + 2, 1, 0, up_z).start()
        a_copy(g, AZ + 3, 1, 0, down_z).start()
        for t in range(1):
            a_copy(g, AZ + 2 * t, t, -1, up_z).wait_recv()
            a_copy(g, AZH + 2 * t, t, -1, up_z, 0).start()
            a_copy(g, AZ + 2 * t + 1, t, 1, down_z).wait_recv()
            a_copy(g, AZH + 2 * t + 1, t, 1, down_z, 1).start()

    def stage3(g):
        t = 1
        a_copy(g, AZ + 2 * t, t, -1, up_z).wait_recv()
        a_copy(g, AZH + 2 * t, t, -1, up_z, 0).start()
        a_copy(g, AZ + 2 * t + 1, t, 1, down_z).wait_recv()
        a_copy(g, AZH + 2 * t + 1, t, 1, down_z, 1).start()

    def stage4(g):
        for t in range(2):
            a_copy(g, AZH + 2 * t, t, 2, up_z, 0).wait_recv()
            a_copy(g, AZH + 2 * t + 1, t, 2, down_z, 1).wait_recv()

    def w_relay(which):
        if which == 0:
            w_copy(WFULL, lax.rem(y + 3, 4), up_y, 0).wait_recv()
            w_copy(WHALF, lax.rem(y + 3, 4), up_y, 0).start()
        else:
            w_copy(WFULL + 3, lax.rem(y + 1, 4), down_y, 1).wait_recv()
            w_copy(WHALF + 1, lax.rem(y + 1, 4), down_y, 1).start()

    def chunk(g, first):
        with jax.named_scope("attend_low"):
            attend(0, g)
        if not first:
            with jax.named_scope("stage1"):
                stage1(g - 1)
        with jax.named_scope("attend_high"):
            attend(1, g)
        with jax.named_scope("values"):
            values(g)
        pair_copy(g).start()

    chunk(0, True)
    chunk(1, False)
    with jax.named_scope("w_relay"):
        w_relay(0)
        w_relay(1)
    chunk(2, False)
    with jax.named_scope("stage2_0"):
        stage2(0)
    chunk(3, False)
    with jax.named_scope("stage3_0"):
        stage3(0)
    with jax.named_scope("stage2_1"):
        stage2(1)
    with jax.named_scope("stage1_3"):
        stage1(3)
    with jax.named_scope("w_in"):
        w_copy(WFULL + 1, lax.rem(y + 3, 4), up_y, 1).wait_recv()
        w_pair(lax.rem(y + 3, 4), 1).start()
        w_copy(WFULL + 2, lax.rem(y + 1, 4), down_y, 0).wait_recv()
        w_pair(lax.rem(y + 1, 4), 2).start()
    with jax.named_scope("stage3_1"):
        stage3(1)
    with jax.named_scope("stage2_2"):
        stage2(2)
    with jax.named_scope("w_in2"):
        w_copy(WHALF, lax.rem(y + 2, 4), up_y, 0).wait_recv()
        w_copy(WHALF + 1, lax.rem(y + 2, 4), down_y, 1).wait_recv()
        w_pair(lax.rem(y + 2, 4), 3).start()
        for k, o in enumerate((0, 3, 1, 2)):
            w_pair_in(lax.rem(y + o, 4), k).wait_recv()

    depth = PER * VD

    def multiply(g):
        def product(first):
            total = jnp.zeros((2 * 2 * HALF, 4 * 224), jnp.float32)
            for core in range(2):
                total = total + lax.dot_general(
                    ag[pl.ds(first, 4), g, core].reshape(4 * HALF, depth),
                    wg[core, :, :, g * depth : (g + 1) * depth].reshape(4 * 224, depth),
                    (((1,), (1,)), ((), ())),
                    preferred_element_type=jnp.float32,
                )
            return total

        for xs in range(2):
            total = product(4 * xs)
            if g > 0:
                total = total + part[xs]
            part[xs] = total

    with jax.named_scope("stage4_0"):
        stage4(0)
    with jax.named_scope("multiply"):
        multiply(0)
    with jax.named_scope("stage3_2"):
        stage3(2)
    with jax.named_scope("stage2_3"):
        stage2(3)
    with jax.named_scope("stage4_1"):
        stage4(1)
    with jax.named_scope("multiply"):
        multiply(1)
    with jax.named_scope("stage3_3"):
        stage3(3)
    with jax.named_scope("stage4_2"):
        stage4(2)
    with jax.named_scope("multiply"):
        multiply(2)
    with jax.named_scope("stage4_3"):
        stage4(3)
    with jax.named_scope("multiply"):
        multiply(3)

    def gathered(k):
        first = k + (3 - 2 * k) * c
        second = 3 - first
        low = part[0, pl.ds(pl.multiple_of(first * HALF, HALF), HALF), :]
        high = part[1, pl.ds(pl.multiple_of(second * HALF, HALF), HALF), :]
        return low, high

    with jax.named_scope("half_out"):

        @pl.when(sums == 0)
        def _():
            for k in range(4):
                low, high = gathered(k)
                outgoing[k, :HALF] = low.astype(jnp.bfloat16)
                outgoing[k, HALF:] = high.astype(jnp.bfloat16)
                copy(outgoing.at[k], summand.at[k], XSUM + k, beside).start()

    with jax.named_scope("whole_out"):

        @pl.when(sums == 1)
        def _():
            for k in range(4):
                copy(outgoing.at[k], summand.at[k], XSUM + k, beside).wait_recv()
                low, high = gathered(k)
                outgoing[k, :HALF] = (low + summand[k, :HALF].astype(jnp.float32)).astype(
                    jnp.bfloat16
                )
                outgoing[k, HALF:] = (high + summand[k, HALF:].astype(jnp.float32)).astype(
                    jnp.bfloat16
                )

                @pl.when((mine == 0) | (z != k))
                def _():
                    copy(
                        outgoing.at[k], landed.at[lax.rem(z, 2)], OUT + lax.rem(z, 2), owners[k], OUT + k
                    ).start()

                @pl.when((mine == 1) & (z == k))
                def _():
                    landed[lax.rem(z, 2)] = outgoing[k]

    with jax.named_scope("finish"):
        for k in range(2):

            @pl.when((mine == 0) | (2 * c + k != z))
            def _(k=k):
                copy(outgoing.at[k], landed.at[k], OUT + k, owners[k]).wait_recv()

            out_ref[:, k * 896 : (k + 1) * 896] = landed[k]

    with jax.named_scope("drain"):
        full = keys.at[0, 0]
        part_key = keys.at[0, 0, pl.ds(0, 32)]

        def sent(ref, number):
            copy(ref, ref, number, partner).wait_send()

        def drain(ref, first, count):
            def one(n, carry):
                sent(ref, first + n)
                return carry

            lax.fori_loop(0, count, one, 0)

        sent(full, CROSS)
        sent(qx.at[0], SWAP)
        drain(full, D1, 4)
        drain(part_key, D1H, 4)
        drain(full, D2, 16)
        drain(part_key, D2H, 16)
        drain(full, PAIR, 32)
        drain(wg.at[0, 0, pl.ds(0, span)], WFULL, 4)
        drain(wg.at[0, 0, pl.ds(0, span)], WHALF, 2)
        drain(wg.at[0, 0], WPAIR, 4)
        for g in range(CHUNKS):
            at = ABASE + ASTRIDE * g
            sent(astage.at[g, 0], at + APAIR)
            sent(ag.at[0, 0], at + AX)
            drain(ag.at[0, 0], at + AZ, 4)
            drain(ag.at[0, 0, 0], at + AZH, 4)
        @pl.when(sums == 0)
        def _():
            drain(outgoing.at[0], XSUM, 4)

        for k in range(4):

            @pl.when((sums == 1) & ((mine == 0) | (z != k)))
            def _(k=k):
                sent(outgoing.at[0], OUT + k)


def local(q_latent, kv_latent, kv_gain, w_q_b, w_kv_b, w_o, prompt_len, response_mask):
    frequency = 10000.0 ** (-np.arange(ROPE // 2, dtype=np.float64) * 2.0 / ROPE)
    fine = np.arange(HALF, dtype=np.float64)[:, None] * np.tile(frequency, 2)[None, :]
    table = np.stack([np.cos(fine), np.sin(fine), np.cos(HALF * fine), np.sin(HALF * fine)])
    vmem = pl.BlockSpec(memory_space=pltpu.VMEM)
    hbm = pl.BlockSpec(memory_space=pl.ANY)
    bf16 = jnp.bfloat16
    depth = PER * VD
    result = pl.pallas_call(
        body,
        out_shape=jax.ShapeDtypeStruct((128, 1792), bf16),
        in_specs=[vmem] * 5 + [pl.BlockSpec(memory_space=pltpu.SMEM)] + [hbm] * 3,
        out_specs=vmem,
        scratch_shapes=[
            pltpu.SemaphoreType.DMA((NSEM,)),
            pltpu.SemaphoreType.DMA((NSEM,)),
            pltpu.SemaphoreType.DMA((10,)),
            pltpu.VMEM((2, HALF, 1536), bf16),
            pltpu.VMEM((8, 1536, 384), bf16),
            pltpu.VMEM((512, 4096), bf16),
            pltpu.VMEM((32, 2, HALF, WIDE), bf16),
            pltpu.VMEM((2, HEADS, HALF, WIDE), bf16),
            pltpu.VMEM((2, PER, HALF, KVR), bf16),
            pltpu.VMEM((CHUNKS, 2, HALF, depth), bf16),
            pltpu.VMEM((8, CHUNKS, 2, HALF, depth), bf16),
            pltpu.VMEM((2, 4, 224, 2048), bf16),
            pltpu.VMEM((2, 4 * HALF, 4 * 224), jnp.float32),
            pltpu.VMEM((4, 2 * HALF, 4 * 224), bf16),
            pltpu.VMEM((4, 2 * HALF, 4 * 224), bf16),
            pltpu.VMEM((2, 2 * HALF, 4 * 224), bf16),
            pltpu.VMEM((4096 // BLOCK, BLOCK), jnp.float32),
            pltpu.VMEM((SUB, PART * HALF, 128), jnp.float32),
            pltpu.VMEM((SUB, PART * HALF, 128), jnp.float32),
            pltpu.VMEM((SUB, PART * HALF, KVR), jnp.float32),
        ],
        compiler_params=pltpu.CompilerParams(
            collective_id=0, has_side_effects=True, vmem_limit_bytes=67000000
        ),
        cost_estimate=pl.CostEstimate(
            flops=20_000_000_000, bytes_accessed=16_000_000, transcendentals=0
        ),
        name="layer",
    )(
        q_latent.reshape(2, HALF, -1),
        kv_latent.T,
        kv_gain.reshape(1, -1),
        jnp.asarray(table, jnp.float32),
        response_mask.reshape(32, 128),
        prompt_len,
        w_q_b,
        w_kv_b,
        w_o.T,
    )
    return result


def solution(mesh):
    finer = Mesh(mesh.devices.reshape(2, 4, 4, 2, 2), AXES)
    placed = (
        P(DP, None),
        P(DP, None),
        P(),
        P(None, HEAD),
        P(None, HEAD),
        P(HEAD, DP),
        P(),
        P(),
    )
    return jax.shard_map(
        local, mesh=finer, in_specs=placed, out_specs=P(DP, HEAD), check_vma=False
    )
```

```python
import functools
import math

import jax
import jax.numpy as jnp
import numpy as np
from jax import lax
from jax.experimental import pallas as pl
from jax.experimental.pallas import tpu as pltpu
from jax.sharding import Mesh
from jax.sharding import PartitionSpec as P

KVR = 512
ROPE = 64
NOPE = 128
VD = 128
WIDE = KVR + ROPE
AXES = ("xh", "z", "y", "xl", "c")
DP = ("xh", "z", "y")
HEAD = ("xl", "c")
MESH = pl.DeviceIdType.MESH

HEADS = 16
CHUNKS = 4
PER = 8
HALF = 64
ROWS = 32
BLOCK = 512
LOG2E = 1.4426950408889634
EPS = 1e-06

CROSS = 0
SWAP = 1
D1 = 2
D1H = 6
D2 = 10
D2H = 26
PAIR = 42
WFULL = 74
WHALF = 78
WPAIR = 80
ABASE = 84
APAIR, AX, AZ, AZH, AX2 = 0, 1, 2, 6, 8
ASTRIDE = 10
OUT = ABASE + ASTRIDE * CHUNKS
XSUM = OUT + 4
NSEM = XSUM + 4


def turn(values, cosine, sine):
    swapped = jnp.concatenate([values[:, ROPE // 2 :], values[:, : ROPE // 2]], axis=1)
    return values * cosine + swapped * sine


def body(
    q_lat,
    kv_lat,
    gain,
    table,
    live,
    prompt,
    wq_hbm,
    wkv_hbm,
    wo_hbm,
    out_ref,
    out_sem,
    in_sem,
    local_sem,
    qx,
    wq,
    wkv,
    keys,
    qs,
    ctx,
    astage,
    ag,
    wg,
    part,
    outgoing,
    summand,
    landed,
    bias,
    m_ref,
    l_ref,
    acc_ref,
):
    xh, z, y, xl, c = (lax.axis_index(a) for a in AXES)
    d1 = y + c * (z - y)
    d2 = z + c * (y - z)

    def place(t, o1, o2):
        a = lax.rem(d1 + o1 + 4, 4)
        b = lax.rem(d2 + o2 + 4, 4)
        zz = b + c * (a - b)
        yy = a + c * (b - a)
        xx = xh + t - 2 * xh * t
        return xx, zz, yy

    def unit(t, o1, o2):
        xx, zz, yy = place(t, o1, o2)
        return xx * 16 + zz * 4 + yy

    def near(o1, o2):
        _, zz, yy = place(0, o1, o2)
        return (xh, zz, yy, xl, c)

    def copy(src, dst, number, device, leaving=None):
        return pltpu.make_async_remote_copy(
            src_ref=src,
            dst_ref=dst,
            send_sem=out_sem.at[number if leaving is None else leaving],
            recv_sem=in_sem.at[number],
            device_id=device,
            device_id_type=MESH,
        )

    me = unit(0, 0, 0)
    partner = (xh, z, y, xl, 1 - c)
    cross = (1 - xh, z, y, 1 - xl, c)
    swap_peer = (1 - xh, 3 - z, y, 1 - xl, c)
    across = (1 - xh, z, y, xl, c)
    up_y = (xh, z, lax.rem(y + 1, 4), xl, c)
    down_y = (xh, z, lax.rem(y + 3, 4), xl, c)
    up_z = (xh, lax.rem(z + 1, 4), y, xl, c)
    down_z = (xh, lax.rem(z + 3, 4), y, xl, c)
    owners = [[(t, 2 * xl + k, y, xh, z // 2) for k in range(2)] for t in range(2)]
    makers = [(xl, 2 * c + k % 2, y, z // 2, k // 2) for k in range(4)]
    beside = (xh, z, y, 1 - xl, c)
    same = lambda u, v: 1 - jnp.minimum((u - v) * (u - v), 1)
    mine = same(c, xh) * same(xl, xh) * same(z // 2, c)
    z_low = z + xh * (3 - 2 * z)
    shard = (z_low * 4 + y, 16 + (3 - z_low) * 4 + y)

    with jax.named_scope("start"):
        for j in range(8):
            pltpu.make_async_copy(wq_hbm.at[:, pl.ds(j * 384, 384)], wq.at[j], local_sem.at[j]).start()
        pltpu.make_async_copy(wkv_hbm, wkv, local_sem.at[8]).start()
        pltpu.make_async_copy(wo_hbm, wg.at[c, y], local_sem.at[9]).start()

    barrier = pltpu.get_barrier_semaphore()
    for peer in (partner, cross, swap_peer, across, beside, up_y, down_y, up_z, down_z):
        pl.semaphore_signal(barrier, inc=1, device_id=peer, device_id_type=MESH)
    for k in range(4):

        @pl.when((mine == 0) | (makers[k][1] != z) | (k // 2 != c))
        def _(k=k):
            pl.semaphore_signal(barrier, inc=1, device_id=makers[k], device_id_type=MESH)

    with jax.named_scope("norm"):
        lane = lax.broadcasted_iota(jnp.int32, (1, ROPE), 1)
        sign = jnp.where(lane < ROPE // 2, -1.0, 1.0)

        def angles(m):
            cos_a, sin_a = table[2, pl.ds(m, 1), :], table[3, pl.ds(m, 1), :]
            cos_b, sin_b = table[0], table[1]
            return cos_a * cos_b - sin_a * sin_b, (sin_a * cos_b + cos_a * sin_b) * sign

        turned_rows = kv_lat[...].astype(jnp.float32).T
        rows = jnp.where(c == 0, turned_rows[:HALF], turned_rows[HALF:])
        latent = rows[:, :KVR]
        inverse = lax.rsqrt(jnp.mean(latent * latent, axis=-1, keepdims=True) + EPS)
        keys[me, c, :, :KVR] = (latent * inverse * gain[...]).astype(jnp.bfloat16)
        keys[me, c, :, KVR:] = turn(rows[:, KVR:], *angles(me * 2 + c)).astype(jnp.bfloat16)
        qx[xh] = q_lat[xh]
        spot = lax.broadcasted_iota(jnp.int32, (32, 128), 0) * 128 + lax.broadcasted_iota(
            jnp.int32, (32, 128), 1
        )
        usable = (spot < prompt[0]) | (live[...] == 1)
        masked = jnp.where(usable, 0.0, -1e30)
        for r in range(32):
            b, at = r // (BLOCK // 128), r % (BLOCK // 128)
            bias[b : b + 1, at * 128 : (at + 1) * 128] = masked[r : r + 1]

    with jax.named_scope("barrier"):
        pl.semaphore_wait(barrier, 13 - mine)

    def key(t, o1, o2, which=None):
        ref = keys.at[unit(t, o1, o2), c]
        if which is None:
            return ref
        return ref.at[pl.ds(32 * which, 32)]

    def key_copy(number, t, o1, o2, device, which=None):
        ref = key(t, o1, o2, which)
        return copy(ref, ref, number, device)

    offsets = (0, 1, 3, 2)

    def spread(k):
        t, o = k % 2, offsets[k // 2]
        key_copy(D2 + 2 * k, t, o, 0, near(0, 1)).start()
        key_copy(D2 + 2 * k + 1, t, o, 0, near(0, -1)).start()
        key_copy(PAIR + k, t, o, 0, partner).start()

    with jax.named_scope("spread"):
        key_copy(CROSS, 0, 0, 0, cross).start()
        swap = copy(q_lat.at[1 - xh], qx.at[xh], SWAP, swap_peer)
        swap_in = copy(q_lat.at[1 - xh], qx.at[1 - xh], SWAP, swap_peer)
        key_copy(D1, 0, 0, 0, near(1, 0)).start()
        key_copy(D1 + 1, 0, 0, 0, near(-1, 0)).start()
        swap.start()
        spread(0)
        with jax.named_scope('cross'):
            key_copy(CROSS, 1, 0, 0, cross).wait_recv()
        key_copy(D1 + 2, 1, 0, 0, near(1, 0)).start()
        key_copy(D1 + 3, 1, 0, 0, near(-1, 0)).start()
        spread(1)
        for t in range(2):
            key_copy(D1 + 2 * t, t, -1, 0, near(1, 0)).wait_recv()
            key_copy(D1H + 2 * t, t, -1, 0, near(1, 0), 0).start()
            spread(4 + t)
            key_copy(D1 + 2 * t + 1, t, 1, 0, near(-1, 0)).wait_recv()
            key_copy(D1H + 2 * t + 1, t, 1, 0, near(-1, 0), 1).start()
            spread(2 + t)
        with jax.named_scope('swap'):
            swap_in.wait_recv()
        with jax.named_scope('wkv'):
            pltpu.make_async_copy(wkv_hbm, wkv, local_sem.at[8]).wait()

    tables = [angles(2 * where + xh) for where in shard]

    def project(j):
        pltpu.make_async_copy(
            wq_hbm.at[:, pl.ds(0, 384)], wq.at[j], local_sem.at[j]
        ).wait()
        both = jnp.dot(
            qx[...].reshape(2 * HALF, -1), wq[j], preferred_element_type=jnp.float32
        ).astype(jnp.bfloat16)
        for e in range(2):
            h = 2 * j + e
            plain = both[:, e * 192 : e * 192 + NOPE]
            roped = both[:, e * 192 + NOPE : (e + 1) * 192].astype(jnp.float32)
            w_key = wkv[:, pl.ds(pl.multiple_of(h * 256, 256), NOPE)]
            absorbed = lax.dot_general(
                plain, w_key, (((1,), (1,)), ((), ())), preferred_element_type=jnp.float32
            ).astype(jnp.bfloat16)
            for half in range(2):
                mine_rows = slice(half * HALF, (half + 1) * HALF)
                qs[half, h, :, :KVR] = absorbed[mine_rows]
                qs[half, h, :, KVR:] = turn(roped[mine_rows], *tables[half]).astype(jnp.bfloat16)

    def relay(k):
        t = lax.rem(k, 2)
        q = k // 2
        o = q + q // 2 - 2 * (q // 3)
        key_copy(D2 + 2 * k, t, o, -1, near(0, 1)).wait_recv()
        key_copy(D2H + 2 * k, t, o, -1, near(0, 1), 0).start()
        key_copy(PAIR + 8 + k, t, o, -1, partner).start()
        key_copy(D2 + 2 * k + 1, t, o, 1, near(0, -1)).wait_recv()
        key_copy(D2H + 2 * k + 1, t, o, 1, near(0, -1), 1).start()
        key_copy(PAIR + 16 + k, t, o, 1, partner).start()

    with jax.named_scope("project"):
        project(0)
    with jax.named_scope("ring1"):
        for t in range(2):
            key_copy(D1H + 2 * t, t, 2, 0, near(1, 0), 0).wait_recv()
            key_copy(D1H + 2 * t + 1, t, 2, 0, near(-1, 0), 1).wait_recv()
            spread(6 + t)

    w_mine = wg.at[c, y]
    pltpu.make_async_copy(wo_hbm, w_mine, local_sem.at[9]).wait()
    span = wo_hbm.shape[0] // 2

    def w_copy(number, row, device, which):
        ref = wg.at[c, row, pl.ds(which * span, span)]
        return copy(ref, ref, number, device)

    def project_step(k, carry):
        with jax.named_scope("relay"):
            relay(k - 1)
        with jax.named_scope("project"):
            project(k)
        return carry

    lax.fori_loop(1, 8, project_step, 0)
    relay(7)
    for which in range(2):
        w_copy(WFULL + which, y, up_y, which).start()
        w_copy(WFULL + 3 - which, y, down_y, 1 - which).start()

    def w_pair(row, number):
        return copy(wg.at[c, row], wg.at[c, row], WPAIR + number, partner)

    def w_pair_in(row, number):
        return copy(wg.at[1 - c, row], wg.at[1 - c, row], WPAIR + number, partner)

    w_pair(y, 0).start()

    def last_in(upper):
        t = xh + upper - 2 * xh * upper

        def one(q, carry):
            k = 2 * q + t
            o = q + q // 2 - 2 * (q // 3)
            key_copy(D2H + 2 * k, t, o, 2, near(0, 1), 0).wait_recv()
            key_copy(D2H + 2 * k + 1, t, o, 2, near(0, -1), 1).wait_recv()
            key_copy(PAIR + 24 + k, t, o, 2, partner).start()
            return carry

        lax.fori_loop(0, 4, one, 0)

    def pair_in(upper):
        t = xh + upper - 2 * xh * upper

        def one(n, carry):
            ref = keys.at[0, 1 - c]
            copy(ref, ref, PAIR + 2 * n + t, partner).wait_recv()
            return carry

        lax.fori_loop(0, 16, one, 0)

    with jax.named_scope("last_in"):
        last_in(0)
    with jax.named_scope("pair_in"):
        pair_in(0)

    scale = LOG2E / math.sqrt(NOPE + ROPE)
    tile_rows = HEADS * HALF
    reach = BLOCK // 128

    def attend(half, hooks):
        where = shard[half]
        blocks = where // reach
        m_ref[...] = jnp.full_like(m_ref, -1e30)
        l_ref[...] = jnp.zeros_like(l_ref)
        acc_ref[...] = jnp.zeros_like(acc_ref)

        def step(b, causal):
            block = keys[pl.ds(b * reach, reach)].reshape(BLOCK, WIDE)
            scores = lax.dot_general(
                qs[half].reshape(tile_rows, WIDE),
                block,
                (((1,), (1,)), ((), ())),
                preferred_element_type=jnp.float32,
            )
            scores = scores * scale + bias[pl.ds(b, 1), :]
            if causal is not None:
                scores = (scores.reshape(HEADS, HALF, BLOCK) + causal[None]).reshape(
                    tile_rows, BLOCK
                )
            before = m_ref[...]
            m_new = jnp.maximum(before, jnp.max(scores, axis=1, keepdims=True))
            alpha = jnp.exp2(before - m_new)
            lifted = jnp.exp2(scores - jnp.concatenate([m_new] * (BLOCK // 128), axis=1))
            total = l_ref[...] * alpha
            for k in range(BLOCK // 128):
                total = total + lifted[:, k * 128 : (k + 1) * 128]
            l_ref[...] = total
            m_ref[...] = m_new
            acc_ref[...] = acc_ref[...] * jnp.concatenate([alpha] * (KVR // 128), axis=1) + jnp.dot(
                lifted.astype(jnp.bfloat16), block[:, :KVR], preferred_element_type=jnp.float32
            )

        def open_step(b, carry):
            for at, hook in hooks:

                @pl.when(b == at)
                def _(hook=hook):
                    hook()

            step(b, None)
            return carry

        lax.fori_loop(0, blocks, open_step, 0)
        token = where * 128 + xh * HALF + lax.broadcasted_iota(jnp.int32, (HALF, BLOCK), 0)
        position = blocks * BLOCK + lax.broadcasted_iota(jnp.int32, (HALF, BLOCK), 1)
        step(blocks, jnp.where(position <= token, 0.0, -1e30))
        total = jnp.sum(l_ref[...], axis=1, keepdims=True)
        ctx[...] = (acc_ref[...] / total).astype(jnp.bfloat16).reshape(HEADS, HALF, KVR)

    here = xh * 4 + z

    def values(half):
        for h in range(HEADS):
            w_value = wkv[:, h * 256 + NOPE : (h + 1) * 256]
            attended = jnp.dot(ctx[h], w_value, preferred_element_type=jnp.float32).astype(
                jnp.bfloat16
            )
            g, at = 2 * half + h // PER, (h % PER) * VD
            astage[g, 0, :, at : at + VD] = attended[:ROWS]
            astage[g, 1, :, at : at + VD] = attended[ROWS:]
        for g in (2 * half, 2 * half + 1):
            pair_copy(g).start()
            ag[here, g, c] = astage[g, c]

    def a_copy(g, number, t, o, device, which=None):
        slot = (xh + t - 2 * xh * t) * 4 + lax.rem(z + o + 4, 4)
        ref = ag.at[slot, g]
        if which is not None:
            ref = ref.at[which]
        return copy(ref, ref, ABASE + ASTRIDE * g + number, device)

    def pair_copy(g):
        return copy(
            astage.at[g, 1 - c], ag.at[here, g, c], ABASE + ASTRIDE * g + APAIR, partner
        )

    def pair_copy_in(g):
        ref = ag.at[here, g, 1 - c]
        return copy(ref, ref, ABASE + ASTRIDE * g + APAIR, partner)

    def stage1(g):
        pair_copy_in(g).wait_recv()
        a_copy(g, AX, 0, 0, across).start()
        a_copy(g, AZ, 0, 0, up_z).start()
        a_copy(g, AZ + 1, 0, 0, down_z).start()

    def stage2(g):
        a_copy(g, AZ, 0, -1, up_z).wait_recv()
        a_copy(g, AZH, 0, -1, up_z, 0).start()
        a_copy(g, AZ + 1, 0, 1, down_z).wait_recv()
        a_copy(g, AZH + 1, 0, 1, down_z, 1).start()

    def stage3(g):
        a_copy(g, AX, 1, 0, across).wait_recv()
        a_copy(g, AZ + 2, 1, 0, up_z).start()
        a_copy(g, AZ + 3, 1, 0, down_z).start()

    def stage4(g):
        a_copy(g, AZH, 0, 2, up_z, 0).wait_recv()
        a_copy(g, AZH + 1, 0, 2, down_z, 1).wait_recv()
        a_copy(g, AX2, 0, 2, across).start()

    def stage5(g):
        a_copy(g, AZ + 2, 1, -1, up_z).wait_recv()
        a_copy(g, AZ + 3, 1, 1, down_z).wait_recv()
        a_copy(g, AX2, 1, 2, across).wait_recv()

    def w_relay(which):
        if which == 0:
            w_copy(WFULL, lax.rem(y + 3, 4), up_y, 0).wait_recv()
            w_copy(WHALF, lax.rem(y + 3, 4), up_y, 0).start()
        else:
            w_copy(WFULL + 3, lax.rem(y + 1, 4), down_y, 1).wait_recv()
            w_copy(WHALF + 1, lax.rem(y + 1, 4), down_y, 1).start()

    def w_middle():
        w_copy(WFULL + 1, lax.rem(y + 3, 4), up_y, 1).wait_recv()
        w_pair(lax.rem(y + 3, 4), 1).start()
        w_copy(WFULL + 2, lax.rem(y + 1, 4), down_y, 0).wait_recv()
        w_pair(lax.rem(y + 1, 4), 2).start()

    def w_last():
        w_copy(WHALF, lax.rem(y + 2, 4), up_y, 0).wait_recv()
        w_copy(WHALF + 1, lax.rem(y + 2, 4), down_y, 1).wait_recv()
        w_pair(lax.rem(y + 2, 4), 3).start()
        for k, o in enumerate((0, 3, 1, 2)):
            w_pair_in(lax.rem(y + o, 4), k).wait_recv()

    depth = PER * VD

    def product(g):
        total = jnp.zeros((8 * ROWS, 4 * 224), jnp.float32)
        for core in range(2):
            total = total + lax.dot_general(
                ag[:, g, core].reshape(8 * ROWS, depth),
                wg[core, :, :, (g % 2) * depth : (g % 2 + 1) * depth].reshape(4 * 224, depth),
                (((1,), (1,)), ((), ())),
                preferred_element_type=jnp.float32,
            )
        return total.reshape(8, ROWS, 4 * 224)

    def slots(half, k):
        straight, mirrored = k, 3 - k
        first = straight if half == 0 else mirrored
        return first, 4 + 3 - first

    def half_out(half):
        for k in range(2):
            low, high = slots(half, 2 * (1 - xl) + k)
            outgoing[half, 0, k, 0] = part[low].astype(jnp.bfloat16)
            outgoing[half, 0, k, 1] = part[high].astype(jnp.bfloat16)
            copy(
                outgoing.at[half, 0, k], summand.at[half, k], XSUM + 2 * half + k, beside
            ).start()

    def whole_out(half):
        place_in = lax.rem(z, 2) + 2 * c
        for k in range(2):
            row = 2 * xl + k
            copy(
                outgoing.at[half, 0, k], summand.at[half, k], XSUM + 2 * half + k, beside
            ).wait_recv()
            low, high = slots(half, row)
            for xs, at in enumerate((low, high)):
                outgoing[half, 1, k, xs] = (
                    part[at] + summand[half, k, xs].astype(jnp.float32)
                ).astype(jnp.bfloat16)
            own = (mine == 1) & (xh == half) & (z == row)

            @pl.when(jnp.logical_not(own))
            def _():
                copy(
                    outgoing.at[half, 1, k],
                    landed.at[place_in],
                    OUT + place_in,
                    owners[half][k],
                    OUT + 2 * half + k,
                ).start()

            @pl.when(own)
            def _():
                landed[place_in] = outgoing[half, 1, k]

    def sum_early():
        part[...] = product(0) + product(1)

    with jax.named_scope("attend_low"):
        attend(0, ())
    with jax.named_scope("values"):
        values(0)
    with jax.named_scope("last_in"):
        last_in(1)
    with jax.named_scope("pair_in"):
        pair_in(1)

    def hook_a():
        with jax.named_scope("hook1"):
            stage1(0)
            stage1(1)

    def hook_b():
        with jax.named_scope("hook2"):
            stage2(0)
            w_relay(0)
            w_relay(1)

    def hook_c():
        with jax.named_scope("hook3"):
            stage2(1)
            stage3(0)

    with jax.named_scope("attend_high"):
        attend(1, ((0, hook_a), (2, hook_b), (3, hook_c)))
    with jax.named_scope("values"):
        values(1)
    with jax.named_scope("stage3_1"):
        stage3(1)
    with jax.named_scope("stage1_2"):
        stage1(2)
        stage1(3)
    with jax.named_scope("stage4_0"):
        stage4(0)
        stage4(1)
    with jax.named_scope("stage2_2"):
        stage2(2)
    with jax.named_scope("w_middle"):
        w_middle()
    with jax.named_scope("stage5_0"):
        stage5(0)
        stage5(1)
    with jax.named_scope("stage3_2"):
        stage2(3)
        stage3(2)
        stage3(3)
    with jax.named_scope("w_last"):
        w_last()
    with jax.named_scope("product_low"):
        sum_early()
    with jax.named_scope("half_out_low"):
        half_out(0)
    with jax.named_scope("stage4_2"):
        stage4(2)
        stage4(3)
    with jax.named_scope("whole_out_low"):
        whole_out(0)
    with jax.named_scope("stage5_2"):
        stage5(2)
    with jax.named_scope("product_high"):
        part[...] = product(2)
    with jax.named_scope("stage5_3"):
        stage5(3)
    with jax.named_scope("product_high"):
        part[...] = part[...] + product(3)
    with jax.named_scope("half_out_high"):
        half_out(1)
    with jax.named_scope("whole_out_high"):
        whole_out(1)

    with jax.named_scope("finish"):
        for k in range(4):

            @pl.when((mine == 0) | (makers[k][1] != z) | (k // 2 != c))
            def _(k=k):
                copy(landed.at[k], landed.at[k], OUT + k, partner).wait_recv()

            for xs in range(2):
                at = xs * HALF + (k // 2) * ROWS
                out_ref[at : at + ROWS, (k % 2) * 896 : (k % 2 + 1) * 896] = landed[k, xs]

    with jax.named_scope("drain"):
        full = keys.at[0, 0]
        part_key = keys.at[0, 0, pl.ds(0, 32)]

        def sent(ref, number):
            copy(ref, ref, number, partner).wait_send()

        def drain(ref, first, count):
            def one(n, carry):
                sent(ref, first + n)
                return carry

            lax.fori_loop(0, count, one, 0)

        sent(full, CROSS)
        sent(qx.at[0], SWAP)
        drain(full, D1, 4)
        drain(part_key, D1H, 4)
        drain(full, D2, 16)
        drain(part_key, D2H, 16)
        drain(full, PAIR, 32)
        drain(wg.at[0, 0, pl.ds(0, span)], WFULL, 4)
        drain(wg.at[0, 0, pl.ds(0, span)], WHALF, 2)
        drain(wg.at[0, 0], WPAIR, 4)
        for g in range(CHUNKS):
            at = ABASE + ASTRIDE * g
            sent(astage.at[g, 0], at + APAIR)
            sent(ag.at[0, 0], at + AX)
            drain(ag.at[0, 0], at + AZ, 4)
            drain(ag.at[0, 0, 0], at + AZH, 2)
            sent(ag.at[0, 0], at + AX2)
        drain(summand.at[0, 0], XSUM, 4)
        for half in range(2):
            for k in range(2):
                own = (mine == 1) & (xh == half) & (z == 2 * xl + k)

                @pl.when(jnp.logical_not(own))
                def _(half=half, k=k):
                    sent(landed.at[0], OUT + 2 * half + k)


def local(q_latent, kv_latent, kv_gain, w_q_b, w_kv_b, w_o, prompt_len, response_mask):
    frequency = 10000.0 ** (-np.arange(ROPE // 2, dtype=np.float64) * 2.0 / ROPE)
    fine = np.arange(HALF, dtype=np.float64)[:, None] * np.tile(frequency, 2)[None, :]
    table = np.stack([np.cos(fine), np.sin(fine), np.cos(HALF * fine), np.sin(HALF * fine)])
    vmem = pl.BlockSpec(memory_space=pltpu.VMEM)
    hbm = pl.BlockSpec(memory_space=pl.ANY)
    bf16 = jnp.bfloat16
    depth = PER * VD
    result = pl.pallas_call(
        body,
        out_shape=jax.ShapeDtypeStruct((128, 1792), bf16),
        in_specs=[vmem] * 5 + [pl.BlockSpec(memory_space=pltpu.SMEM)] + [hbm] * 3,
        out_specs=vmem,
        scratch_shapes=[
            pltpu.SemaphoreType.DMA((NSEM,)),
            pltpu.SemaphoreType.DMA((NSEM,)),
            pltpu.SemaphoreType.DMA((10,)),
            pltpu.VMEM((2, HALF, 1536), bf16),
            pltpu.VMEM((8, 1536, 384), bf16),
            pltpu.VMEM((512, 4096), bf16),
            pltpu.VMEM((32, 2, HALF, WIDE), bf16),
            pltpu.VMEM((2, HEADS, HALF, WIDE), bf16),
            pltpu.VMEM((HEADS, HALF, KVR), bf16),
            pltpu.VMEM((CHUNKS, 2, ROWS, depth), bf16),
            pltpu.VMEM((8, CHUNKS, 2, ROWS, depth), bf16),
            pltpu.VMEM((2, 4, 224, 2048), bf16),
            pltpu.VMEM((8, ROWS, 4 * 224), jnp.float32),
            pltpu.VMEM((2, 2, 2, 2, ROWS, 4 * 224), bf16),
            pltpu.VMEM((2, 2, 2, ROWS, 4 * 224), bf16),
            pltpu.VMEM((4, 2, ROWS, 4 * 224), bf16),
            pltpu.VMEM((4096 // BLOCK, BLOCK), jnp.float32),
            pltpu.VMEM((HEADS * HALF, 128), jnp.float32),
            pltpu.VMEM((HEADS * HALF, 128), jnp.float32),
            pltpu.VMEM((HEADS * HALF, KVR), jnp.float32),
        ],
        compiler_params=pltpu.CompilerParams(
            collective_id=0, has_side_effects=True, vmem_limit_bytes=67000000
        ),
        cost_estimate=pl.CostEstimate(
            flops=20_000_000_000, bytes_accessed=16_000_000, transcendentals=0
        ),
        name="layer",
    )(
        q_latent.reshape(2, HALF, -1),
        kv_latent.T,
        kv_gain.reshape(1, -1),
        jnp.asarray(table, jnp.float32),
        response_mask.reshape(32, 128),
        prompt_len,
        w_q_b,
        w_kv_b,
        w_o.T,
    )
    return result


def solution(mesh):
    finer = Mesh(mesh.devices.reshape(2, 4, 4, 2, 2), AXES)
    placed = (
        P(DP, None),
        P(DP, None),
        P(),
        P(None, HEAD),
        P(None, HEAD),
        P(HEAD, DP),
        P(),
        P(),
    )
    return jax.shard_map(
        local, mesh=finer, in_specs=placed, out_specs=P(DP, HEAD), check_vma=False
    )
```

```python
import functools
import math

import jax
import jax.numpy as jnp
import numpy as np
from jax import lax
from jax.experimental import pallas as pl
from jax.experimental.pallas import tpu as pltpu
from jax.sharding import Mesh
from jax.sharding import PartitionSpec as P

KVR = 512
ROPE = 64
NOPE = 128
VD = 128
WIDE = KVR + ROPE
AXES = ("xh", "z", "y", "xl", "c")
DP = ("xh", "z", "y")
HEAD = ("xl", "c")
MESH = pl.DeviceIdType.MESH

HEADS = 16
CHUNKS = 4
HALF = 64
ROWS = 16
BLOCK = 512
LOG2E = 1.4426950408889634
EPS = 1e-06

CROSS = 0
SWAP = 1
D1 = 2
D1H = 6
D2 = 10
D2H = 26
PAIR = 42
WFULL = 74
WHALF = 78
WPAIR = 80
ABASE = 84
APAIR, AX, AZ, AZH, AX2 = 0, 1, 2, 6, 8
ASTRIDE = 10
OUT = ABASE + ASTRIDE * CHUNKS
XSUM = OUT + 8
NSEM = XSUM + 8


def turn(values, cosine, sine):
    swapped = jnp.concatenate([values[:, ROPE // 2 :], values[:, : ROPE // 2]], axis=1)
    return values * cosine + swapped * sine


def body(
    q_lat,
    kv_lat,
    gain,
    table,
    live,
    prompt,
    wq_hbm,
    wkv_hbm,
    wo_hbm,
    out_ref,
    out_sem,
    in_sem,
    local_sem,
    qx,
    wq,
    wkv,
    keys,
    qs,
    ctx,
    astage,
    ag,
    wg,
    part,
    outgoing,
    summand,
    landed,
    bias,
    m_ref,
    l_ref,
    acc_ref,
):
    xh, z, y, xl, c = (lax.axis_index(a) for a in AXES)
    d1 = y + c * (z - y)
    d2 = z + c * (y - z)

    def place(t, o1, o2):
        a = lax.rem(d1 + o1 + 4, 4)
        b = lax.rem(d2 + o2 + 4, 4)
        zz = b + c * (a - b)
        yy = a + c * (b - a)
        xx = xh + t - 2 * xh * t
        return xx, zz, yy

    def unit(t, o1, o2):
        xx, zz, yy = place(t, o1, o2)
        return xx * 16 + zz * 4 + yy

    def near(o1, o2):
        _, zz, yy = place(0, o1, o2)
        return (xh, zz, yy, xl, c)

    def copy(src, dst, number, device, leaving=None):
        return pltpu.make_async_remote_copy(
            src_ref=src,
            dst_ref=dst,
            send_sem=out_sem.at[number if leaving is None else leaving],
            recv_sem=in_sem.at[number],
            device_id=device,
            device_id_type=MESH,
        )

    me = unit(0, 0, 0)
    partner = (xh, z, y, xl, 1 - c)
    cross = (1 - xh, z, y, 1 - xl, c)
    swap_peer = (1 - xh, 3 - z, y, 1 - xl, c)
    across = (1 - xh, z, y, xl, c)
    up_y = (xh, z, lax.rem(y + 1, 4), xl, c)
    down_y = (xh, z, lax.rem(y + 3, 4), xl, c)
    up_z = (xh, lax.rem(z + 1, 4), y, xl, c)
    down_z = (xh, lax.rem(z + 3, 4), y, xl, c)
    owners = [[(t, 2 * xl + k, y, xh, z // 2) for k in range(2)] for t in range(2)]
    makers = [(xl, 2 * c + k % 2, y, z // 2, k // 2) for k in range(4)]
    beside = (xh, z, y, 1 - xl, c)
    same = lambda u, v: 1 - jnp.minimum((u - v) * (u - v), 1)
    mine = same(c, xh) * same(xl, xh) * same(z // 2, c)
    z_low = z + xh * (3 - 2 * z)
    shard = (z_low * 4 + y, 16 + (3 - z_low) * 4 + y)

    with jax.named_scope("start"):
        pltpu.make_async_copy(wkv_hbm, wkv, local_sem.at[8]).start()
        for j in range(8):
            pltpu.make_async_copy(
                wq_hbm.at[:, pl.ds(j * 384, 384)], wq.at[j], local_sem.at[j]
            ).start()
        pltpu.make_async_copy(wo_hbm, wg.at[c, y], local_sem.at[9]).start()

    barrier = pltpu.get_barrier_semaphore()
    far = near(2, 0)
    for peer in (partner, cross, swap_peer, across, beside, far, up_y, down_y, up_z, down_z):
        pl.semaphore_signal(barrier, inc=1, device_id=peer, device_id_type=MESH)
    for k in range(4):

        @pl.when((mine == 0) | (makers[k][1] != z) | (k // 2 != c))
        def _(k=k):
            pl.semaphore_signal(barrier, inc=1, device_id=makers[k], device_id_type=MESH)

    with jax.named_scope("norm"):
        lane = lax.broadcasted_iota(jnp.int32, (1, ROPE), 1)
        sign = jnp.where(lane < ROPE // 2, -1.0, 1.0)

        def angles(m):
            cos_a, sin_a = table[2, pl.ds(m, 1), :], table[3, pl.ds(m, 1), :]
            cos_b, sin_b = table[0], table[1]
            return cos_a * cos_b - sin_a * sin_b, (sin_a * cos_b + cos_a * sin_b) * sign

        turned_rows = kv_lat[...].astype(jnp.float32).T
        rows = jnp.where(c == 0, turned_rows[:HALF], turned_rows[HALF:])
        latent = rows[:, :KVR]
        inverse = lax.rsqrt(jnp.mean(latent * latent, axis=-1, keepdims=True) + EPS)
        keys[me, c, :, :KVR] = (latent * inverse * gain[...]).astype(jnp.bfloat16)
        keys[me, c, :, KVR:] = turn(rows[:, KVR:], *angles(me * 2 + c)).astype(jnp.bfloat16)
        qx[xh] = q_lat[xh]
        spot = lax.broadcasted_iota(jnp.int32, (32, 128), 0) * 128 + lax.broadcasted_iota(
            jnp.int32, (32, 128), 1
        )
        usable = (spot < prompt[0]) | (live[...] == 1)
        masked = jnp.where(usable, 0.0, -1e30)
        for r in range(32):
            b, at = r // (BLOCK // 128), r % (BLOCK // 128)
            bias[b : b + 1, at * 128 : (at + 1) * 128] = masked[r : r + 1]

    with jax.named_scope("barrier"):
        pl.semaphore_wait(barrier, 14 - mine)

    def key(t, o1, o2, which=None):
        ref = keys.at[unit(t, o1, o2), c]
        if which is None:
            return ref
        return ref.at[pl.ds(32 * which, 32)]

    def key_copy(number, t, o1, o2, device, which=None):
        ref = key(t, o1, o2, which)
        return copy(ref, ref, number, device)

    offsets = (0, 1, 3, 2)

    def spread(k):
        t, o = k % 2, offsets[k // 2]
        key_copy(D2 + 2 * k, t, o, 0, near(0, 1)).start()
        key_copy(D2 + 2 * k + 1, t, o, 0, near(0, -1)).start()
        key_copy(PAIR + k, t, o, 0, partner).start()

    def first_in(t):
        key_copy(D1 + 2 * t, t, -1, 0, near(1, 0)).wait_recv()
        spread(4 + t)
        key_copy(D1 + 2 * t + 1, t, 1, 0, near(-1, 0)).wait_recv()
        spread(2 + t)

    def first_out(t):
        key_copy(D1 + 2 * t, t, 0, 0, near(1, 0)).start()
        key_copy(D1 + 2 * t + 1, t, 0, 0, near(-1, 0)).start()
        spread(t)
        key_copy(D1H + t, t, 0, 0, far).start()

    def far_in(t):
        key_copy(D1H + t, t, 2, 0, far).wait_recv()
        spread(6 + t)

    with jax.named_scope("spread"):
        key_copy(CROSS, 0, 0, 0, cross).start()
        first_out(0)
        swap = copy(q_lat.at[1 - xh], qx.at[xh], SWAP, swap_peer)
        swap_in = copy(q_lat.at[1 - xh], qx.at[1 - xh], SWAP, swap_peer)
        swap.start()
        first_in(0)
    with jax.named_scope("cross"):
        key_copy(CROSS, 1, 0, 0, cross).wait_recv()
        first_out(1)

    tables = [angles(2 * where + xh) for where in shard]

    def project(j):
        pltpu.make_async_copy(
            wq_hbm.at[:, pl.ds(0, 384)], wq.at[j], local_sem.at[j]
        ).wait()
        both = jnp.dot(
            qx[...].reshape(2 * HALF, -1), wq[j], preferred_element_type=jnp.float32
        ).astype(jnp.bfloat16)
        for e in range(2):
            h = 2 * j + e
            plain = both[:, e * 192 : e * 192 + NOPE]
            roped = both[:, e * 192 + NOPE : (e + 1) * 192].astype(jnp.float32)
            w_key = wkv[:, pl.ds(pl.multiple_of(h * 256, 256), NOPE)]
            absorbed = lax.dot_general(
                plain, w_key, (((1,), (1,)), ((), ())), preferred_element_type=jnp.float32
            ).astype(jnp.bfloat16)
            for half in range(2):
                mine_rows = slice(half * HALF, (half + 1) * HALF)
                qs[half, h, :, :KVR] = absorbed[mine_rows]
                qs[half, h, :, KVR:] = turn(roped[mine_rows], *tables[half]).astype(jnp.bfloat16)

    def relay(k):
        t = lax.rem(k, 2)
        q = k // 2
        o = q + q // 2 - 2 * (q // 3)
        key_copy(D2 + 2 * k, t, o, -1, near(0, 1)).wait_recv()
        key_copy(D2H + 2 * k, t, o, -1, near(0, 1), 0).start()
        key_copy(PAIR + 8 + k, t, o, -1, partner).start()
        key_copy(D2 + 2 * k + 1, t, o, 1, near(0, -1)).wait_recv()
        key_copy(D2H + 2 * k + 1, t, o, 1, near(0, -1), 1).start()
        key_copy(PAIR + 16 + k, t, o, 1, partner).start()

    span = wo_hbm.shape[0] // 2

    def w_copy(number, row, device, which):
        ref = wg.at[c, row, pl.ds(which * span, span)]
        return copy(ref, ref, number, device)

    with jax.named_scope("relay0"):
        relay(0)
    with jax.named_scope("far0"):
        far_in(0)
    with jax.named_scope("swap"):
        swap_in.wait_recv()
    with jax.named_scope("wkv"):
        pltpu.make_async_copy(wkv_hbm, wkv, local_sem.at[8]).wait()
    with jax.named_scope("project"):
        project(0)
    with jax.named_scope("first1"):
        first_in(1)
    with jax.named_scope("relay42"):
        relay(4)
        relay(2)
    with jax.named_scope("project"):
        project(1)
    with jax.named_scope("far1"):
        far_in(1)
    for at, k in enumerate((1, 5, 3, 6, 7)):
        with jax.named_scope("relays"):
            relay(k)
        with jax.named_scope("project"):
            project(2 + at)
    pltpu.make_async_copy(wo_hbm, wg.at[c, y], local_sem.at[9]).wait()
    for which in range(2):
        w_copy(WFULL + which, y, up_y, which).start()
        w_copy(WFULL + 3 - which, y, down_y, 1 - which).start()

    def w_pair(row, number):
        return copy(wg.at[c, row], wg.at[c, row], WPAIR + number, partner)

    def w_pair_in(row, number):
        return copy(wg.at[1 - c, row], wg.at[1 - c, row], WPAIR + number, partner)

    w_pair(y, 0).start()
    with jax.named_scope("project"):
        project(7)

    def last_in(upper):
        t = xh + upper - 2 * xh * upper

        def one(q, carry):
            k = 2 * q + t
            o = q + q // 2 - 2 * (q // 3)
            key_copy(D2H + 2 * k, t, o, 2, near(0, 1), 0).wait_recv()
            key_copy(D2H + 2 * k + 1, t, o, 2, near(0, -1), 1).wait_recv()
            key_copy(PAIR + 24 + k, t, o, 2, partner).start()
            return carry

        lax.fori_loop(0, 4, one, 0)

    def pair_in(upper):
        t = xh + upper - 2 * xh * upper

        def one(n, carry):
            ref = keys.at[0, 1 - c]
            copy(ref, ref, PAIR + 2 * n + t, partner).wait_recv()
            return carry

        lax.fori_loop(0, 16, one, 0)

    with jax.named_scope("last_in"):
        last_in(0)
    with jax.named_scope("pair_in"):
        pair_in(0)

    scale = LOG2E / math.sqrt(NOPE + ROPE)
    tile_rows = HEADS * HALF
    reach = BLOCK // 128

    def attend(half, hooks):
        where = shard[half]
        blocks = where // reach
        m_ref[...] = jnp.full_like(m_ref, -1e30)
        l_ref[...] = jnp.zeros_like(l_ref)
        acc_ref[...] = jnp.zeros_like(acc_ref)

        def step(b, causal):
            block = keys[pl.ds(b * reach, reach)].reshape(BLOCK, WIDE)
            scores = lax.dot_general(
                qs[half].reshape(tile_rows, WIDE),
                block,
                (((1,), (1,)), ((), ())),
                preferred_element_type=jnp.float32,
            )
            scores = scores * scale + bias[pl.ds(b, 1), :]
            if causal is not None:
                scores = (scores.reshape(HEADS, HALF, BLOCK) + causal[None]).reshape(
                    tile_rows, BLOCK
                )
            before = m_ref[...]
            m_new = jnp.maximum(before, jnp.max(scores, axis=1, keepdims=True))
            alpha = jnp.exp2(before - m_new)
            lifted = jnp.exp2(scores - jnp.concatenate([m_new] * (BLOCK // 128), axis=1))
            total = l_ref[...] * alpha
            for k in range(BLOCK // 128):
                total = total + lifted[:, k * 128 : (k + 1) * 128]
            l_ref[...] = total
            m_ref[...] = m_new
            acc_ref[...] = acc_ref[...] * jnp.concatenate([alpha] * (KVR // 128), axis=1) + jnp.dot(
                lifted.astype(jnp.bfloat16), block[:, :KVR], preferred_element_type=jnp.float32
            )

        def open_step(b, carry):
            hooks(b, blocks)
            step(b, None)
            return carry

        lax.fori_loop(0, blocks, open_step, 0)
        token = where * 128 + xh * HALF + lax.broadcasted_iota(jnp.int32, (HALF, BLOCK), 0)
        position = blocks * BLOCK + lax.broadcasted_iota(jnp.int32, (HALF, BLOCK), 1)
        step(blocks, jnp.where(position <= token, 0.0, -1e30))
        total = jnp.sum(l_ref[...], axis=1, keepdims=True)
        ctx[...] = (acc_ref[...] / total).astype(jnp.bfloat16).reshape(HEADS, HALF, KVR)

    here = xh * 4 + z

    def values(half):
        for h in range(HEADS):
            w_value = wkv[:, h * 256 + NOPE : (h + 1) * 256]
            attended = jnp.dot(ctx[h], w_value, preferred_element_type=jnp.float32).astype(
                jnp.bfloat16
            )
            for r in range(2):
                for to in range(2):
                    at = to * 2 * ROWS + r * ROWS
                    astage[2 * half + r, to, :, h * VD : (h + 1) * VD] = attended[at : at + ROWS]
        for g in (2 * half, 2 * half + 1):
            pair_copy(g).start()
            ag[here, g, c] = astage[g, c]

    def a_copy(g, number, t, o, device, which=None):
        slot = (xh + t - 2 * xh * t) * 4 + lax.rem(z + o + 4, 4)
        ref = ag.at[slot, g]
        if which is not None:
            ref = ref.at[which]
        return copy(ref, ref, ABASE + ASTRIDE * g + number, device)

    def pair_copy(g):
        return copy(
            astage.at[g, 1 - c], ag.at[here, g, c], ABASE + ASTRIDE * g + APAIR, partner
        )

    def pair_copy_in(g):
        ref = ag.at[here, g, 1 - c]
        return copy(ref, ref, ABASE + ASTRIDE * g + APAIR, partner)

    def stage1(g):
        pair_copy_in(g).wait_recv()
        a_copy(g, AX, 0, 0, across).start()
        a_copy(g, AZ, 0, 0, up_z).start()
        a_copy(g, AZ + 1, 0, 0, down_z).start()

    def stage2(g):
        a_copy(g, AZ, 0, -1, up_z).wait_recv()
        a_copy(g, AZH, 0, -1, up_z, 0).start()
        a_copy(g, AZ + 1, 0, 1, down_z).wait_recv()
        a_copy(g, AZH + 1, 0, 1, down_z, 1).start()

    def stage3(g):
        a_copy(g, AX, 1, 0, across).wait_recv()
        a_copy(g, AZ + 2, 1, 0, up_z).start()
        a_copy(g, AZ + 3, 1, 0, down_z).start()

    def stage4(g):
        a_copy(g, AZH, 0, 2, up_z, 0).wait_recv()
        a_copy(g, AZH + 1, 0, 2, down_z, 1).wait_recv()
        a_copy(g, AX2, 0, 2, across).start()

    def stage5(g):
        a_copy(g, AZ + 2, 1, -1, up_z).wait_recv()
        a_copy(g, AZ + 3, 1, 1, down_z).wait_recv()
        a_copy(g, AX2, 1, 2, across).wait_recv()

    def w_relay(which):
        if which == 0:
            w_copy(WFULL, lax.rem(y + 3, 4), up_y, 0).wait_recv()
            w_copy(WHALF, lax.rem(y + 3, 4), up_y, 0).start()
        else:
            w_copy(WFULL + 3, lax.rem(y + 1, 4), down_y, 1).wait_recv()
            w_copy(WHALF + 1, lax.rem(y + 1, 4), down_y, 1).start()

    def w_middle():
        w_copy(WFULL + 1, lax.rem(y + 3, 4), up_y, 1).wait_recv()
        w_pair(lax.rem(y + 3, 4), 1).start()
        w_copy(WFULL + 2, lax.rem(y + 1, 4), down_y, 0).wait_recv()
        w_pair(lax.rem(y + 1, 4), 2).start()

    def w_last():
        w_copy(WHALF, lax.rem(y + 2, 4), up_y, 0).wait_recv()
        w_copy(WHALF + 1, lax.rem(y + 2, 4), down_y, 1).wait_recv()
        w_pair(lax.rem(y + 2, 4), 3).start()
        for k, o in enumerate((0, 3, 1, 2)):
            w_pair_in(lax.rem(y + o, 4), k).wait_recv()

    def product(first, count):
        rows = 8 * count * ROWS
        total = jnp.zeros((rows, 4 * 224), jnp.float32)
        for core in range(2):
            total = total + lax.dot_general(
                ag[:, first : first + count, core].reshape(rows, HEADS * VD),
                wg[core].reshape(4 * 224, HEADS * VD),
                (((1,), (1,)), ((), ())),
                preferred_element_type=jnp.float32,
            )
        total = total.reshape(8, count * ROWS, 4 * 224)
        for n in range(count):
            part[first + n] = total[:, n * ROWS : (n + 1) * ROWS]

    def slots(half, k):
        straight, mirrored = k, 3 - k
        first = straight if half == 0 else mirrored
        return first, 4 + 3 - first

    def half_out(g):
        for k in range(2):
            low, high = slots(g // 2, 2 * (1 - xl) + k)
            outgoing[g, 0, k, 0] = part[g, low].astype(jnp.bfloat16)
            outgoing[g, 0, k, 1] = part[g, high].astype(jnp.bfloat16)
            copy(outgoing.at[g, 0, k], summand.at[g, k], XSUM + 2 * g + k, beside).start()

    def whole_out(g):
        half = g // 2
        place_in = lax.rem(z, 2) + 2 * c + 4 * (g % 2)
        for k in range(2):
            row = 2 * xl + k
            copy(outgoing.at[g, 0, k], summand.at[g, k], XSUM + 2 * g + k, beside).wait_recv()
            low, high = slots(half, row)
            for xs, at in enumerate((low, high)):
                outgoing[g, 1, k, xs] = (
                    part[g, at] + summand[g, k, xs].astype(jnp.float32)
                ).astype(jnp.bfloat16)
            own = (mine == 1) & (xh == half) & (z == row)

            @pl.when(jnp.logical_not(own))
            def _():
                copy(
                    outgoing.at[g, 1, k],
                    landed.at[place_in],
                    OUT + place_in,
                    owners[half][k],
                    OUT + 2 * g + k,
                ).start()

            @pl.when(own)
            def _():
                landed[place_in] = outgoing[g, 1, k]

    with jax.named_scope("attend_low"):
        attend(0, lambda b, blocks: None)
    with jax.named_scope("values"):
        values(0)
    with jax.named_scope("last_in"):
        last_in(1)
    with jax.named_scope("pair_in"):
        pair_in(1)

    def late_hooks(b, blocks):
        @pl.when(b == 0)
        def _():
            with jax.named_scope("hook1"):
                stage1(0)
                stage1(1)

        @pl.when(b == blocks - 1)
        def _():
            with jax.named_scope("hook2"):
                stage2(0)
                stage3(0)
                w_relay(0)
                w_relay(1)

    with jax.named_scope("attend_high"):
        attend(1, late_hooks)
    with jax.named_scope("values"):
        values(1)
    with jax.named_scope("stage23_1"):
        stage2(1)
        stage3(1)
    with jax.named_scope("stage1_23"):
        stage1(2)
        stage1(3)
    with jax.named_scope("stage4_01"):
        stage4(0)
        stage4(1)
    with jax.named_scope("w_middle"):
        w_middle()
    with jax.named_scope("stage5_01"):
        stage5(0)
        stage5(1)
    with jax.named_scope("stage2_2"):
        stage2(2)
    with jax.named_scope("w_last"):
        w_last()
    with jax.named_scope("product_low"):
        product(0, 2)
    with jax.named_scope("half_out_low"):
        half_out(0)
        half_out(1)
    with jax.named_scope("stage3_2"):
        stage3(2)
    with jax.named_scope("stage23_3"):
        stage2(3)
        stage3(3)
    with jax.named_scope("whole_out_low"):
        whole_out(0)
        whole_out(1)
    with jax.named_scope("stage4_23"):
        stage4(2)
        stage4(3)
    with jax.named_scope("stage5_2"):
        stage5(2)
    with jax.named_scope("product_2"):
        product(2, 1)
    with jax.named_scope("half_out_2"):
        half_out(2)
    with jax.named_scope("stage5_3"):
        stage5(3)
    with jax.named_scope("product_3"):
        product(3, 1)
    with jax.named_scope("half_out_3"):
        half_out(3)
    with jax.named_scope("whole_out_2"):
        whole_out(2)
    with jax.named_scope("whole_out_3"):
        whole_out(3)

    with jax.named_scope("finish"):
        for n in range(8):
            r, k = n // 4, n % 4

            @pl.when((mine == 0) | (makers[k][1] != z) | (k // 2 != c))
            def _(n=n):
                copy(landed.at[n], landed.at[n], OUT + n, partner).wait_recv()

            for xs in range(2):
                at = xs * HALF + (k // 2) * 2 * ROWS + r * ROWS
                out_ref[at : at + ROWS, (k % 2) * 896 : (k % 2 + 1) * 896] = landed[n, xs]

    with jax.named_scope("drain"):
        full = keys.at[0, 0]
        part_key = keys.at[0, 0, pl.ds(0, 32)]

        def sent(ref, number):
            copy(ref, ref, number, partner).wait_send()

        def drain(ref, first, count):
            def one(n, carry):
                sent(ref, first + n)
                return carry

            lax.fori_loop(0, count, one, 0)

        sent(full, CROSS)
        sent(qx.at[0], SWAP)
        drain(full, D1, 4)
        drain(full, D1H, 2)
        drain(full, D2, 16)
        drain(part_key, D2H, 16)
        drain(full, PAIR, 32)
        drain(wg.at[0, 0, pl.ds(0, span)], WFULL, 4)
        drain(wg.at[0, 0, pl.ds(0, span)], WHALF, 2)
        drain(wg.at[0, 0], WPAIR, 4)
        for g in range(CHUNKS):
            at = ABASE + ASTRIDE * g
            sent(astage.at[g, 0], at + APAIR)
            sent(ag.at[0, 0], at + AX)
            drain(ag.at[0, 0], at + AZ, 4)
            drain(ag.at[0, 0, 0], at + AZH, 2)
            sent(ag.at[0, 0], at + AX2)
        drain(summand.at[0, 0], XSUM, 8)
        for g in range(CHUNKS):
            for k in range(2):
                own = (mine == 1) & (xh == g // 2) & (z == 2 * xl + k)

                @pl.when(jnp.logical_not(own))
                def _(g=g, k=k):
                    sent(landed.at[0], OUT + 2 * g + k)


def local(q_latent, kv_latent, kv_gain, w_q_b, w_kv_b, w_o, prompt_len, response_mask):
    frequency = 10000.0 ** (-np.arange(ROPE // 2, dtype=np.float64) * 2.0 / ROPE)
    fine = np.arange(HALF, dtype=np.float64)[:, None] * np.tile(frequency, 2)[None, :]
    table = np.stack([np.cos(fine), np.sin(fine), np.cos(HALF * fine), np.sin(HALF * fine)])
    vmem = pl.BlockSpec(memory_space=pltpu.VMEM)
    hbm = pl.BlockSpec(memory_space=pl.ANY)
    bf16 = jnp.bfloat16
    depth = HEADS * VD
    result = pl.pallas_call(
        body,
        out_shape=jax.ShapeDtypeStruct((128, 1792), bf16),
        in_specs=[vmem] * 5 + [pl.BlockSpec(memory_space=pltpu.SMEM)] + [hbm] * 3,
        out_specs=vmem,
        scratch_shapes=[
            pltpu.SemaphoreType.DMA((NSEM,)),
            pltpu.SemaphoreType.DMA((NSEM,)),
            pltpu.SemaphoreType.DMA((10,)),
            pltpu.VMEM((2, HALF, 1536), bf16),
            pltpu.VMEM((8, 1536, 384), bf16),
            pltpu.VMEM((512, 4096), bf16),
            pltpu.VMEM((32, 2, HALF, WIDE), bf16),
            pltpu.VMEM((2, HEADS, HALF, WIDE), bf16),
            pltpu.VMEM((HEADS, HALF, KVR), bf16),
            pltpu.VMEM((CHUNKS, 2, ROWS, depth), bf16),
            pltpu.VMEM((8, CHUNKS, 2, ROWS, depth), bf16),
            pltpu.VMEM((2, 4, 224, 2048), bf16),
            pltpu.VMEM((CHUNKS, 8, ROWS, 4 * 224), jnp.float32),
            pltpu.VMEM((CHUNKS, 2, 2, 2, ROWS, 4 * 224), bf16),
            pltpu.VMEM((CHUNKS, 2, 2, ROWS, 4 * 224), bf16),
            pltpu.VMEM((8, 2, ROWS, 4 * 224), bf16),
            pltpu.VMEM((4096 // BLOCK, BLOCK), jnp.float32),
            pltpu.VMEM((HEADS * HALF, 128), jnp.float32),
            pltpu.VMEM((HEADS * HALF, 128), jnp.float32),
            pltpu.VMEM((HEADS * HALF, KVR), jnp.float32),
        ],
        compiler_params=pltpu.CompilerParams(
            collective_id=0, has_side_effects=True, vmem_limit_bytes=67000000
        ),
        cost_estimate=pl.CostEstimate(
            flops=20_000_000_000, bytes_accessed=16_000_000, transcendentals=0
        ),
        name="layer",
    )(
        q_latent.reshape(2, HALF, -1),
        kv_latent.T,
        kv_gain.reshape(1, -1),
        jnp.asarray(table, jnp.float32),
        response_mask.reshape(32, 128),
        prompt_len,
        w_q_b,
        w_kv_b,
        w_o.T,
    )
    return result


def solution(mesh):
    finer = Mesh(mesh.devices.reshape(2, 4, 4, 2, 2), AXES)
    placed = (
        P(DP, None),
        P(DP, None),
        P(),
        P(None, HEAD),
        P(None, HEAD),
        P(HEAD, DP),
        P(),
        P(),
    )
    return jax.shard_map(
        local, mesh=finer, in_specs=placed, out_specs=P(DP, HEAD), check_vma=False
    )
```

```python
import functools
import math

import jax
import jax.numpy as jnp
import numpy as np
from jax import lax
from jax.experimental import pallas as pl
from jax.experimental.pallas import tpu as pltpu
from jax.sharding import Mesh
from jax.sharding import PartitionSpec as P

KVR = 512
ROPE = 64
NOPE = 128
VD = 128
WIDE = KVR + ROPE
AXES = ("xh", "z", "y", "xl", "c")
DP = ("xh", "z", "y")
HEAD = ("xl", "c")
MESH = pl.DeviceIdType.MESH

HEADS = 16
CHUNKS = 4
HALF = 64
ROWS = 16
BLOCK = 512
LOG2E = 1.4426950408889634
EPS = 1e-06

CROSS = 0
SWAP = 1
D1 = 2
D1H = 6
D2 = 10
D2H = 26
PAIR = 42
WFULL = 74
WHALF = 78
WPAIR = 80
ABASE = 84
APAIR, AX, AZ, AZH, AX2 = 0, 1, 2, 6, 8
ASTRIDE = 10
OUT = ABASE + ASTRIDE * CHUNKS
XSUM = OUT + 8
NSEM = XSUM + 8


def turn(values, cosine, sine):
    swapped = jnp.concatenate([values[:, ROPE // 2 :], values[:, : ROPE // 2]], axis=1)
    return values * cosine + swapped * sine


def body(
    q_lat,
    kv_lat,
    gain,
    table,
    live,
    prompt,
    wq_hbm,
    wkv_hbm,
    wo_hbm,
    out_ref,
    out_sem,
    in_sem,
    local_sem,
    qx,
    wq,
    wkv,
    keys,
    qs,
    ctx,
    astage,
    ag,
    wg,
    part,
    outgoing,
    summand,
    bias,
    m_ref,
    l_ref,
    acc_ref,
):
    xh, z, y, xl, c = (lax.axis_index(a) for a in AXES)
    d1 = y + c * (z - y)
    d2 = z + c * (y - z)

    def place(t, o1, o2):
        a = lax.rem(d1 + o1 + 4, 4)
        b = lax.rem(d2 + o2 + 4, 4)
        zz = b + c * (a - b)
        yy = a + c * (b - a)
        xx = xh + t - 2 * xh * t
        return xx, zz, yy

    def unit(t, o1, o2):
        xx, zz, yy = place(t, o1, o2)
        return xx * 16 + zz * 4 + yy

    def near(o1, o2):
        _, zz, yy = place(0, o1, o2)
        return (xh, zz, yy, xl, c)

    def copy(src, dst, number, device, leaving=None):
        return pltpu.make_async_remote_copy(
            src_ref=src,
            dst_ref=dst,
            send_sem=out_sem.at[number if leaving is None else leaving],
            recv_sem=in_sem.at[number],
            device_id=device,
            device_id_type=MESH,
        )

    me = unit(0, 0, 0)
    partner = (xh, z, y, xl, 1 - c)
    cross = (1 - xh, z, y, 1 - xl, c)
    swap_peer = (1 - xh, 3 - z, y, 1 - xl, c)
    across = (1 - xh, z, y, xl, c)
    up_y = (xh, z, lax.rem(y + 1, 4), xl, c)
    down_y = (xh, z, lax.rem(y + 3, 4), xl, c)
    up_z = (xh, lax.rem(z + 1, 4), y, xl, c)
    down_z = (xh, lax.rem(z + 3, 4), y, xl, c)
    owners = [[(t, 2 * xl + k, y, xh, z // 2) for k in range(2)] for t in range(2)]
    makers = [(xl, 2 * c + k % 2, y, z // 2, k // 2) for k in range(4)]
    beside = (xh, z, y, 1 - xl, c)
    same = lambda u, v: 1 - jnp.minimum((u - v) * (u - v), 1)
    mine = same(c, xh) * same(xl, xh) * same(z // 2, c)
    z_low = z + xh * (3 - 2 * z)
    shard = (z_low * 4 + y, 16 + (3 - z_low) * 4 + y)

    with jax.named_scope("start"):
        pltpu.make_async_copy(wkv_hbm, wkv, local_sem.at[8]).start()
        for j in range(8):
            pltpu.make_async_copy(
                wq_hbm.at[:, pl.ds(j * 384, 384)], wq.at[j], local_sem.at[j]
            ).start()
        pltpu.make_async_copy(wo_hbm, wg.at[c, y], local_sem.at[9]).start()

    barrier = pltpu.get_barrier_semaphore()
    far = near(2, 0)
    for peer in (partner, cross, swap_peer, across, beside, far, up_y, down_y, up_z, down_z):
        pl.semaphore_signal(barrier, inc=1, device_id=peer, device_id_type=MESH)
    for k in range(4):

        @pl.when((mine == 0) | (makers[k][1] != z) | (k // 2 != c))
        def _(k=k):
            pl.semaphore_signal(barrier, inc=1, device_id=makers[k], device_id_type=MESH)

    with jax.named_scope("norm"):
        lane = lax.broadcasted_iota(jnp.int32, (1, ROPE), 1)
        sign = jnp.where(lane < ROPE // 2, -1.0, 1.0)

        def angles(m):
            cos_a, sin_a = table[2, pl.ds(m, 1), :], table[3, pl.ds(m, 1), :]
            cos_b, sin_b = table[0], table[1]
            return cos_a * cos_b - sin_a * sin_b, (sin_a * cos_b + cos_a * sin_b) * sign

        turned_rows = kv_lat[...].astype(jnp.float32).T
        rows = jnp.where(c == 0, turned_rows[:HALF], turned_rows[HALF:])
        latent = rows[:, :KVR]
        inverse = lax.rsqrt(jnp.mean(latent * latent, axis=-1, keepdims=True) + EPS)
        keys[me, c, :, :KVR] = (latent * inverse * gain[...]).astype(jnp.bfloat16)
        keys[me, c, :, KVR:] = turn(rows[:, KVR:], *angles(me * 2 + c)).astype(jnp.bfloat16)
        qx[xh] = q_lat[xh]
        spot = lax.broadcasted_iota(jnp.int32, (32, 128), 0) * 128 + lax.broadcasted_iota(
            jnp.int32, (32, 128), 1
        )
        usable = (spot < prompt[0]) | (live[...] == 1)
        masked = jnp.where(usable, 0.0, -1e30)
        for r in range(32):
            b, at = r // (BLOCK // 128), r % (BLOCK // 128)
            bias[b : b + 1, at * 128 : (at + 1) * 128] = masked[r : r + 1]

    with jax.named_scope("barrier"):
        pl.semaphore_wait(barrier, 14 - mine)

    def key(t, o1, o2, which=None):
        ref = keys.at[unit(t, o1, o2), c]
        if which is None:
            return ref
        return ref.at[pl.ds(32 * which, 32)]

    def key_copy(number, t, o1, o2, device, which=None):
        ref = key(t, o1, o2, which)
        return copy(ref, ref, number, device)

    offsets = (0, 1, 3, 2)
    lower, upper = xh, 1 - xh

    def spread(q, t):
        k, o = 2 * q + t, offsets[q]
        key_copy(D2 + 2 * k, t, o, 0, near(0, 1)).start()
        key_copy(D2 + 2 * k + 1, t, o, 0, near(0, -1)).start()
        key_copy(PAIR + k, t, o, 0, partner).start()

    def first_out(t):
        key_copy(D1 + 2 * t, t, 0, 0, near(1, 0)).start()
        key_copy(D1 + 2 * t + 1, t, 0, 0, near(-1, 0)).start()
        spread(0, t)
        key_copy(D1H + t, t, 0, 0, far).start()

    def first_in(t):
        key_copy(D1 + 2 * t, t, -1, 0, near(1, 0)).wait_recv()
        spread(2, t)
        key_copy(D1 + 2 * t + 1, t, 1, 0, near(-1, 0)).wait_recv()
        spread(1, t)

    def far_in(t):
        key_copy(D1H + t, t, 2, 0, far).wait_recv()
        spread(3, t)

    def cross_in():
        key_copy(CROSS, 1, 0, 0, cross).wait_recv()

    with jax.named_scope("spread"):
        key_copy(CROSS, 0, 0, 0, cross).start()
        pl.when(xh == 1)(cross_in)
        first_out(lower)
        swap = copy(q_lat.at[1 - xh], qx.at[xh], SWAP, swap_peer)
        swap_in = copy(q_lat.at[1 - xh], qx.at[1 - xh], SWAP, swap_peer)
        swap.start()
        pl.when(xh == 0)(cross_in)
        first_out(upper)

    tables = [angles(2 * where + xh) for where in shard]

    def project(j):
        pltpu.make_async_copy(
            wq_hbm.at[:, pl.ds(0, 384)], wq.at[j], local_sem.at[j]
        ).wait()
        both = jnp.dot(
            qx[...].reshape(2 * HALF, -1), wq[j], preferred_element_type=jnp.float32
        ).astype(jnp.bfloat16)
        for e in range(2):
            h = 2 * j + e
            plain = both[:, e * 192 : e * 192 + NOPE]
            roped = both[:, e * 192 + NOPE : (e + 1) * 192].astype(jnp.float32)
            w_key = wkv[:, pl.ds(pl.multiple_of(h * 256, 256), NOPE)]
            absorbed = lax.dot_general(
                plain, w_key, (((1,), (1,)), ((), ())), preferred_element_type=jnp.float32
            ).astype(jnp.bfloat16)
            for half in range(2):
                mine_rows = slice(half * HALF, (half + 1) * HALF)
                qs[half, h, :, :KVR] = absorbed[mine_rows]
                qs[half, h, :, KVR:] = turn(roped[mine_rows], *tables[half]).astype(jnp.bfloat16)

    def relay(q, t):
        k, o = 2 * q + t, offsets[q]
        key_copy(D2 + 2 * k, t, o, -1, near(0, 1)).wait_recv()
        key_copy(D2H + 2 * k, t, o, -1, near(0, 1), 0).start()
        key_copy(PAIR + 8 + k, t, o, -1, partner).start()
        key_copy(D2 + 2 * k + 1, t, o, 1, near(0, -1)).wait_recv()
        key_copy(D2H + 2 * k + 1, t, o, 1, near(0, -1), 1).start()
        key_copy(PAIR + 16 + k, t, o, 1, partner).start()

    def last_in(q, t):
        k, o = 2 * q + t, offsets[q]
        key_copy(D2H + 2 * k, t, o, 2, near(0, 1), 0).wait_recv()
        key_copy(D2H + 2 * k + 1, t, o, 2, near(0, -1), 1).wait_recv()
        key_copy(PAIR + 24 + k, t, o, 2, partner).start()

    def pair_in(t):
        def one(n, carry):
            ref = keys.at[0, 1 - c]
            copy(ref, ref, PAIR + 2 * n + t, partner).wait_recv()
            return carry

        lax.fori_loop(0, 16, one, 0)

    span = wo_hbm.shape[0] // 2

    def w_copy(number, row, device, which):
        ref = wg.at[c, row, pl.ds(which * span, span)]
        return copy(ref, ref, number, device)

    def w_pair(row, number):
        return copy(wg.at[c, row], wg.at[c, row], WPAIR + number, partner)

    def w_pair_in(row, number):
        return copy(wg.at[1 - c, row], wg.at[1 - c, row], WPAIR + number, partner)

    with jax.named_scope("first_in_l"):
        first_in(lower)
    with jax.named_scope("relay_l0"):
        relay(0, lower)
    with jax.named_scope("far_l"):
        far_in(lower)
    with jax.named_scope("swap"):
        swap_in.wait_recv()
    with jax.named_scope("wkv"):
        pltpu.make_async_copy(wkv_hbm, wkv, local_sem.at[8]).wait()
    with jax.named_scope("project"):
        project(0)
    with jax.named_scope("relay_l21"):
        relay(2, lower)
        relay(1, lower)
    with jax.named_scope("project"):
        project(1)
    with jax.named_scope("first_in_u"):
        first_in(upper)
    with jax.named_scope("project"):
        project(2)
    with jax.named_scope("relay_l3"):
        relay(3, lower)
    with jax.named_scope("project"):
        project(3)
    with jax.named_scope("far_u"):
        far_in(upper)
    with jax.named_scope("relay_u0"):
        relay(0, upper)
    with jax.named_scope("project"):
        project(4)
    with jax.named_scope("last_in_l"):
        for q in (0, 2, 1):
            last_in(q, lower)
    with jax.named_scope("project"):
        project(5)
        project(6)
    with jax.named_scope("last_in_l3"):
        last_in(3, lower)
    with jax.named_scope("relay_u21"):
        relay(2, upper)
        relay(1, upper)
    with jax.named_scope("project"):
        project(7)
    with jax.named_scope("pair_in_l"):
        pair_in(lower)

    scale = LOG2E / math.sqrt(NOPE + ROPE)
    tile_rows = HEADS * HALF
    reach = BLOCK // 128

    def attend(half, hooks):
        where = shard[half]
        blocks = where // reach
        m_ref[...] = jnp.full_like(m_ref, -1e30)
        l_ref[...] = jnp.zeros_like(l_ref)
        acc_ref[...] = jnp.zeros_like(acc_ref)

        def step(b, causal):
            block = keys[pl.ds(b * reach, reach)].reshape(BLOCK, WIDE)
            scores = lax.dot_general(
                qs[half].reshape(tile_rows, WIDE),
                block,
                (((1,), (1,)), ((), ())),
                preferred_element_type=jnp.float32,
            )
            scores = scores * scale + bias[pl.ds(b, 1), :]
            if causal is not None:
                scores = (scores.reshape(HEADS, HALF, BLOCK) + causal[None]).reshape(
                    tile_rows, BLOCK
                )
            before = m_ref[...]
            m_new = jnp.maximum(before, jnp.max(scores, axis=1, keepdims=True))
            alpha = jnp.exp2(before - m_new)
            lifted = jnp.exp2(scores - jnp.concatenate([m_new] * (BLOCK // 128), axis=1))
            total = l_ref[...] * alpha
            for k in range(BLOCK // 128):
                total = total + lifted[:, k * 128 : (k + 1) * 128]
            l_ref[...] = total
            m_ref[...] = m_new
            acc_ref[...] = acc_ref[...] * jnp.concatenate([alpha] * (KVR // 128), axis=1) + jnp.dot(
                lifted.astype(jnp.bfloat16), block[:, :KVR], preferred_element_type=jnp.float32
            )

        def open_step(b, carry):
            hooks(b, blocks)
            step(b, None)
            return carry

        lax.fori_loop(0, blocks, open_step, 0)
        hooks(blocks, blocks)
        token = where * 128 + xh * HALF + lax.broadcasted_iota(jnp.int32, (HALF, BLOCK), 0)
        position = blocks * BLOCK + lax.broadcasted_iota(jnp.int32, (HALF, BLOCK), 1)
        step(blocks, jnp.where(position <= token, 0.0, -1e30))
        total = jnp.sum(l_ref[...], axis=1, keepdims=True)
        ctx[...] = (acc_ref[...] / total).astype(jnp.bfloat16).reshape(HEADS, HALF, KVR)

    here = xh * 4 + z

    def values(half):
        for h in range(HEADS):
            w_value = wkv[:, h * 256 + NOPE : (h + 1) * 256]
            attended = jnp.dot(ctx[h], w_value, preferred_element_type=jnp.float32).astype(
                jnp.bfloat16
            )
            for r in range(2):
                for to in range(2):
                    at = to * 2 * ROWS + r * ROWS
                    astage[2 * half + r, to, :, h * VD : (h + 1) * VD] = attended[at : at + ROWS]
        for g in (2 * half, 2 * half + 1):
            pair_copy(g).start()
            ag[here, g, c] = astage[g, c]

    def a_copy(g, number, t, o, device, which=None):
        slot = (xh + t - 2 * xh * t) * 4 + lax.rem(z + o + 4, 4)
        ref = ag.at[slot, g]
        if which is not None:
            ref = ref.at[which]
        return copy(ref, ref, ABASE + ASTRIDE * g + number, device)

    def pair_copy(g):
        return copy(
            astage.at[g, 1 - c], ag.at[here, g, c], ABASE + ASTRIDE * g + APAIR, partner
        )

    def pair_copy_in(g):
        ref = ag.at[here, g, 1 - c]
        return copy(ref, ref, ABASE + ASTRIDE * g + APAIR, partner)

    def stage1(g):
        pair_copy_in(g).wait_recv()
        a_copy(g, AX, 0, 0, across).start()
        a_copy(g, AZ, 0, 0, up_z).start()
        a_copy(g, AZ + 1, 0, 0, down_z).start()

    def stage2(g):
        a_copy(g, AZ, 0, -1, up_z).wait_recv()
        a_copy(g, AZH, 0, -1, up_z, 0).start()
        a_copy(g, AZ + 1, 0, 1, down_z).wait_recv()
        a_copy(g, AZH + 1, 0, 1, down_z, 1).start()

    def stage3(g):
        a_copy(g, AX, 1, 0, across).wait_recv()
        a_copy(g, AZ + 2, 1, 0, up_z).start()
        a_copy(g, AZ + 3, 1, 0, down_z).start()

    def stage4(g):
        a_copy(g, AZH, 0, 2, up_z, 0).wait_recv()
        a_copy(g, AZH + 1, 0, 2, down_z, 1).wait_recv()
        a_copy(g, AX2, 0, 2, across).start()

    def stage5(g):
        a_copy(g, AZ + 2, 1, -1, up_z).wait_recv()
        a_copy(g, AZ + 3, 1, 1, down_z).wait_recv()
        a_copy(g, AX2, 1, 2, across).wait_recv()

    def w_relay(which):
        if which == 0:
            w_copy(WFULL, lax.rem(y + 3, 4), up_y, 0).wait_recv()
            w_copy(WHALF, lax.rem(y + 3, 4), up_y, 0).start()
        else:
            w_copy(WFULL + 3, lax.rem(y + 1, 4), down_y, 1).wait_recv()
            w_copy(WHALF + 1, lax.rem(y + 1, 4), down_y, 1).start()

    def w_middle():
        w_copy(WFULL + 1, lax.rem(y + 3, 4), up_y, 1).wait_recv()
        w_pair(lax.rem(y + 3, 4), 1).start()
        w_copy(WFULL + 2, lax.rem(y + 1, 4), down_y, 0).wait_recv()
        w_pair(lax.rem(y + 1, 4), 2).start()

    def w_last():
        w_copy(WHALF, lax.rem(y + 2, 4), up_y, 0).wait_recv()
        w_copy(WHALF + 1, lax.rem(y + 2, 4), down_y, 1).wait_recv()
        w_pair(lax.rem(y + 2, 4), 3).start()

    def w_all():
        for k, o in enumerate((0, 3, 1, 2)):
            w_pair_in(lax.rem(y + o, 4), k).wait_recv()

    def product(first, count):
        rows = 8 * count * ROWS
        total = jnp.zeros((rows, 4 * 224), jnp.float32)
        for core in range(2):
            total = total + lax.dot_general(
                ag[:, first : first + count, core].reshape(rows, HEADS * VD),
                wg[core].reshape(4 * 224, HEADS * VD),
                (((1,), (1,)), ((), ())),
                preferred_element_type=jnp.float32,
            )
        total = total.reshape(8, count * ROWS, 4 * 224)
        for n in range(count):
            part[first + n] = total[:, n * ROWS : (n + 1) * ROWS]

    def slots(half, k):
        straight, mirrored = k, 3 - k
        first = straight if half == 0 else mirrored
        return first, 4 + 3 - first

    def half_out(g):
        for k in range(2):
            low, high = slots(g // 2, 2 * (1 - xl) + k)
            outgoing[g, 0, k, 0] = part[g, low].astype(jnp.bfloat16)
            outgoing[g, 0, k, 1] = part[g, high].astype(jnp.bfloat16)
            copy(outgoing.at[g, 0, k], summand.at[g, k], XSUM + 2 * g + k, beside).start()

    def whole_out(g):
        half = g // 2
        number = lax.rem(z, 2) + 2 * c + 4 * (g % 2)
        for k in range(2):
            row = 2 * xl + k
            copy(outgoing.at[g, 0, k], summand.at[g, k], XSUM + 2 * g + k, beside).wait_recv()
            low, high = slots(half, row)
            for xs, at in enumerate((low, high)):
                outgoing[g, 1, k, xs] = (
                    part[g, at] + summand[g, k, xs].astype(jnp.float32)
                ).astype(jnp.bfloat16)
            own = (mine == 1) & (xh == half) & (z == row)
            target = out_ref.at[:, 2 * c + g % 2, :, pl.ds(lax.rem(z, 2) * 896, 896)]

            @pl.when(jnp.logical_not(own))
            def _():
                copy(
                    outgoing.at[g, 1, k], target, OUT + number, owners[half][k], OUT + 2 * g + k
                ).start()

            @pl.when(own)
            def _():
                pltpu.make_async_copy(
                    outgoing.at[g, 1, k], target, local_sem.at[10 + g % 2]
                ).start()

    def start_w():
        pltpu.make_async_copy(wo_hbm, wg.at[c, y], local_sem.at[9]).wait()
        for which in range(2):
            w_copy(WFULL + which, y, up_y, which).start()
            w_copy(WFULL + 3 - which, y, down_y, 1 - which).start()
        w_pair(y, 0).start()

    def early_hooks(b, blocks):
        @pl.when(b == jnp.minimum(1, blocks))
        def _():
            with jax.named_scope("relay_u3"):
                relay(3, upper)
                start_w()

    def late_hooks(b, blocks):
        @pl.when(b == 0)
        def _():
            with jax.named_scope("last_in_u"):
                for q in (0, 2, 1, 3):
                    last_in(q, upper)

        @pl.when(b == 1)
        def _():
            with jax.named_scope("stage1_01"):
                stage1(0)
                stage1(1)

        @pl.when(b == 4)
        def _():
            with jax.named_scope("pair_in_u"):
                pair_in(upper)

        @pl.when(b == blocks)
        def _():
            with jax.named_scope("stage23_0"):
                stage2(0)
                stage3(0)
                w_relay(0)
                w_relay(1)

    with jax.named_scope("attend_low"):
        attend(0, early_hooks)
    with jax.named_scope("values"):
        values(0)
    with jax.named_scope("attend_high"):
        attend(1, late_hooks)
    with jax.named_scope("values"):
        values(1)
    with jax.named_scope("stage23_1"):
        stage2(1)
        stage3(1)
    with jax.named_scope("stage4_0"):
        stage4(0)
    with jax.named_scope("stage4_1"):
        stage4(1)
    with jax.named_scope("stage1_23"):
        stage1(2)
        stage1(3)
    with jax.named_scope("w_middle"):
        w_middle()
    with jax.named_scope("stage5_0"):
        stage5(0)
    with jax.named_scope("stage5_1"):
        stage5(1)
    with jax.named_scope("stage23_2"):
        stage2(2)
        stage3(2)
    with jax.named_scope("w_last"):
        w_last()
        w_all()
    with jax.named_scope("product_low"):
        product(0, 2)
    with jax.named_scope("half_out_low"):
        half_out(0)
        half_out(1)
    with jax.named_scope("stage23_3"):
        stage2(3)
        stage3(3)
    with jax.named_scope("stage4_2"):
        stage4(2)
    with jax.named_scope("whole_out_low"):
        whole_out(0)
        whole_out(1)
    with jax.named_scope("stage4_3"):
        stage4(3)
    with jax.named_scope("stage5_2"):
        stage5(2)
    with jax.named_scope("stage5_3"):
        stage5(3)
    with jax.named_scope("product_high"):
        product(2, 2)
    with jax.named_scope("half_out_high"):
        half_out(2)
        half_out(3)
    with jax.named_scope("whole_out_high"):
        whole_out(2)
        whole_out(3)

    with jax.named_scope("finish"):
        for n in range(8):
            r, k = n // 4, n % 4
            piece = out_ref.at[:, 2 * (k // 2) + r, :, (k % 2) * 896 : (k % 2 + 1) * 896]
            self_made = (mine == 1) & (makers[k][1] == z) & (k // 2 == c)

            @pl.when(jnp.logical_not(self_made))
            def _(n=n, piece=piece):
                copy(piece, piece, OUT + n, partner).wait_recv()

            @pl.when(self_made)
            def _(r=r, piece=piece):
                pltpu.make_async_copy(outgoing.at[0, 1, 0], piece, local_sem.at[10 + r]).wait()

    with jax.named_scope("drain"):
        full = keys.at[0, 0]
        part_key = keys.at[0, 0, pl.ds(0, 32)]

        def sent(ref, number):
            copy(ref, ref, number, partner).wait_send()

        def drain(ref, first, count):
            def one(n, carry):
                sent(ref, first + n)
                return carry

            lax.fori_loop(0, count, one, 0)

        sent(full, CROSS)
        sent(qx.at[0], SWAP)
        drain(full, D1, 4)
        drain(full, D1H, 2)
        drain(full, D2, 16)
        drain(part_key, D2H, 16)
        drain(full, PAIR, 32)
        drain(wg.at[0, 0, pl.ds(0, span)], WFULL, 4)
        drain(wg.at[0, 0, pl.ds(0, span)], WHALF, 2)
        drain(wg.at[0, 0], WPAIR, 4)
        for g in range(CHUNKS):
            at = ABASE + ASTRIDE * g
            sent(astage.at[g, 0], at + APAIR)
            sent(ag.at[0, 0], at + AX)
            drain(ag.at[0, 0], at + AZ, 4)
            drain(ag.at[0, 0, 0], at + AZH, 2)
            sent(ag.at[0, 0], at + AX2)
        drain(summand.at[0, 0], XSUM, 8)
        for g in range(CHUNKS):
            for k in range(2):
                own = (mine == 1) & (xh == g // 2) & (z == 2 * xl + k)

                @pl.when(jnp.logical_not(own))
                def _(g=g, k=k):
                    sent(summand.at[0, 0], OUT + 2 * g + k)


def local(q_latent, kv_latent, kv_gain, w_q_b, w_kv_b, w_o, prompt_len, response_mask):
    frequency = 10000.0 ** (-np.arange(ROPE // 2, dtype=np.float64) * 2.0 / ROPE)
    fine = np.arange(HALF, dtype=np.float64)[:, None] * np.tile(frequency, 2)[None, :]
    table = np.stack([np.cos(fine), np.sin(fine), np.cos(HALF * fine), np.sin(HALF * fine)])
    vmem = pl.BlockSpec(memory_space=pltpu.VMEM)
    hbm = pl.BlockSpec(memory_space=pl.ANY)
    bf16 = jnp.bfloat16
    depth = HEADS * VD
    result = pl.pallas_call(
        body,
        out_shape=jax.ShapeDtypeStruct((2, 4, ROWS, 1792), bf16),
        in_specs=[vmem] * 5 + [pl.BlockSpec(memory_space=pltpu.SMEM)] + [hbm] * 3,
        out_specs=hbm,
        scratch_shapes=[
            pltpu.SemaphoreType.DMA((NSEM,)),
            pltpu.SemaphoreType.DMA((NSEM,)),
            pltpu.SemaphoreType.DMA((12,)),
            pltpu.VMEM((2, HALF, 1536), bf16),
            pltpu.VMEM((8, 1536, 384), bf16),
            pltpu.VMEM((512, 4096), bf16),
            pltpu.VMEM((32, 2, HALF, WIDE), bf16),
            pltpu.VMEM((2, HEADS, HALF, WIDE), bf16),
            pltpu.VMEM((HEADS, HALF, KVR), bf16),
            pltpu.VMEM((CHUNKS, 2, ROWS, depth), bf16),
            pltpu.VMEM((8, CHUNKS, 2, ROWS, depth), bf16),
            pltpu.VMEM((2, 4, 224, 2048), bf16),
            pltpu.VMEM((CHUNKS, 8, ROWS, 4 * 224), jnp.float32),
            pltpu.VMEM((CHUNKS, 2, 2, 2, ROWS, 4 * 224), bf16),
            pltpu.VMEM((CHUNKS, 2, 2, ROWS, 4 * 224), bf16),
            pltpu.VMEM((4096 // BLOCK, BLOCK), jnp.float32),
            pltpu.VMEM((HEADS * HALF, 128), jnp.float32),
            pltpu.VMEM((HEADS * HALF, 128), jnp.float32),
            pltpu.VMEM((HEADS * HALF, KVR), jnp.float32),
        ],
        compiler_params=pltpu.CompilerParams(
            collective_id=0, has_side_effects=True, vmem_limit_bytes=67000000
        ),
        cost_estimate=pl.CostEstimate(
            flops=20_000_000_000, bytes_accessed=16_000_000, transcendentals=0
        ),
        name="layer",
    )(
        q_latent.reshape(2, HALF, -1),
        kv_latent.T,
        kv_gain.reshape(1, -1),
        jnp.asarray(table, jnp.float32),
        response_mask.reshape(32, 128),
        prompt_len,
        w_q_b,
        w_kv_b,
        w_o.T,
    )
    return result.reshape(128, 1792)


def solution(mesh):
    finer = Mesh(mesh.devices.reshape(2, 4, 4, 2, 2), AXES)
    placed = (
        P(DP, None),
        P(DP, None),
        P(),
        P(None, HEAD),
        P(None, HEAD),
        P(HEAD, DP),
        P(),
        P(),
    )
    return jax.shard_map(
        local, mesh=finer, in_specs=placed, out_specs=P(DP, HEAD), check_vma=False
    )
```

```python
import functools
import math

import jax
import jax.numpy as jnp
import numpy as np
from jax import lax
from jax.experimental import pallas as pl
from jax.experimental.pallas import tpu as pltpu
from jax.sharding import Mesh
from jax.sharding import PartitionSpec as P

KVR = 512
ROPE = 64
NOPE = 128
VD = 128
WIDE = KVR + ROPE
AXES = ("xh", "z", "y", "xl", "c")
DP = ("xh", "z", "y")
HEAD = ("xl", "c")
MESH = pl.DeviceIdType.MESH

HEADS = 16
CHUNKS = 4
HALF = 64
ROWS = 16
BLOCK = 512
LOG2E = 1.4426950408889634
EPS = 1e-06

CROSS = 0
SWAP = 1
D1 = 2
D1H = 6
SWAP2 = 8
D2 = 10
D2H = 26
PAIR = 42
WFULL = 74
WHALF = 78
WPAIR = 80
ABASE = 84
APAIR, AX, AZ, AZH, AX2 = 0, 1, 2, 6, 8
ASTRIDE = 10
OUT = ABASE + ASTRIDE * CHUNKS
XSUM = OUT + 8
NSEM = XSUM + 8


def turn(values, cosine, sine):
    swapped = jnp.concatenate([values[:, ROPE // 2 :], values[:, : ROPE // 2]], axis=1)
    return values * cosine + swapped * sine


def body(
    q_hbm,
    kv_hbm,
    gain_hbm,
    table_hbm,
    live_hbm,
    prompt,
    wq_hbm,
    wkv_hbm,
    wo_hbm,
    out_ref,
    out_sem,
    in_sem,
    local_sem,
    kv_lat,
    gain,
    table,
    live,
    qx,
    wq,
    wkv,
    keys,
    qs,
    ctx,
    astage,
    ag,
    wg,
    part,
    outgoing,
    summand,
    bias,
    m_ref,
    l_ref,
    acc_ref,
):
    xh, z, y, xl, c = (lax.axis_index(a) for a in AXES)
    d1 = y + c * (z - y)
    d2 = z + c * (y - z)

    def place(t, o1, o2):
        a = lax.rem(d1 + o1 + 4, 4)
        b = lax.rem(d2 + o2 + 4, 4)
        zz = b + c * (a - b)
        yy = a + c * (b - a)
        xx = xh + t - 2 * xh * t
        return xx, zz, yy

    def unit(t, o1, o2):
        xx, zz, yy = place(t, o1, o2)
        return xx * 16 + zz * 4 + yy

    def near(o1, o2):
        _, zz, yy = place(0, o1, o2)
        return (xh, zz, yy, xl, c)

    def copy(src, dst, number, device, leaving=None):
        return pltpu.make_async_remote_copy(
            src_ref=src,
            dst_ref=dst,
            send_sem=out_sem.at[number if leaving is None else leaving],
            recv_sem=in_sem.at[number],
            device_id=device,
            device_id_type=MESH,
        )

    me = unit(0, 0, 0)
    partner = (xh, z, y, xl, 1 - c)
    cross = (1 - xh, z, y, 1 - xl, c)
    swap_peer = (1 - xh, 3 - z, y, 1 - xl, c)
    across = (1 - xh, z, y, xl, c)
    up_y = (xh, z, lax.rem(y + 1, 4), xl, c)
    down_y = (xh, z, lax.rem(y + 3, 4), xl, c)
    up_z = (xh, lax.rem(z + 1, 4), y, xl, c)
    down_z = (xh, lax.rem(z + 3, 4), y, xl, c)
    owners = [[(t, 2 * xl + k, y, xh, z // 2) for k in range(2)] for t in range(2)]
    makers = [(xl, 2 * c + k % 2, y, z // 2, k // 2) for k in range(4)]
    beside = (xh, z, y, 1 - xl, c)
    same = lambda u, v: 1 - jnp.minimum((u - v) * (u - v), 1)
    mine = same(c, xh) * same(xl, xh) * same(z // 2, c)
    z_low = z + xh * (3 - 2 * z)
    shard = (z_low * 4 + y, 16 + (3 - z_low) * 4 + y)

    barrier = pltpu.get_barrier_semaphore()
    far = near(2, 0)
    for peer in (partner, cross, swap_peer, across, beside, far, up_y, down_y, up_z, down_z):
        pl.semaphore_signal(barrier, inc=1, device_id=peer, device_id_type=MESH)
    for k in range(4):

        @pl.when((mine == 0) | (makers[k][1] != z) | (k // 2 != c))
        def _(k=k):
            pl.semaphore_signal(barrier, inc=1, device_id=makers[k], device_id_type=MESH)

    inputs = ((kv_hbm, kv_lat), (gain_hbm, gain), (table_hbm, table), (live_hbm, live))
    for n, (far_away, close) in enumerate(inputs):
        pltpu.make_async_copy(far_away, close, local_sem.at[12 + n]).start()
    own_rows = pltpu.make_async_copy(q_hbm.at[xh], qx.at[xh], local_sem.at[16])
    own_rows.start()
    pltpu.make_async_copy(wkv_hbm, wkv, local_sem.at[8]).start()
    for j in range(8):
        pltpu.make_async_copy(wq_hbm.at[:, pl.ds(j * 384, 384)], wq.at[j], local_sem.at[j]).start()
    pltpu.make_async_copy(wo_hbm, wg.at[c, y], local_sem.at[9]).start()

    with jax.named_scope("norm"):
        for n, (far_away, close) in enumerate(inputs):
            pltpu.make_async_copy(far_away, close, local_sem.at[12 + n]).wait()
        lane = lax.broadcasted_iota(jnp.int32, (1, ROPE), 1)
        sign = jnp.where(lane < ROPE // 2, -1.0, 1.0)

        def angles(m):
            cos_a, sin_a = table[2, pl.ds(m, 1), :], table[3, pl.ds(m, 1), :]
            cos_b, sin_b = table[0], table[1]
            return cos_a * cos_b - sin_a * sin_b, (sin_a * cos_b + cos_a * sin_b) * sign

        turned_rows = kv_lat[...].astype(jnp.float32).T
        rows = jnp.where(c == 0, turned_rows[:HALF], turned_rows[HALF:])
        latent = rows[:, :KVR]
        inverse = lax.rsqrt(jnp.mean(latent * latent, axis=-1, keepdims=True) + EPS)
        keys[me, c, :, :KVR] = (latent * inverse * gain[...]).astype(jnp.bfloat16)
        keys[me, c, :, KVR:] = turn(rows[:, KVR:], *angles(me * 2 + c)).astype(jnp.bfloat16)
        spot = lax.broadcasted_iota(jnp.int32, (32, 128), 0) * 128 + lax.broadcasted_iota(
            jnp.int32, (32, 128), 1
        )
        usable = (spot < prompt[0]) | (live[...] == 1)
        masked = jnp.where(usable, 0.0, -1e30)
        for r in range(32):
            b, at = r // (BLOCK // 128), r % (BLOCK // 128)
            bias[b : b + 1, at * 128 : (at + 1) * 128] = masked[r : r + 1]

    with jax.named_scope("barrier"):
        pl.semaphore_wait(barrier, 14 - mine)

    def key(t, o1, o2, which=None):
        ref = keys.at[unit(t, o1, o2), c]
        if which is None:
            return ref
        return ref.at[pl.ds(32 * which, 32)]

    def key_copy(number, t, o1, o2, device, which=None):
        ref = key(t, o1, o2, which)
        return copy(ref, ref, number, device)

    offsets = (0, 1, 3, 2)
    lower, upper = xh, 1 - xh

    def spread(q, t):
        k, o = 2 * q + t, offsets[q]
        key_copy(D2 + 2 * k, t, o, 0, near(0, 1)).start()
        key_copy(D2 + 2 * k + 1, t, o, 0, near(0, -1)).start()
        key_copy(PAIR + k, t, o, 0, partner).start()

    def first_out(t):
        key_copy(D1 + 2 * t, t, 0, 0, near(1, 0)).start()
        key_copy(D1 + 2 * t + 1, t, 0, 0, near(-1, 0)).start()
        spread(0, t)
        key_copy(D1H + t, t, 0, 0, far).start()

    def first_in(t):
        key_copy(D1 + 2 * t, t, -1, 0, near(1, 0)).wait_recv()
        spread(2, t)
        key_copy(D1 + 2 * t + 1, t, 1, 0, near(-1, 0)).wait_recv()
        spread(1, t)

    def far_in(t):
        key_copy(D1H + t, t, 2, 0, far).wait_recv()
        spread(3, t)

    def cross_in():
        key_copy(CROSS, 1, 0, 0, cross).wait_recv()

    with jax.named_scope("spread"):
        key_copy(CROSS, 0, 0, 0, cross).start()
        copy(q_hbm.at[1 - xh, c], qx.at[xh, c], SWAP, swap_peer).start()
        pl.when(xh == 1)(cross_in)
        first_out(lower)
        pl.when(xh == 0)(cross_in)
        first_out(upper)

    tables = [angles(2 * where + xh) for where in shard]

    def project(j):
        pltpu.make_async_copy(
            wq_hbm.at[:, pl.ds(0, 384)], wq.at[j], local_sem.at[j]
        ).wait()
        both = jnp.dot(
            qx[...].reshape(2 * HALF, 1536), wq[j], preferred_element_type=jnp.float32
        ).astype(jnp.bfloat16)
        for e in range(2):
            h = 2 * j + e
            plain = both[:, e * 192 : e * 192 + NOPE]
            roped = both[:, e * 192 + NOPE : (e + 1) * 192].astype(jnp.float32)
            w_key = wkv[:, pl.ds(pl.multiple_of(h * 256, 256), NOPE)]
            absorbed = lax.dot_general(
                plain, w_key, (((1,), (1,)), ((), ())), preferred_element_type=jnp.float32
            ).astype(jnp.bfloat16)
            for half in range(2):
                mine_rows = slice(half * HALF, (half + 1) * HALF)
                qs[half, h, :, :KVR] = absorbed[mine_rows]
                qs[half, h, :, KVR:] = turn(roped[mine_rows], *tables[half]).astype(jnp.bfloat16)

    def relay(q, t):
        k, o = 2 * q + t, offsets[q]
        key_copy(D2 + 2 * k, t, o, -1, near(0, 1)).wait_recv()
        key_copy(D2H + 2 * k, t, o, -1, near(0, 1), 0).start()
        key_copy(PAIR + 8 + k, t, o, -1, partner).start()
        key_copy(D2 + 2 * k + 1, t, o, 1, near(0, -1)).wait_recv()
        key_copy(D2H + 2 * k + 1, t, o, 1, near(0, -1), 1).start()
        key_copy(PAIR + 16 + k, t, o, 1, partner).start()

    def last_in(q, t):
        k, o = 2 * q + t, offsets[q]
        key_copy(D2H + 2 * k, t, o, 2, near(0, 1), 0).wait_recv()
        key_copy(D2H + 2 * k + 1, t, o, 2, near(0, -1), 1).wait_recv()
        key_copy(PAIR + 24 + k, t, o, 2, partner).start()

    def pair_in(t):
        def one(n, carry):
            ref = keys.at[0, 1 - c]
            copy(ref, ref, PAIR + 2 * n + t, partner).wait_recv()
            return carry

        lax.fori_loop(0, 16, one, 0)

    span = wo_hbm.shape[0] // 2

    def w_copy(number, row, device, which):
        ref = wg.at[c, row, pl.ds(which * span, span)]
        return copy(ref, ref, number, device)

    def w_pair(row, number):
        return copy(wg.at[c, row], wg.at[c, row], WPAIR + number, partner)

    def w_pair_in(row, number):
        return copy(wg.at[1 - c, row], wg.at[1 - c, row], WPAIR + number, partner)

    def project_in(*order):
        with jax.named_scope("project"):
            for j in order:
                project(j)

    def start_w():
        pltpu.make_async_copy(wo_hbm, wg.at[c, y], local_sem.at[9]).wait()
        for which in range(2):
            w_copy(WFULL + which, y, up_y, which).start()
            w_copy(WFULL + 3 - which, y, down_y, 1 - which).start()
        w_pair(y, 0).start()

    with jax.named_scope("first_in_l"):
        first_in(lower)
    with jax.named_scope("relay_l0"):
        relay(0, lower)
    with jax.named_scope("far_l"):
        far_in(lower)
    with jax.named_scope("swap"):
        copy(qx.at[1 - xh, c], qx.at[1 - xh, c], SWAP, swap_peer).wait_recv()
        copy(qx.at[1 - xh, c], qx.at[1 - xh, c], SWAP2, partner).start()
    with jax.named_scope("relay_l21"):
        relay(2, lower)
        relay(1, lower)
    with jax.named_scope("swap2"):
        copy(qx.at[1 - xh, 1 - c], qx.at[1 - xh, 1 - c], SWAP2, partner).wait_recv()
        own_rows.wait()
        pltpu.make_async_copy(wkv_hbm, wkv, local_sem.at[8]).wait()
    project_in(0)
    with jax.named_scope("relay_l3"):
        relay(3, lower)
    with jax.named_scope("first_in_u"):
        first_in(upper)
    project_in(1)
    with jax.named_scope("far_u"):
        far_in(upper)
    with jax.named_scope("last_in_l"):
        for q in (0, 2, 1):
            last_in(q, lower)
    project_in(2)
    with jax.named_scope("last_in_l3"):
        last_in(3, lower)
    project_in(3)
    with jax.named_scope("relay_u0"):
        relay(0, upper)
    project_in(4)
    with jax.named_scope("relay_u21"):
        relay(2, upper)
        relay(1, upper)
    project_in(5)
    with jax.named_scope("start_w"):
        start_w()
    project_in(6, 7)
    with jax.named_scope("pair_in_l"):
        pair_in(lower)

    scale = LOG2E / math.sqrt(NOPE + ROPE)
    tile_rows = HEADS * HALF
    reach = BLOCK // 128

    def attend(half, hooks):
        where = shard[half]
        blocks = where // reach
        m_ref[...] = jnp.full_like(m_ref, -1e30)
        l_ref[...] = jnp.zeros_like(l_ref)
        acc_ref[...] = jnp.zeros_like(acc_ref)

        def step(b, causal):
            block = keys[pl.ds(b * reach, reach)].reshape(BLOCK, WIDE)
            scores = lax.dot_general(
                qs[half].reshape(tile_rows, WIDE),
                block,
                (((1,), (1,)), ((), ())),
                preferred_element_type=jnp.float32,
            )
            scores = scores * scale + bias[pl.ds(b, 1), :]
            if causal is not None:
                scores = (scores.reshape(HEADS, HALF, BLOCK) + causal[None]).reshape(
                    tile_rows, BLOCK
                )
            before = m_ref[...]
            m_new = jnp.maximum(before, jnp.max(scores, axis=1, keepdims=True))
            alpha = jnp.exp2(before - m_new)
            lifted = jnp.exp2(scores - jnp.concatenate([m_new] * (BLOCK // 128), axis=1))
            total = l_ref[...] * alpha
            for k in range(BLOCK // 128):
                total = total + lifted[:, k * 128 : (k + 1) * 128]
            l_ref[...] = total
            m_ref[...] = m_new
            acc_ref[...] = acc_ref[...] * jnp.concatenate([alpha] * (KVR // 128), axis=1) + jnp.dot(
                lifted.astype(jnp.bfloat16), block[:, :KVR], preferred_element_type=jnp.float32
            )

        def open_step(b, carry):
            hooks(b, blocks)
            step(b, None)
            return carry

        lax.fori_loop(0, blocks, open_step, 0)
        hooks(blocks, blocks)
        token = where * 128 + xh * HALF + lax.broadcasted_iota(jnp.int32, (HALF, BLOCK), 0)
        position = blocks * BLOCK + lax.broadcasted_iota(jnp.int32, (HALF, BLOCK), 1)
        step(blocks, jnp.where(position <= token, 0.0, -1e30))
        total = jnp.sum(l_ref[...], axis=1, keepdims=True)
        ctx[...] = (acc_ref[...] / total).astype(jnp.bfloat16).reshape(HEADS, HALF, KVR)

    here = xh * 4 + z

    def values(half):
        for h in range(HEADS):
            w_value = wkv[:, h * 256 + NOPE : (h + 1) * 256]
            attended = jnp.dot(ctx[h], w_value, preferred_element_type=jnp.float32).astype(
                jnp.bfloat16
            )
            for r in range(2):
                for to in range(2):
                    at = to * 2 * ROWS + r * ROWS
                    astage[2 * half + r, to, :, h * VD : (h + 1) * VD] = attended[at : at + ROWS]
        for g in (2 * half, 2 * half + 1):
            pair_copy(g).start()
            ag[here, g, c] = astage[g, c]

    def a_copy(g, number, t, o, device, which=None):
        slot = (xh + t - 2 * xh * t) * 4 + lax.rem(z + o + 4, 4)
        ref = ag.at[slot, g]
        if which is not None:
            ref = ref.at[which]
        return copy(ref, ref, ABASE + ASTRIDE * g + number, device)

    def pair_copy(g):
        return copy(
            astage.at[g, 1 - c], ag.at[here, g, c], ABASE + ASTRIDE * g + APAIR, partner
        )

    def pair_copy_in(g):
        ref = ag.at[here, g, 1 - c]
        return copy(ref, ref, ABASE + ASTRIDE * g + APAIR, partner)

    def stage1(g):
        pair_copy_in(g).wait_recv()
        a_copy(g, AX, 0, 0, across).start()
        a_copy(g, AZ, 0, 0, up_z).start()
        a_copy(g, AZ + 1, 0, 0, down_z).start()

    def stage2(g):
        a_copy(g, AZ, 0, -1, up_z).wait_recv()
        a_copy(g, AZH, 0, -1, up_z, 0).start()
        a_copy(g, AZ + 1, 0, 1, down_z).wait_recv()
        a_copy(g, AZH + 1, 0, 1, down_z, 1).start()

    def stage3(g):
        a_copy(g, AX, 1, 0, across).wait_recv()
        a_copy(g, AZ + 2, 1, 0, up_z).start()
        a_copy(g, AZ + 3, 1, 0, down_z).start()

    def stage4(g):
        a_copy(g, AZH, 0, 2, up_z, 0).wait_recv()
        a_copy(g, AZH + 1, 0, 2, down_z, 1).wait_recv()
        a_copy(g, AX2, 0, 2, across).start()

    def stage5(g):
        a_copy(g, AZ + 2, 1, -1, up_z).wait_recv()
        a_copy(g, AZ + 3, 1, 1, down_z).wait_recv()
        a_copy(g, AX2, 1, 2, across).wait_recv()

    def w_relay(which):
        if which == 0:
            w_copy(WFULL, lax.rem(y + 3, 4), up_y, 0).wait_recv()
            w_copy(WHALF, lax.rem(y + 3, 4), up_y, 0).start()
        else:
            w_copy(WFULL + 3, lax.rem(y + 1, 4), down_y, 1).wait_recv()
            w_copy(WHALF + 1, lax.rem(y + 1, 4), down_y, 1).start()

    def w_middle():
        w_copy(WFULL + 1, lax.rem(y + 3, 4), up_y, 1).wait_recv()
        w_pair(lax.rem(y + 3, 4), 1).start()
        w_copy(WFULL + 2, lax.rem(y + 1, 4), down_y, 0).wait_recv()
        w_pair(lax.rem(y + 1, 4), 2).start()

    def w_last():
        w_copy(WHALF, lax.rem(y + 2, 4), up_y, 0).wait_recv()
        w_copy(WHALF + 1, lax.rem(y + 2, 4), down_y, 1).wait_recv()
        w_pair(lax.rem(y + 2, 4), 3).start()

    def w_all():
        for k, o in enumerate((0, 3, 1, 2)):
            w_pair_in(lax.rem(y + o, 4), k).wait_recv()

    def product(first, count):
        rows = 8 * count * ROWS
        total = jnp.zeros((rows, 4 * 224), jnp.float32)
        for core in range(2):
            total = total + lax.dot_general(
                ag[:, first : first + count, core].reshape(rows, HEADS * VD),
                wg[core].reshape(4 * 224, HEADS * VD),
                (((1,), (1,)), ((), ())),
                preferred_element_type=jnp.float32,
            )
        total = total.reshape(8, count * ROWS, 4 * 224)
        for n in range(count):
            part[first + n] = total[:, n * ROWS : (n + 1) * ROWS]

    def slots(half, k):
        straight, mirrored = k, 3 - k
        first = straight if half == 0 else mirrored
        return first, 4 + 3 - first

    def half_out(g):
        for k in range(2):
            low, high = slots(g // 2, 2 * (1 - xl) + k)
            outgoing[g, 0, k, 0] = part[g, low].astype(jnp.bfloat16)
            outgoing[g, 0, k, 1] = part[g, high].astype(jnp.bfloat16)
            copy(outgoing.at[g, 0, k], summand.at[g, k], XSUM + 2 * g + k, beside).start()

    def whole_out(g):
        half = g // 2
        number = lax.rem(z, 2) + 2 * c + 4 * (g % 2)
        for k in range(2):
            row = 2 * xl + k
            copy(outgoing.at[g, 0, k], summand.at[g, k], XSUM + 2 * g + k, beside).wait_recv()
            low, high = slots(half, row)
            for xs, at in enumerate((low, high)):
                outgoing[g, 1, k, xs] = (
                    part[g, at] + summand[g, k, xs].astype(jnp.float32)
                ).astype(jnp.bfloat16)
            own = (mine == 1) & (xh == half) & (z == row)
            target = out_ref.at[:, 2 * c + g % 2, :, pl.ds(lax.rem(z, 2) * 896, 896)]

            @pl.when(jnp.logical_not(own))
            def _():
                copy(
                    outgoing.at[g, 1, k], target, OUT + number, owners[half][k], OUT + 2 * g + k
                ).start()

            @pl.when(own)
            def _():
                pltpu.make_async_copy(
                    outgoing.at[g, 1, k], target, local_sem.at[10 + g % 2]
                ).start()

    def early_hooks(b, blocks):
        @pl.when(b == jnp.minimum(1, blocks))
        def _():
            with jax.named_scope("relay_u3"):
                relay(3, upper)

    def late_hooks(b, blocks):
        @pl.when(b == 0)
        def _():
            with jax.named_scope("last_in_u"):
                for q in (0, 2, 1, 3):
                    last_in(q, upper)

        @pl.when(b == 1)
        def _():
            with jax.named_scope("stage1_01"):
                stage1(0)
                stage1(1)

        @pl.when(b == 4)
        def _():
            with jax.named_scope("pair_in_u"):
                pair_in(upper)

        @pl.when(b == blocks)
        def _():
            with jax.named_scope("stage23_0"):
                stage2(0)
                stage3(0)
                w_relay(0)
                w_relay(1)

    with jax.named_scope("attend_low"):
        attend(0, early_hooks)
    with jax.named_scope("values"):
        values(0)
    with jax.named_scope("attend_high"):
        attend(1, late_hooks)
    with jax.named_scope("values"):
        values(1)
    with jax.named_scope("stage23_1"):
        stage2(1)
        stage3(1)
    with jax.named_scope("stage4_0"):
        stage4(0)
    with jax.named_scope("stage4_1"):
        stage4(1)
    with jax.named_scope("stage1_23"):
        stage1(2)
        stage1(3)
    with jax.named_scope("w_middle"):
        w_middle()
    with jax.named_scope("stage5_0"):
        stage5(0)
    with jax.named_scope("stage5_1"):
        stage5(1)
    with jax.named_scope("stage23_2"):
        stage2(2)
        stage3(2)
    with jax.named_scope("w_last"):
        w_last()
    with jax.named_scope("stage23_3"):
        stage2(3)
        stage3(3)
    with jax.named_scope("w_all"):
        w_all()
    with jax.named_scope("stage4_2"):
        stage4(2)
    with jax.named_scope("product_low"):
        product(0, 2)
    with jax.named_scope("half_out_low"):
        half_out(0)
        half_out(1)
    with jax.named_scope("stage4_3"):
        stage4(3)
    with jax.named_scope("whole_out_low"):
        whole_out(0)
        whole_out(1)
    with jax.named_scope("stage5_2"):
        stage5(2)
    with jax.named_scope("stage5_3"):
        stage5(3)
    with jax.named_scope("product_high"):
        product(2, 2)
    with jax.named_scope("half_out_high"):
        half_out(2)
        half_out(3)
    with jax.named_scope("whole_out_high"):
        whole_out(2)
        whole_out(3)

    with jax.named_scope("finish"):
        for n in range(8):
            r, k = n // 4, n % 4
            piece = out_ref.at[:, 2 * (k // 2) + r, :, (k % 2) * 896 : (k % 2 + 1) * 896]
            self_made = (mine == 1) & (makers[k][1] == z) & (k // 2 == c)

            @pl.when(jnp.logical_not(self_made))
            def _(n=n, piece=piece):
                copy(piece, piece, OUT + n, partner).wait_recv()

            @pl.when(self_made)
            def _(r=r, piece=piece):
                pltpu.make_async_copy(outgoing.at[0, 1, 0], piece, local_sem.at[10 + r]).wait()

    with jax.named_scope("drain"):
        full = keys.at[0, 0]
        part_key = keys.at[0, 0, pl.ds(0, 32)]

        def sent(ref, number):
            copy(ref, ref, number, partner).wait_send()

        def drain(ref, first, count):
            def one(n, carry):
                sent(ref, first + n)
                return carry

            lax.fori_loop(0, count, one, 0)

        sent(full, CROSS)
        sent(qx.at[0, 0], SWAP)
        sent(qx.at[0, 0], SWAP2)
        drain(full, D1, 4)
        drain(full, D1H, 2)
        drain(full, D2, 16)
        drain(part_key, D2H, 16)
        drain(full, PAIR, 32)
        drain(wg.at[0, 0, pl.ds(0, span)], WFULL, 4)
        drain(wg.at[0, 0, pl.ds(0, span)], WHALF, 2)
        drain(wg.at[0, 0], WPAIR, 4)
        for g in range(CHUNKS):
            at = ABASE + ASTRIDE * g
            sent(astage.at[g, 0], at + APAIR)
            sent(ag.at[0, 0], at + AX)
            drain(ag.at[0, 0], at + AZ, 4)
            drain(ag.at[0, 0, 0], at + AZH, 2)
            sent(ag.at[0, 0], at + AX2)
        drain(summand.at[0, 0], XSUM, 8)
        for g in range(CHUNKS):
            for k in range(2):
                own = (mine == 1) & (xh == g // 2) & (z == 2 * xl + k)

                @pl.when(jnp.logical_not(own))
                def _(g=g, k=k):
                    sent(summand.at[0, 0], OUT + 2 * g + k)


def local(q_latent, kv_latent, kv_gain, w_q_b, w_kv_b, w_o, prompt_len, response_mask):
    frequency = 10000.0 ** (-np.arange(ROPE // 2, dtype=np.float64) * 2.0 / ROPE)
    fine = np.arange(HALF, dtype=np.float64)[:, None] * np.tile(frequency, 2)[None, :]
    table = np.stack([np.cos(fine), np.sin(fine), np.cos(HALF * fine), np.sin(HALF * fine)])
    hbm = pl.BlockSpec(memory_space=pltpu.HBM)
    bf16 = jnp.bfloat16
    depth = HEADS * VD
    result = pl.pallas_call(
        body,
        out_shape=jax.ShapeDtypeStruct((2, 4, ROWS, 1792), bf16),
        in_specs=[hbm] * 5 + [pl.BlockSpec(memory_space=pltpu.SMEM)] + [hbm] * 3,
        out_specs=hbm,
        scratch_shapes=[
            pltpu.SemaphoreType.DMA((NSEM,)),
            pltpu.SemaphoreType.DMA((NSEM,)),
            pltpu.SemaphoreType.DMA((17,)),
            pltpu.VMEM((WIDE, 128), bf16),
            pltpu.VMEM((1, KVR), jnp.float32),
            pltpu.VMEM((4, HALF, ROPE), jnp.float32),
            pltpu.VMEM((32, 128), jnp.int32),
            pltpu.VMEM((2, 2, HALF // 2, 1536), bf16),
            pltpu.VMEM((8, 1536, 384), bf16),
            pltpu.VMEM((512, 4096), bf16),
            pltpu.VMEM((32, 2, HALF, WIDE), bf16),
            pltpu.VMEM((2, HEADS, HALF, WIDE), bf16),
            pltpu.VMEM((HEADS, HALF, KVR), bf16),
            pltpu.VMEM((CHUNKS, 2, ROWS, depth), bf16),
            pltpu.VMEM((8, CHUNKS, 2, ROWS, depth), bf16),
            pltpu.VMEM((2, 4, 224, 2048), bf16),
            pltpu.VMEM((CHUNKS, 8, ROWS, 4 * 224), jnp.float32),
            pltpu.VMEM((CHUNKS, 2, 2, 2, ROWS, 4 * 224), bf16),
            pltpu.VMEM((CHUNKS, 2, 2, ROWS, 4 * 224), bf16),
            pltpu.VMEM((4096 // BLOCK, BLOCK), jnp.float32),
            pltpu.VMEM((HEADS * HALF, 128), jnp.float32),
            pltpu.VMEM((HEADS * HALF, 128), jnp.float32),
            pltpu.VMEM((HEADS * HALF, KVR), jnp.float32),
        ],
        compiler_params=pltpu.CompilerParams(
            collective_id=0, has_side_effects=True, vmem_limit_bytes=67000000
        ),
        cost_estimate=pl.CostEstimate(
            flops=20_000_000_000, bytes_accessed=16_000_000, transcendentals=0
        ),
        name="layer",
    )(
        q_latent.reshape(2, 2, HALF // 2, 1536),
        kv_latent.T,
        kv_gain.reshape(1, -1),
        jnp.asarray(table, jnp.float32),
        response_mask.reshape(32, 128),
        prompt_len,
        w_q_b,
        w_kv_b,
        w_o.T,
    )
    return result.reshape(128, 1792)


def solution(mesh):
    finer = Mesh(mesh.devices.reshape(2, 4, 4, 2, 2), AXES)
    placed = (
        P(DP, None),
        P(DP, None),
        P(),
        P(None, HEAD),
        P(None, HEAD),
        P(HEAD, DP),
        P(),
        P(),
    )
    return jax.shard_map(
        local, mesh=finer, in_specs=placed, out_specs=P(DP, HEAD), check_vma=False
    )
```

```python
import functools
import math

import jax
import jax.numpy as jnp
import numpy as np
from jax import lax
from jax.experimental import pallas as pl
from jax.experimental.pallas import tpu as pltpu
from jax.sharding import Mesh
from jax.sharding import PartitionSpec as P

KVR = 512
ROPE = 64
NOPE = 128
VD = 128
WIDE = KVR + ROPE
AXES = ("xh", "z", "y", "xl", "c")
DP = ("xh", "z", "y")
HEAD = ("xl", "c")
MESH = pl.DeviceIdType.MESH

HEADS = 16
CHUNKS = 4
HALF = 64
ROWS = 16
BLOCK = 512
LOG2E = 1.4426950408889634
EPS = 1e-06

CROSS = 0
SWAP = 1
D1 = 2
D1H = 6
SWAP2 = 8
D2 = 10
D2H = 26
PAIR = 42
WFULL = 74
WHALF = 78
WPAIR = 80
ABASE = 84
APAIR, AX, AZ, AZH, AX2 = 0, 1, 2, 6, 8
ASTRIDE = 10
OUT = ABASE + ASTRIDE * CHUNKS
XSUM = OUT + 8
NSEM = XSUM + 8


def turn(values, cosine, sine):
    swapped = jnp.concatenate([values[:, ROPE // 2 :], values[:, : ROPE // 2]], axis=1)
    return values * cosine + swapped * sine


def body(
    q_hbm,
    kv_hbm,
    gain_hbm,
    table_hbm,
    live_hbm,
    prompt,
    wq_hbm,
    wkv_hbm,
    wo_hbm,
    out_ref,
    out_sem,
    in_sem,
    local_sem,
    kv_lat,
    gain,
    table,
    live,
    qx,
    wq,
    wkv,
    keys,
    qs,
    ctx,
    astage,
    ag,
    wg,
    part,
    outgoing,
    summand,
    bias,
    m_ref,
    l_ref,
    acc_ref,
):
    xh, z, y, xl, c = (lax.axis_index(a) for a in AXES)
    d1 = y + c * (z - y)
    d2 = z + c * (y - z)

    def place(t, o1, o2):
        a = lax.rem(d1 + o1 + 4, 4)
        b = lax.rem(d2 + o2 + 4, 4)
        zz = b + c * (a - b)
        yy = a + c * (b - a)
        xx = xh + t - 2 * xh * t
        return xx, zz, yy

    def unit(t, o1, o2):
        xx, zz, yy = place(t, o1, o2)
        return xx * 16 + zz * 4 + yy

    def near(o1, o2):
        _, zz, yy = place(0, o1, o2)
        return (xh, zz, yy, xl, c)

    def copy(src, dst, number, device, leaving=None):
        return pltpu.make_async_remote_copy(
            src_ref=src,
            dst_ref=dst,
            send_sem=out_sem.at[number if leaving is None else leaving],
            recv_sem=in_sem.at[number],
            device_id=device,
            device_id_type=MESH,
        )

    me = unit(0, 0, 0)
    partner = (xh, z, y, xl, 1 - c)
    cross = (1 - xh, z, y, 1 - xl, c)
    swap_peer = (1 - xh, 3 - z, y, 1 - xl, c)
    across = (1 - xh, z, y, xl, c)
    up_y = (xh, z, lax.rem(y + 1, 4), xl, c)
    down_y = (xh, z, lax.rem(y + 3, 4), xl, c)
    up_z = (xh, lax.rem(z + 1, 4), y, xl, c)
    down_z = (xh, lax.rem(z + 3, 4), y, xl, c)
    owners = [[(t, 2 * xl + k, y, xh, z // 2) for k in range(2)] for t in range(2)]
    makers = [(xl, 2 * c + k % 2, y, z // 2, k // 2) for k in range(4)]
    beside = (xh, z, y, 1 - xl, c)
    same = lambda u, v: 1 - jnp.minimum((u - v) * (u - v), 1)
    mine = same(c, xh) * same(xl, xh) * same(z // 2, c)
    z_low = z + xh * (3 - 2 * z)
    shard = (z_low * 4 + y, 16 + (3 - z_low) * 4 + y)

    barrier = pltpu.get_barrier_semaphore()
    far = near(2, 0)
    for peer in (partner, cross, swap_peer, across, beside, far, up_y, down_y, up_z, down_z):
        pl.semaphore_signal(barrier, inc=1, device_id=peer, device_id_type=MESH)
    for k in range(4):

        @pl.when((mine == 0) | (makers[k][1] != z) | (k // 2 != c))
        def _(k=k):
            pl.semaphore_signal(barrier, inc=1, device_id=makers[k], device_id_type=MESH)

    inputs = ((kv_hbm, kv_lat), (gain_hbm, gain), (table_hbm, table), (live_hbm, live))
    for n, (far_away, close) in enumerate(inputs):
        pltpu.make_async_copy(far_away, close, local_sem.at[12 + n]).start()
    own_rows = pltpu.make_async_copy(q_hbm.at[xh], qx.at[xh], local_sem.at[16])
    own_rows.start()
    pltpu.make_async_copy(wkv_hbm, wkv, local_sem.at[8]).start()
    for j in range(8):
        pltpu.make_async_copy(wq_hbm.at[:, pl.ds(j * 384, 384)], wq.at[j], local_sem.at[j]).start()
    pltpu.make_async_copy(wo_hbm, wg.at[c, y], local_sem.at[9]).start()

    with jax.named_scope("norm"):
        for n, (far_away, close) in enumerate(inputs):
            pltpu.make_async_copy(far_away, close, local_sem.at[12 + n]).wait()
        lane = lax.broadcasted_iota(jnp.int32, (1, ROPE), 1)
        sign = jnp.where(lane < ROPE // 2, -1.0, 1.0)

        def angles(m):
            cos_a, sin_a = table[2, pl.ds(m, 1), :], table[3, pl.ds(m, 1), :]
            cos_b, sin_b = table[0], table[1]
            return cos_a * cos_b - sin_a * sin_b, (sin_a * cos_b + cos_a * sin_b) * sign

        turned_rows = kv_lat[...].astype(jnp.float32).T
        rows = jnp.where(c == 0, turned_rows[:HALF], turned_rows[HALF:])
        latent = rows[:, :KVR]
        inverse = lax.rsqrt(jnp.mean(latent * latent, axis=-1, keepdims=True) + EPS)
        keys[me, c, :, :KVR] = (latent * inverse * gain[...]).astype(jnp.bfloat16)
        keys[me, c, :, KVR:] = turn(rows[:, KVR:], *angles(me * 2 + c)).astype(jnp.bfloat16)
        spot = lax.broadcasted_iota(jnp.int32, (32, 128), 0) * 128 + lax.broadcasted_iota(
            jnp.int32, (32, 128), 1
        )
        usable = (spot < prompt[0]) | (live[...] == 1)
        masked = jnp.where(usable, 0.0, -1e30)
        for r in range(32):
            b, at = r // (BLOCK // 128), r % (BLOCK // 128)
            bias[b : b + 1, at * 128 : (at + 1) * 128] = masked[r : r + 1]

    with jax.named_scope("barrier"):
        pl.semaphore_wait(barrier, 14 - mine)

    def key(t, o1, o2, which=None):
        ref = keys.at[unit(t, o1, o2), c]
        if which is None:
            return ref
        return ref.at[pl.ds(32 * which, 32)]

    def key_copy(number, t, o1, o2, device, which=None):
        ref = key(t, o1, o2, which)
        return copy(ref, ref, number, device)

    offsets = (0, 1, 3, 2)
    lower, upper = xh, 1 - xh

    def spread(q, t):
        k, o = 2 * q + t, offsets[q]
        key_copy(D2 + 2 * k, t, o, 0, near(0, 1)).start()
        key_copy(D2 + 2 * k + 1, t, o, 0, near(0, -1)).start()
        key_copy(PAIR + k, t, o, 0, partner).start()

    def first_out(t):
        key_copy(D1 + 2 * t, t, 0, 0, near(1, 0)).start()
        key_copy(D1 + 2 * t + 1, t, 0, 0, near(-1, 0)).start()
        spread(0, t)
        key_copy(D1H + t, t, 0, 0, far).start()

    def first_in(t):
        key_copy(D1 + 2 * t, t, -1, 0, near(1, 0)).wait_recv()
        spread(2, t)
        key_copy(D1 + 2 * t + 1, t, 1, 0, near(-1, 0)).wait_recv()
        spread(1, t)

    def far_in(t):
        key_copy(D1H + t, t, 2, 0, far).wait_recv()
        spread(3, t)

    def cross_in():
        key_copy(CROSS, 1, 0, 0, cross).wait_recv()

    with jax.named_scope("spread"):
        key_copy(CROSS, 0, 0, 0, cross).start()
        copy(q_hbm.at[1 - xh, c], qx.at[xh, c], SWAP, swap_peer).start()
        pl.when(xh == 1)(cross_in)
        first_out(lower)
        pl.when(xh == 0)(cross_in)
        first_out(upper)

    tables = [angles(2 * where + xh) for where in shard]

    def project(j):
        pltpu.make_async_copy(
            wq_hbm.at[:, pl.ds(0, 384)], wq.at[j], local_sem.at[j]
        ).wait()
        both = jnp.dot(
            qx[...].reshape(2 * HALF, 1536), wq[j], preferred_element_type=jnp.float32
        ).astype(jnp.bfloat16)
        for e in range(2):
            h = 2 * j + e
            plain = both[:, e * 192 : e * 192 + NOPE]
            roped = both[:, e * 192 + NOPE : (e + 1) * 192].astype(jnp.float32)
            w_key = wkv[:, pl.ds(pl.multiple_of(h * 256, 256), NOPE)]
            absorbed = lax.dot_general(
                plain, w_key, (((1,), (1,)), ((), ())), preferred_element_type=jnp.float32
            ).astype(jnp.bfloat16)
            for half in range(2):
                mine_rows = slice(half * HALF, (half + 1) * HALF)
                qs[half, h, :, :KVR] = absorbed[mine_rows]
                qs[half, h, :, KVR:] = turn(roped[mine_rows], *tables[half]).astype(jnp.bfloat16)

    def relay(q, t):
        k, o = 2 * q + t, offsets[q]
        key_copy(D2 + 2 * k, t, o, -1, near(0, 1)).wait_recv()
        key_copy(D2H + 2 * k, t, o, -1, near(0, 1), 0).start()
        key_copy(PAIR + 8 + k, t, o, -1, partner).start()
        key_copy(D2 + 2 * k + 1, t, o, 1, near(0, -1)).wait_recv()
        key_copy(D2H + 2 * k + 1, t, o, 1, near(0, -1), 1).start()
        key_copy(PAIR + 16 + k, t, o, 1, partner).start()

    def last_in(q, t):
        k, o = 2 * q + t, offsets[q]
        key_copy(D2H + 2 * k, t, o, 2, near(0, 1), 0).wait_recv()
        key_copy(D2H + 2 * k + 1, t, o, 2, near(0, -1), 1).wait_recv()
        key_copy(PAIR + 24 + k, t, o, 2, partner).start()

    def pair_in(t):
        def one(n, carry):
            ref = keys.at[0, 1 - c]
            copy(ref, ref, PAIR + 2 * n + t, partner).wait_recv()
            return carry

        lax.fori_loop(0, 16, one, 0)

    span = wo_hbm.shape[0] // 2

    def w_copy(number, row, device, which):
        ref = wg.at[c, row, pl.ds(which * span, span)]
        return copy(ref, ref, number, device)

    def w_pair(row, number):
        return copy(wg.at[c, row], wg.at[c, row], WPAIR + number, partner)

    def w_pair_in(row, number):
        return copy(wg.at[1 - c, row], wg.at[1 - c, row], WPAIR + number, partner)

    def project_in(*order):
        with jax.named_scope("project"):
            for j in order:
                project(j)

    def start_w():
        pltpu.make_async_copy(wo_hbm, wg.at[c, y], local_sem.at[9]).wait()
        for which in range(2):
            w_copy(WFULL + which, y, up_y, which).start()
            w_copy(WFULL + 3 - which, y, down_y, 1 - which).start()
        w_pair(y, 0).start()

    with jax.named_scope("first_in_l"):
        first_in(lower)
    with jax.named_scope("relay_l0"):
        relay(0, lower)
    with jax.named_scope("far_l"):
        far_in(lower)
    with jax.named_scope("swap"):
        copy(qx.at[1 - xh, c], qx.at[1 - xh, c], SWAP, swap_peer).wait_recv()
        copy(qx.at[1 - xh, c], qx.at[1 - xh, c], SWAP2, partner).start()
    with jax.named_scope("relay_l21"):
        relay(2, lower)
        relay(1, lower)
    with jax.named_scope("swap2"):
        copy(qx.at[1 - xh, 1 - c], qx.at[1 - xh, 1 - c], SWAP2, partner).wait_recv()
        own_rows.wait()
        pltpu.make_async_copy(wkv_hbm, wkv, local_sem.at[8]).wait()
    project_in(0)
    with jax.named_scope("relay_l3"):
        relay(3, lower)
    with jax.named_scope("first_in_u"):
        first_in(upper)
    project_in(1)
    with jax.named_scope("far_u"):
        far_in(upper)
    with jax.named_scope("last_in_l"):
        for q in (0, 2, 1):
            last_in(q, lower)
    project_in(2)
    with jax.named_scope("last_in_l3"):
        last_in(3, lower)
    project_in(3)
    with jax.named_scope("relay_u0"):
        relay(0, upper)
    project_in(4)
    with jax.named_scope("relay_u21"):
        relay(2, upper)
        relay(1, upper)
    project_in(5, 6)
    with jax.named_scope("relay_u3"):
        relay(3, upper)
    with jax.named_scope("start_w"):
        start_w()
    project_in(7)
    with jax.named_scope("pair_in_l"):
        pair_in(lower)

    scale = LOG2E / math.sqrt(NOPE + ROPE)
    tile_rows = HEADS * HALF
    reach = BLOCK // 128

    def attend(half, hooks):
        where = shard[half]
        blocks = where // reach
        m_ref[...] = jnp.full_like(m_ref, -1e30)
        l_ref[...] = jnp.zeros_like(l_ref)
        acc_ref[...] = jnp.zeros_like(acc_ref)

        def step(b, causal):
            block = keys[pl.ds(b * reach, reach)].reshape(BLOCK, WIDE)
            scores = lax.dot_general(
                qs[half].reshape(tile_rows, WIDE),
                block,
                (((1,), (1,)), ((), ())),
                preferred_element_type=jnp.float32,
            )
            scores = scores * scale + bias[pl.ds(b, 1), :]
            if causal is not None:
                scores = (scores.reshape(HEADS, HALF, BLOCK) + causal[None]).reshape(
                    tile_rows, BLOCK
                )
            before = m_ref[...]
            m_new = jnp.maximum(before, jnp.max(scores, axis=1, keepdims=True))
            alpha = jnp.exp2(before - m_new)
            lifted = jnp.exp2(scores - jnp.concatenate([m_new] * (BLOCK // 128), axis=1))
            total = l_ref[...] * alpha
            for k in range(BLOCK // 128):
                total = total + lifted[:, k * 128 : (k + 1) * 128]
            l_ref[...] = total
            m_ref[...] = m_new
            acc_ref[...] = acc_ref[...] * jnp.concatenate([alpha] * (KVR // 128), axis=1) + jnp.dot(
                lifted.astype(jnp.bfloat16), block[:, :KVR], preferred_element_type=jnp.float32
            )

        def open_step(b, carry):
            hooks(b, blocks)
            step(b, None)
            return carry

        lax.fori_loop(0, blocks, open_step, 0)
        hooks(blocks, blocks)
        token = where * 128 + xh * HALF + lax.broadcasted_iota(jnp.int32, (HALF, BLOCK), 0)
        position = blocks * BLOCK + lax.broadcasted_iota(jnp.int32, (HALF, BLOCK), 1)
        step(blocks, jnp.where(position <= token, 0.0, -1e30))
        total = jnp.sum(l_ref[...], axis=1, keepdims=True)
        ctx[...] = (acc_ref[...] / total).astype(jnp.bfloat16).reshape(HEADS, HALF, KVR)

    here = xh * 4 + z

    def values(half):
        for h in range(HEADS):
            w_value = wkv[:, h * 256 + NOPE : (h + 1) * 256]
            attended = jnp.dot(ctx[h], w_value, preferred_element_type=jnp.float32).astype(
                jnp.bfloat16
            )
            for r in range(2):
                for to in range(2):
                    at = to * 2 * ROWS + r * ROWS
                    astage[2 * half + r, to, :, h * VD : (h + 1) * VD] = attended[at : at + ROWS]
        for g in (2 * half, 2 * half + 1):
            pair_copy(g).start()
            ag[here, g, c] = astage[g, c]

    def a_copy(g, number, t, o, device, which=None):
        slot = (xh + t - 2 * xh * t) * 4 + lax.rem(z + o + 4, 4)
        ref = ag.at[slot, g]
        if which is not None:
            ref = ref.at[which]
        return copy(ref, ref, ABASE + ASTRIDE * g + number, device)

    def pair_copy(g):
        return copy(
            astage.at[g, 1 - c], ag.at[here, g, c], ABASE + ASTRIDE * g + APAIR, partner
        )

    def pair_copy_in(g):
        ref = ag.at[here, g, 1 - c]
        return copy(ref, ref, ABASE + ASTRIDE * g + APAIR, partner)

    def stage1(g):
        pair_copy_in(g).wait_recv()
        a_copy(g, AX, 0, 0, across).start()
        a_copy(g, AZ, 0, 0, up_z).start()
        a_copy(g, AZ + 1, 0, 0, down_z).start()

    def stage2(g):
        a_copy(g, AZ, 0, -1, up_z).wait_recv()
        a_copy(g, AZH, 0, -1, up_z, 0).start()
        a_copy(g, AZ + 1, 0, 1, down_z).wait_recv()
        a_copy(g, AZH + 1, 0, 1, down_z, 1).start()

    def stage3(g):
        a_copy(g, AX, 1, 0, across).wait_recv()
        a_copy(g, AZ + 2, 1, 0, up_z).start()
        a_copy(g, AZ + 3, 1, 0, down_z).start()

    def stage4(g):
        a_copy(g, AZH, 0, 2, up_z, 0).wait_recv()
        a_copy(g, AZH + 1, 0, 2, down_z, 1).wait_recv()
        a_copy(g, AX2, 0, 2, across).start()

    def stage5(g):
        a_copy(g, AZ + 2, 1, -1, up_z).wait_recv()
        a_copy(g, AZ + 3, 1, 1, down_z).wait_recv()
        a_copy(g, AX2, 1, 2, across).wait_recv()

    def w_relay(which):
        if which == 0:
            w_copy(WFULL, lax.rem(y + 3, 4), up_y, 0).wait_recv()
            w_copy(WHALF, lax.rem(y + 3, 4), up_y, 0).start()
        else:
            w_copy(WFULL + 3, lax.rem(y + 1, 4), down_y, 1).wait_recv()
            w_copy(WHALF + 1, lax.rem(y + 1, 4), down_y, 1).start()

    def w_middle():
        w_copy(WFULL + 1, lax.rem(y + 3, 4), up_y, 1).wait_recv()
        w_pair(lax.rem(y + 3, 4), 1).start()
        w_copy(WFULL + 2, lax.rem(y + 1, 4), down_y, 0).wait_recv()
        w_pair(lax.rem(y + 1, 4), 2).start()

    def w_last():
        w_copy(WHALF, lax.rem(y + 2, 4), up_y, 0).wait_recv()
        w_copy(WHALF + 1, lax.rem(y + 2, 4), down_y, 1).wait_recv()
        w_pair(lax.rem(y + 2, 4), 3).start()

    def w_all():
        for k, o in enumerate((0, 3, 1, 2)):
            w_pair_in(lax.rem(y + o, 4), k).wait_recv()

    def product(first, count):
        rows = 8 * count * ROWS
        total = jnp.zeros((rows, 4 * 224), jnp.float32)
        for core in range(2):
            total = total + lax.dot_general(
                ag[:, first : first + count, core].reshape(rows, HEADS * VD),
                wg[core].reshape(4 * 224, HEADS * VD),
                (((1,), (1,)), ((), ())),
                preferred_element_type=jnp.float32,
            )
        total = total.reshape(8, count * ROWS, 4 * 224)
        for n in range(count):
            part[first + n] = total[:, n * ROWS : (n + 1) * ROWS]

    def slots(half, k):
        straight, mirrored = k, 3 - k
        first = straight if half == 0 else mirrored
        return first, 4 + 3 - first

    def half_out(g):
        for k in range(2):
            low, high = slots(g // 2, 2 * (1 - xl) + k)
            outgoing[g, 0, k, 0] = part[g, low].astype(jnp.bfloat16)
            outgoing[g, 0, k, 1] = part[g, high].astype(jnp.bfloat16)
            copy(outgoing.at[g, 0, k], summand.at[g, k], XSUM + 2 * g + k, beside).start()

    def whole_out(g):
        half = g // 2
        number = lax.rem(z, 2) + 2 * c + 4 * (g % 2)
        for k in range(2):
            row = 2 * xl + k
            copy(outgoing.at[g, 0, k], summand.at[g, k], XSUM + 2 * g + k, beside).wait_recv()
            low, high = slots(half, row)
            for xs, at in enumerate((low, high)):
                outgoing[g, 1, k, xs] = (
                    part[g, at] + summand[g, k, xs].astype(jnp.float32)
                ).astype(jnp.bfloat16)
            own = (mine == 1) & (xh == half) & (z == row)
            target = out_ref.at[:, 2 * c + g % 2, :, pl.ds(lax.rem(z, 2) * 896, 896)]

            @pl.when(jnp.logical_not(own))
            def _():
                copy(
                    outgoing.at[g, 1, k], target, OUT + number, owners[half][k], OUT + 2 * g + k
                ).start()

            @pl.when(own)
            def _():
                pltpu.make_async_copy(
                    outgoing.at[g, 1, k], target, local_sem.at[10 + g % 2]
                ).start()

    def early_hooks(b, blocks):
        @pl.when(b == jnp.minimum(1, blocks))
        def _():
            with jax.named_scope("last_in_u"):
                for q in (0, 2, 1):
                    last_in(q, upper)

    def late_hooks(b, blocks):
        @pl.when(b == 0)
        def _():
            with jax.named_scope("last_in_u3"):
                last_in(3, upper)

        @pl.when(b == 1)
        def _():
            with jax.named_scope("stage1_01"):
                stage1(0)
                stage1(1)

        @pl.when(b == 4)
        def _():
            with jax.named_scope("pair_in_u"):
                pair_in(upper)

        @pl.when(b == blocks)
        def _():
            with jax.named_scope("stage23_0"):
                stage2(0)
                stage3(0)
                w_relay(0)
                w_relay(1)

    with jax.named_scope("attend_low"):
        attend(0, early_hooks)
    with jax.named_scope("values"):
        values(0)
    with jax.named_scope("attend_high"):
        attend(1, late_hooks)
    with jax.named_scope("values"):
        values(1)
    with jax.named_scope("stage23_1"):
        stage2(1)
        stage3(1)
    with jax.named_scope("stage4_0"):
        stage4(0)
    with jax.named_scope("stage4_1"):
        stage4(1)
    with jax.named_scope("stage1_23"):
        stage1(2)
        stage1(3)
    with jax.named_scope("w_middle"):
        w_middle()
    with jax.named_scope("stage5_0"):
        stage5(0)
    with jax.named_scope("stage5_1"):
        stage5(1)
    with jax.named_scope("stage23_2"):
        stage2(2)
        stage3(2)
    with jax.named_scope("w_last"):
        w_last()
    with jax.named_scope("stage23_3"):
        stage2(3)
        stage3(3)
    with jax.named_scope("w_all"):
        w_all()
    with jax.named_scope("stage4_2"):
        stage4(2)
    with jax.named_scope("product_low"):
        product(0, 2)
    with jax.named_scope("half_out_low"):
        half_out(0)
        half_out(1)
    with jax.named_scope("stage4_3"):
        stage4(3)
    with jax.named_scope("whole_out_low"):
        whole_out(0)
        whole_out(1)
    with jax.named_scope("stage5_2"):
        stage5(2)
    with jax.named_scope("stage5_3"):
        stage5(3)
    with jax.named_scope("product_high"):
        product(2, 2)
    with jax.named_scope("half_out_high"):
        half_out(2)
        half_out(3)
    with jax.named_scope("whole_out_high"):
        whole_out(2)
        whole_out(3)

    with jax.named_scope("finish"):
        for n in range(8):
            r, k = n // 4, n % 4
            piece = out_ref.at[:, 2 * (k // 2) + r, :, (k % 2) * 896 : (k % 2 + 1) * 896]
            self_made = (mine == 1) & (makers[k][1] == z) & (k // 2 == c)

            @pl.when(jnp.logical_not(self_made))
            def _(n=n, piece=piece):
                copy(piece, piece, OUT + n, partner).wait_recv()

            @pl.when(self_made)
            def _(r=r, piece=piece):
                pltpu.make_async_copy(outgoing.at[0, 1, 0], piece, local_sem.at[10 + r]).wait()

    with jax.named_scope("drain"):
        full = keys.at[0, 0]
        part_key = keys.at[0, 0, pl.ds(0, 32)]

        def sent(ref, number):
            copy(ref, ref, number, partner).wait_send()

        def drain(ref, first, count):
            def one(n, carry):
                sent(ref, first + n)
                return carry

            lax.fori_loop(0, count, one, 0)

        sent(full, CROSS)
        sent(qx.at[0, 0], SWAP)
        sent(qx.at[0, 0], SWAP2)
        drain(full, D1, 4)
        drain(full, D1H, 2)
        drain(full, D2, 16)
        drain(part_key, D2H, 16)
        drain(full, PAIR, 32)
        drain(wg.at[0, 0, pl.ds(0, span)], WFULL, 4)
        drain(wg.at[0, 0, pl.ds(0, span)], WHALF, 2)
        drain(wg.at[0, 0], WPAIR, 4)
        for g in range(CHUNKS):
            at = ABASE + ASTRIDE * g
            sent(astage.at[g, 0], at + APAIR)
            sent(ag.at[0, 0], at + AX)
            drain(ag.at[0, 0], at + AZ, 4)
            drain(ag.at[0, 0, 0], at + AZH, 2)
            sent(ag.at[0, 0], at + AX2)
        drain(summand.at[0, 0], XSUM, 8)
        for g in range(CHUNKS):
            for k in range(2):
                own = (mine == 1) & (xh == g // 2) & (z == 2 * xl + k)

                @pl.when(jnp.logical_not(own))
                def _(g=g, k=k):
                    sent(summand.at[0, 0], OUT + 2 * g + k)


def local(q_latent, kv_latent, kv_gain, w_q_b, w_kv_b, w_o, prompt_len, response_mask):
    frequency = 10000.0 ** (-np.arange(ROPE // 2, dtype=np.float64) * 2.0 / ROPE)
    fine = np.arange(HALF, dtype=np.float64)[:, None] * np.tile(frequency, 2)[None, :]
    table = np.stack([np.cos(fine), np.sin(fine), np.cos(HALF * fine), np.sin(HALF * fine)])
    hbm = pl.BlockSpec(memory_space=pltpu.HBM)
    bf16 = jnp.bfloat16
    depth = HEADS * VD
    result = pl.pallas_call(
        body,
        out_shape=jax.ShapeDtypeStruct((2, 4, ROWS, 1792), bf16),
        in_specs=[hbm] * 5 + [pl.BlockSpec(memory_space=pltpu.SMEM)] + [hbm] * 3,
        out_specs=hbm,
        scratch_shapes=[
            pltpu.SemaphoreType.DMA((NSEM,)),
            pltpu.SemaphoreType.DMA((NSEM,)),
            pltpu.SemaphoreType.DMA((17,)),
            pltpu.VMEM((WIDE, 128), bf16),
            pltpu.VMEM((1, KVR), jnp.float32),
            pltpu.VMEM((4, HALF, ROPE), jnp.float32),
            pltpu.VMEM((32, 128), jnp.int32),
            pltpu.VMEM((2, 2, HALF // 2, 1536), bf16),
            pltpu.VMEM((8, 1536, 384), bf16),
            pltpu.VMEM((512, 4096), bf16),
            pltpu.VMEM((32, 2, HALF, WIDE), bf16),
            pltpu.VMEM((2, HEADS, HALF, WIDE), bf16),
            pltpu.VMEM((HEADS, HALF, KVR), bf16),
            pltpu.VMEM((CHUNKS, 2, ROWS, depth), bf16),
            pltpu.VMEM((8, CHUNKS, 2, ROWS, depth), bf16),
            pltpu.VMEM((2, 4, 224, 2048), bf16),
            pltpu.VMEM((CHUNKS, 8, ROWS, 4 * 224), jnp.float32),
            pltpu.VMEM((CHUNKS, 2, 2, 2, ROWS, 4 * 224), bf16),
            pltpu.VMEM((CHUNKS, 2, 2, ROWS, 4 * 224), bf16),
            pltpu.VMEM((4096 // BLOCK, BLOCK), jnp.float32),
            pltpu.VMEM((HEADS * HALF, 128), jnp.float32),
            pltpu.VMEM((HEADS * HALF, 128), jnp.float32),
            pltpu.VMEM((HEADS * HALF, KVR), jnp.float32),
        ],
        compiler_params=pltpu.CompilerParams(
            collective_id=0, has_side_effects=True, vmem_limit_bytes=67000000
        ),
        cost_estimate=pl.CostEstimate(
            flops=20_000_000_000, bytes_accessed=16_000_000, transcendentals=0
        ),
        name="layer",
    )(
        q_latent.reshape(2, 2, HALF // 2, 1536),
        kv_latent.T,
        kv_gain.reshape(1, -1),
        jnp.asarray(table, jnp.float32),
        response_mask.reshape(32, 128),
        prompt_len,
        w_q_b,
        w_kv_b,
        w_o.T,
    )
    return result.reshape(128, 1792)


def solution(mesh):
    finer = Mesh(mesh.devices.reshape(2, 4, 4, 2, 2), AXES)
    placed = (
        P(DP, None),
        P(DP, None),
        P(),
        P(None, HEAD),
        P(None, HEAD),
        P(HEAD, DP),
        P(),
        P(),
    )
    return jax.shard_map(
        local, mesh=finer, in_specs=placed, out_specs=P(DP, HEAD), check_vma=False
    )
```

```python
import functools
import math

import jax
import jax.numpy as jnp
import numpy as np
from jax import lax
from jax.experimental import pallas as pl
from jax.experimental.pallas import tpu as pltpu
from jax.sharding import Mesh
from jax.sharding import PartitionSpec as P

KVR = 512
ROPE = 64
NOPE = 128
VD = 128
WIDE = KVR + ROPE
AXES = ("xh", "z", "y", "xl", "c")
DP = ("xh", "z", "y")
HEAD = ("xl", "c")
MESH = pl.DeviceIdType.MESH

HEADS = 16
CHUNKS = 4
HALF = 64
ROWS = 16
BLOCK = 512
LOG2E = 1.4426950408889634
EPS = 1e-06

CROSS = 0
SWAP = 1
SWAP2 = 2
D1 = 3
FAR = 7
D2 = 9
D2H = 25
PAIR = 33
WFULL = 35
WHALF = 39
WPAIR = 40
ABASE = 44
APAIR, AX, AZ, AZH, AX2 = 0, 1, 2, 6, 7
ASTRIDE = 8
OUT = ABASE + ASTRIDE * CHUNKS
XSUM = OUT + 8
NSEM = XSUM + 8


def turn(values, cosine, sine):
    swapped = jnp.concatenate([values[:, ROPE // 2 :], values[:, : ROPE // 2]], axis=1)
    return values * cosine + swapped * sine


def body(
    q_hbm,
    kv_hbm,
    gain_hbm,
    table_hbm,
    live_hbm,
    prompt,
    wq_hbm,
    wkv_hbm,
    wo_hbm,
    out_ref,
    out_sem,
    in_sem,
    local_sem,
    kv_lat,
    gain,
    table,
    live,
    qx,
    wq,
    wkv,
    keys,
    qs,
    ctx,
    astage,
    ag,
    wg,
    part,
    outgoing,
    summand,
    bias,
    m_ref,
    l_ref,
    acc_ref,
):
    xh, z, y, xl, c = (lax.axis_index(a) for a in AXES)
    d1 = y + c * (z - y)
    d2 = z + c * (y - z)

    def place(t, o1, o2):
        a = lax.rem(d1 + o1 + 4, 4)
        b = lax.rem(d2 + o2 + 4, 4)
        zz = b + c * (a - b)
        yy = a + c * (b - a)
        xx = xh + t - 2 * xh * t
        return xx, zz, yy

    def unit(t, o1, o2):
        xx, zz, yy = place(t, o1, o2)
        return xx * 16 + zz * 4 + yy

    def near(o1, o2):
        _, zz, yy = place(0, o1, o2)
        return (xh, zz, yy, xl, c)

    def copy(src, dst, number, device, leaving=None):
        return pltpu.make_async_remote_copy(
            src_ref=src,
            dst_ref=dst,
            send_sem=out_sem.at[number if leaving is None else leaving],
            recv_sem=in_sem.at[number],
            device_id=device,
            device_id_type=MESH,
        )

    me = unit(0, 0, 0)
    partner = (xh, z, y, xl, 1 - c)
    cross = (1 - xh, z, y, 1 - xl, c)
    swap_peer = (1 - xh, 3 - z, y, 1 - xl, c)
    across = (1 - xh, z, y, xl, c)
    up_y = (xh, z, lax.rem(y + 1, 4), xl, c)
    down_y = (xh, z, lax.rem(y + 3, 4), xl, c)
    up_z = (xh, lax.rem(z + 1, 4), y, xl, c)
    down_z = (xh, lax.rem(z + 3, 4), y, xl, c)
    owners = [[(t, 2 * xl + k, y, xh, z // 2) for k in range(2)] for t in range(2)]
    makers = [(xl, 2 * c + k % 2, y, z // 2, k // 2) for k in range(4)]
    beside = (xh, z, y, 1 - xl, c)
    same = lambda u, v: 1 - jnp.minimum((u - v) * (u - v), 1)
    mine = same(c, xh) * same(xl, xh) * same(z // 2, c)
    z_low = z + xh * (3 - 2 * z)
    shard = (z_low * 4 + y, 16 + (3 - z_low) * 4 + y)

    barrier = pltpu.get_barrier_semaphore()
    far = near(2, 0)
    for peer in (partner, cross, swap_peer, across, beside, far, up_y, down_y, up_z, down_z):
        pl.semaphore_signal(barrier, inc=1, device_id=peer, device_id_type=MESH)
    for k in range(4):

        @pl.when((mine == 0) | (makers[k][1] != z) | (k // 2 != c))
        def _(k=k):
            pl.semaphore_signal(barrier, inc=1, device_id=makers[k], device_id_type=MESH)

    inputs = ((kv_hbm, kv_lat), (gain_hbm, gain), (table_hbm, table), (live_hbm, live))
    for n, (far_away, close) in enumerate(inputs):
        pltpu.make_async_copy(far_away, close, local_sem.at[12 + n]).start()
    own_rows = pltpu.make_async_copy(q_hbm.at[xh], qx.at[xh], local_sem.at[16])
    own_rows.start()
    pltpu.make_async_copy(wkv_hbm, wkv, local_sem.at[8]).start()
    for j in range(8):
        pltpu.make_async_copy(wq_hbm.at[:, pl.ds(j * 384, 384)], wq.at[j], local_sem.at[j]).start()
    pltpu.make_async_copy(wo_hbm, wg.at[c, y], local_sem.at[9]).start()

    with jax.named_scope("norm"):
        for n, (far_away, close) in enumerate(inputs):
            pltpu.make_async_copy(far_away, close, local_sem.at[12 + n]).wait()
        lane = lax.broadcasted_iota(jnp.int32, (1, ROPE), 1)
        sign = jnp.where(lane < ROPE // 2, -1.0, 1.0)

        def angles(m):
            cos_a, sin_a = table[2, pl.ds(m, 1), :], table[3, pl.ds(m, 1), :]
            cos_b, sin_b = table[0], table[1]
            return cos_a * cos_b - sin_a * sin_b, (sin_a * cos_b + cos_a * sin_b) * sign

        turned_rows = kv_lat[...].astype(jnp.float32).T
        rows = jnp.where(c == 0, turned_rows[:HALF], turned_rows[HALF:])
        latent = rows[:, :KVR]
        inverse = lax.rsqrt(jnp.mean(latent * latent, axis=-1, keepdims=True) + EPS)
        keys[me, c, :, :KVR] = (latent * inverse * gain[...]).astype(jnp.bfloat16)
        keys[me, c, :, KVR:] = turn(rows[:, KVR:], *angles(me * 2 + c)).astype(jnp.bfloat16)
        spot = lax.broadcasted_iota(jnp.int32, (32, 128), 0) * 128 + lax.broadcasted_iota(
            jnp.int32, (32, 128), 1
        )
        usable = (spot < prompt[0]) | (live[...] == 1)
        masked = jnp.where(usable, 0.0, -1e30)
        for r in range(32):
            b, at = r // (BLOCK // 128), r % (BLOCK // 128)
            bias[b : b + 1, at * 128 : (at + 1) * 128] = masked[r : r + 1]

    with jax.named_scope("barrier"):
        pl.semaphore_wait(barrier, 14 - mine)

    def key(t, o1, o2, which=None):
        ref = keys.at[unit(t, o1, o2), c]
        if which is None:
            return ref
        return ref.at[pl.ds(32 * which, 32)]

    def key_copy(number, t, o1, o2, device, which=None):
        ref = key(t, o1, o2, which)
        return copy(ref, ref, number, device)

    offsets = (0, 1, 3, 2)
    lower, upper = xh, 1 - xh

    def spread(q, t):
        k, o = 2 * q + t, offsets[q]
        key_copy(D2 + 2 * k, t, o, 0, near(0, 1)).start()
        key_copy(D2 + 2 * k + 1, t, o, 0, near(0, -1)).start()
        key_copy(PAIR + t, t, o, 0, partner).start()

    def first_out(t):
        key_copy(D1 + 2 * t, t, 0, 0, near(1, 0)).start()
        key_copy(D1 + 2 * t + 1, t, 0, 0, near(-1, 0)).start()
        spread(0, t)
        key_copy(FAR + t, t, 0, 0, far).start()

    def first_in(t):
        key_copy(D1 + 2 * t, t, -1, 0, near(1, 0)).wait_recv()
        spread(2, t)
        key_copy(D1 + 2 * t + 1, t, 1, 0, near(-1, 0)).wait_recv()
        spread(1, t)

    def far_in(t):
        key_copy(FAR + t, t, 2, 0, far).wait_recv()
        spread(3, t)

    def cross_in():
        key_copy(CROSS, 1, 0, 0, cross).wait_recv()

    with jax.named_scope("spread"):
        key_copy(CROSS, 0, 0, 0, cross).start()
        copy(q_hbm.at[1 - xh, c], qx.at[xh, c], SWAP, swap_peer).start()
        pl.when(xh == 1)(cross_in)
        first_out(lower)
        pl.when(xh == 0)(cross_in)
        first_out(upper)

    tables = [angles(2 * where + xh) for where in shard]

    def project(j):
        pltpu.make_async_copy(
            wq_hbm.at[:, pl.ds(0, 384)], wq.at[j], local_sem.at[j]
        ).wait()
        both = jnp.dot(
            qx[...].reshape(2 * HALF, 1536), wq[j], preferred_element_type=jnp.float32
        ).astype(jnp.bfloat16)
        for e in range(2):
            h = 2 * j + e
            plain = both[:, e * 192 : e * 192 + NOPE]
            roped = both[:, e * 192 + NOPE : (e + 1) * 192].astype(jnp.float32)
            w_key = wkv[:, pl.ds(pl.multiple_of(h * 256, 256), NOPE)]
            absorbed = lax.dot_general(
                plain, w_key, (((1,), (1,)), ((), ())), preferred_element_type=jnp.float32
            ).astype(jnp.bfloat16)
            for half in range(2):
                mine_rows = slice(half * HALF, (half + 1) * HALF)
                qs[half, h, :, :KVR] = absorbed[mine_rows]
                qs[half, h, :, KVR:] = turn(roped[mine_rows], *tables[half]).astype(jnp.bfloat16)

    def relay(q, t):
        k, o = 2 * q + t, offsets[q]
        key_copy(D2 + 2 * k, t, o, -1, near(0, 1)).wait_recv()
        key_copy(D2H + k, t, o, -1, near(0, 1), 0).start()
        key_copy(PAIR + t, t, o, -1, partner).start()
        key_copy(D2 + 2 * k + 1, t, o, 1, near(0, -1)).wait_recv()
        key_copy(D2H + k, t, o, 1, near(0, -1), 1).start()
        key_copy(PAIR + t, t, o, 1, partner).start()

    def last_in(q, t):
        k, o = 2 * q + t, offsets[q]
        key_copy(D2H + k, t, o, 2, near(0, 1)).wait_recv()
        key_copy(PAIR + t, t, o, 2, partner).start()

    def pair_in(t):
        ref = keys.at[pl.ds(0, 16), 1 - c]
        copy(ref, ref, PAIR + t, partner).wait_recv()

    span = wo_hbm.shape[0] // 2

    def w_copy(number, row, device, which):
        ref = wg.at[c, row, pl.ds(which * span, span)]
        return copy(ref, ref, number, device)

    def w_pair(row, number):
        return copy(wg.at[c, row], wg.at[c, row], WPAIR + number, partner)

    def w_pair_in(row, number):
        return copy(wg.at[1 - c, row], wg.at[1 - c, row], WPAIR + number, partner)

    def project_in(*order):
        with jax.named_scope("project"):
            for j in order:
                project(j)

    def start_w():
        pltpu.make_async_copy(wo_hbm, wg.at[c, y], local_sem.at[9]).wait()
        for which in range(2):
            w_copy(WFULL + which, y, up_y, which).start()
            w_copy(WFULL + 3 - which, y, down_y, 1 - which).start()
        w_pair(y, 0).start()

    def swap_on():
        copy(qx.at[1 - xh, c], qx.at[1 - xh, c], SWAP, swap_peer).wait_recv()
        copy(qx.at[1 - xh, c], qx.at[1 - xh, c], SWAP2, partner).start()

    with jax.named_scope("swap"):
        pl.when(xh == 1)(swap_on)
    with jax.named_scope("first_in_l"):
        first_in(lower)
    with jax.named_scope("relay_l0"):
        relay(0, lower)
    with jax.named_scope("far_l"):
        far_in(lower)
    with jax.named_scope("swap"):
        pl.when(xh == 0)(swap_on)
    with jax.named_scope("swap2"):
        own_rows.wait()
        pltpu.make_async_copy(wkv_hbm, wkv, local_sem.at[8]).wait()
        copy(qx.at[1 - xh, 1 - c], qx.at[1 - xh, 1 - c], SWAP2, partner).wait_recv()
    project_in(0, 1)
    with jax.named_scope("relay_l21"):
        relay(2, lower)
        relay(1, lower)
    project_in(2)
    with jax.named_scope("relay_l3"):
        relay(3, lower)
    with jax.named_scope("first_in_u"):
        first_in(upper)
    project_in(3)
    with jax.named_scope("far_u"):
        far_in(upper)
    with jax.named_scope("last_in_l"):
        for q in (0, 2, 1):
            last_in(q, lower)
    project_in(4)
    with jax.named_scope("last_in_l3"):
        last_in(3, lower)
    with jax.named_scope("relay_u0"):
        relay(0, upper)
    project_in(5, 6, 7)
    with jax.named_scope("pair_in_l"):
        pair_in(lower)

    scale = LOG2E / math.sqrt(NOPE + ROPE)
    tile_rows = HEADS * HALF
    reach = BLOCK // 128

    def attend(half, hooks):
        where = shard[half]
        blocks = where // reach
        m_ref[...] = jnp.full_like(m_ref, -1e30)
        l_ref[...] = jnp.zeros_like(l_ref)
        acc_ref[...] = jnp.zeros_like(acc_ref)

        def step(b, causal):
            block = keys[pl.ds(b * reach, reach)].reshape(BLOCK, WIDE)
            scores = lax.dot_general(
                qs[half].reshape(tile_rows, WIDE),
                block,
                (((1,), (1,)), ((), ())),
                preferred_element_type=jnp.float32,
            )
            scores = scores * scale + bias[pl.ds(b, 1), :]
            if causal is not None:
                scores = (scores.reshape(HEADS, HALF, BLOCK) + causal[None]).reshape(
                    tile_rows, BLOCK
                )
            before = m_ref[...]
            m_new = jnp.maximum(before, jnp.max(scores, axis=1, keepdims=True))
            alpha = jnp.exp2(before - m_new)
            lifted = jnp.exp2(scores - jnp.concatenate([m_new] * (BLOCK // 128), axis=1))
            total = l_ref[...] * alpha
            for k in range(BLOCK // 128):
                total = total + lifted[:, k * 128 : (k + 1) * 128]
            l_ref[...] = total
            m_ref[...] = m_new
            acc_ref[...] = acc_ref[...] * jnp.concatenate([alpha] * (KVR // 128), axis=1) + jnp.dot(
                lifted.astype(jnp.bfloat16), block[:, :KVR], preferred_element_type=jnp.float32
            )

        def open_step(b, carry):
            hooks(b, blocks)
            step(b, None)
            return carry

        lax.fori_loop(0, blocks, open_step, 0)
        hooks(blocks, blocks)
        token = where * 128 + xh * HALF + lax.broadcasted_iota(jnp.int32, (HALF, BLOCK), 0)
        position = blocks * BLOCK + lax.broadcasted_iota(jnp.int32, (HALF, BLOCK), 1)
        step(blocks, jnp.where(position <= token, 0.0, -1e30))
        total = jnp.sum(l_ref[...], axis=1, keepdims=True)
        ctx[...] = (acc_ref[...] / total).astype(jnp.bfloat16).reshape(HEADS, HALF, KVR)

    here = xh * 4 + z

    def values(half):
        for h in range(HEADS):
            w_value = wkv[:, h * 256 + NOPE : (h + 1) * 256]
            attended = jnp.dot(ctx[h], w_value, preferred_element_type=jnp.float32).astype(
                jnp.bfloat16
            )
            for r in range(2):
                for to in range(2):
                    at = to * 2 * ROWS + r * ROWS
                    astage[2 * half + r, to, :, h * VD : (h + 1) * VD] = attended[at : at + ROWS]
        for g in (2 * half, 2 * half + 1):
            pair_copy(g).start()
            ag[here, g, c] = astage[g, c]

    def a_copy(g, number, t, o, device, which=None):
        slot = (xh + t - 2 * xh * t) * 4 + lax.rem(z + o + 4, 4)
        ref = ag.at[slot, g]
        if which is not None:
            ref = ref.at[which]
        return copy(ref, ref, ABASE + ASTRIDE * g + number, device)

    def pair_copy(g):
        return copy(
            astage.at[g, 1 - c], ag.at[here, g, c], ABASE + ASTRIDE * g + APAIR, partner
        )

    def pair_copy_in(g):
        ref = ag.at[here, g, 1 - c]
        return copy(ref, ref, ABASE + ASTRIDE * g + APAIR, partner)

    def stage1(g):
        pair_copy_in(g).wait_recv()
        a_copy(g, AX, 0, 0, across).start()
        a_copy(g, AZ, 0, 0, up_z).start()
        a_copy(g, AZ + 1, 0, 0, down_z).start()

    def stage2(g):
        a_copy(g, AZ, 0, -1, up_z).wait_recv()
        a_copy(g, AZH, 0, -1, up_z, 0).start()
        a_copy(g, AZ + 1, 0, 1, down_z).wait_recv()
        a_copy(g, AZH, 0, 1, down_z, 1).start()

    def stage3(g):
        a_copy(g, AX, 1, 0, across).wait_recv()
        a_copy(g, AZ + 2, 1, 0, up_z).start()
        a_copy(g, AZ + 3, 1, 0, down_z).start()

    def stage4(g):
        a_copy(g, AZH, 0, 2, up_z).wait_recv()
        a_copy(g, AX2, 0, 2, across).start()

    def stage5(g):
        a_copy(g, AZ + 2, 1, -1, up_z).wait_recv()
        a_copy(g, AZ + 3, 1, 1, down_z).wait_recv()
        a_copy(g, AX2, 1, 2, across).wait_recv()

    def w_relay(which):
        if which == 0:
            w_copy(WFULL, lax.rem(y + 3, 4), up_y, 0).wait_recv()
            w_copy(WHALF, lax.rem(y + 3, 4), up_y, 0).start()
        else:
            w_copy(WFULL + 3, lax.rem(y + 1, 4), down_y, 1).wait_recv()
            w_copy(WHALF, lax.rem(y + 1, 4), down_y, 1).start()

    def w_middle():
        w_copy(WFULL + 1, lax.rem(y + 3, 4), up_y, 1).wait_recv()
        w_pair(lax.rem(y + 3, 4), 1).start()
        w_copy(WFULL + 2, lax.rem(y + 1, 4), down_y, 0).wait_recv()
        w_pair(lax.rem(y + 1, 4), 2).start()

    def w_last():
        ref = wg.at[c, lax.rem(y + 2, 4)]
        copy(ref, ref, WHALF, up_y).wait_recv()
        w_pair(lax.rem(y + 2, 4), 3).start()

    def w_all():
        for k, o in enumerate((0, 3, 1, 2)):
            w_pair_in(lax.rem(y + o, 4), k).wait_recv()

    def product(first, count):
        rows = 8 * count * ROWS
        total = jnp.zeros((rows, 4 * 224), jnp.float32)
        for core in range(2):
            total = total + lax.dot_general(
                ag[:, first : first + count, core].reshape(rows, HEADS * VD),
                wg[core].reshape(4 * 224, HEADS * VD),
                (((1,), (1,)), ((), ())),
                preferred_element_type=jnp.float32,
            )
        total = total.reshape(8, count * ROWS, 4 * 224)
        for n in range(count):
            part[first + n] = total[:, n * ROWS : (n + 1) * ROWS]

    def slots(half, k):
        straight, mirrored = k, 3 - k
        first = straight if half == 0 else mirrored
        return first, 4 + 3 - first

    def half_out(g):
        for k in range(2):
            low, high = slots(g // 2, 2 * (1 - xl) + k)
            outgoing[g, 0, k, 0] = part[g, low].astype(jnp.bfloat16)
            outgoing[g, 0, k, 1] = part[g, high].astype(jnp.bfloat16)
            copy(outgoing.at[g, 0, k], summand.at[g, k], XSUM + 2 * g + k, beside).start()

    def whole_out(g):
        half = g // 2
        number = lax.rem(z, 2) + 2 * c + 4 * (g % 2)
        for k in range(2):
            row = 2 * xl + k
            copy(outgoing.at[g, 0, k], summand.at[g, k], XSUM + 2 * g + k, beside).wait_recv()
            low, high = slots(half, row)
            for xs, at in enumerate((low, high)):
                outgoing[g, 1, k, xs] = (
                    part[g, at] + summand[g, k, xs].astype(jnp.float32)
                ).astype(jnp.bfloat16)
            own = (mine == 1) & (xh == half) & (z == row)
            target = out_ref.at[:, 2 * c + g % 2, :, pl.ds(lax.rem(z, 2) * 896, 896)]

            @pl.when(jnp.logical_not(own))
            def _():
                copy(
                    outgoing.at[g, 1, k], target, OUT + number, owners[half][k], OUT + 2 * g + k
                ).start()

            @pl.when(own)
            def _():
                pltpu.make_async_copy(
                    outgoing.at[g, 1, k], target, local_sem.at[10 + g % 2]
                ).start()

    def early_hooks(b, blocks):
        @pl.when(b == 0)
        def _():
            with jax.named_scope("relay_u"):
                for q in (2, 1, 3):
                    relay(q, upper)
                start_w()

        @pl.when((b == blocks) & (blocks > 0))
        def _():
            with jax.named_scope("last_in_u"):
                for q in (0, 2, 1, 3):
                    last_in(q, upper)

    def late_hooks(b, blocks):
        @pl.when((b == 0) & (shard[0] < reach))
        def _():
            with jax.named_scope("last_in_u"):
                for q in (0, 2, 1, 3):
                    last_in(q, upper)

        @pl.when(b == 1)
        def _():
            with jax.named_scope("stage1_01"):
                stage1(0)
                stage1(1)

        @pl.when(b == 4)
        def _():
            with jax.named_scope("pair_in_u"):
                pair_in(upper)

        @pl.when(b == blocks)
        def _():
            with jax.named_scope("stage23_0"):
                stage2(0)
                stage3(0)
                w_relay(0)
                w_relay(1)

    with jax.named_scope("attend_low"):
        attend(0, early_hooks)
    with jax.named_scope("values"):
        values(0)
    with jax.named_scope("attend_high"):
        attend(1, late_hooks)
    with jax.named_scope("values"):
        values(1)
    with jax.named_scope("stage1_23"):
        stage1(2)
        stage1(3)
    with jax.named_scope("stage23_1"):
        stage2(1)
        stage3(1)
    with jax.named_scope("stage4_0"):
        stage4(0)
    with jax.named_scope("w_middle"):
        w_middle()
    with jax.named_scope("stage2_2"):
        stage2(2)
    with jax.named_scope("stage2_3"):
        stage2(3)
    with jax.named_scope("stage3_2"):
        stage3(2)
    with jax.named_scope("stage3_3"):
        stage3(3)
    with jax.named_scope("stage4_1"):
        stage4(1)
    with jax.named_scope("w_last"):
        w_last()
    with jax.named_scope("stage4_2"):
        stage4(2)
    with jax.named_scope("stage5_0"):
        stage5(0)
    with jax.named_scope("stage4_3"):
        stage4(3)
    with jax.named_scope("stage5_1"):
        stage5(1)
    with jax.named_scope("w_all"):
        w_all()
    with jax.named_scope("product_low"):
        product(0, 2)
    with jax.named_scope("half_out_low"):
        half_out(0)
        half_out(1)
    with jax.named_scope("stage5_2"):
        stage5(2)
    with jax.named_scope("product_2"):
        product(2, 1)
    with jax.named_scope("half_out_2"):
        half_out(2)
    with jax.named_scope("stage5_3"):
        stage5(3)
    with jax.named_scope("product_3"):
        product(3, 1)
    with jax.named_scope("half_out_3"):
        half_out(3)
    with jax.named_scope("whole_out_low"):
        whole_out(0)
        whole_out(1)
    with jax.named_scope("whole_out_2"):
        whole_out(2)
    with jax.named_scope("whole_out_3"):
        whole_out(3)

    with jax.named_scope("finish"):
        for n in range(8):
            r, k = n // 4, n % 4
            piece = out_ref.at[:, 2 * (k // 2) + r, :, (k % 2) * 896 : (k % 2 + 1) * 896]
            self_made = (mine == 1) & (makers[k][1] == z) & (k // 2 == c)

            @pl.when(jnp.logical_not(self_made))
            def _(n=n, piece=piece):
                copy(piece, piece, OUT + n, partner).wait_recv()

            @pl.when(self_made)
            def _(r=r, piece=piece):
                pltpu.make_async_copy(outgoing.at[0, 1, 0], piece, local_sem.at[10 + r]).wait()

    with jax.named_scope("drain"):
        full = keys.at[0, 0]

        def sent(ref, number):
            copy(ref, ref, number, partner).wait_send()

        def drain(ref, first, count):
            def one(n, carry):
                sent(ref, first + n)
                return carry

            lax.fori_loop(0, count, one, 0)

        sent(full, CROSS)
        sent(qx.at[0, 0], SWAP)
        sent(qx.at[0, 0], SWAP2)
        drain(full, D1, 4)
        drain(full, FAR, 2)
        drain(full, D2, 16)
        drain(full, D2H, 8)
        drain(keys.at[pl.ds(0, 16), 0], PAIR, 2)
        drain(wg.at[0, 0, pl.ds(0, span)], WFULL, 4)
        sent(wg.at[0, 0], WHALF)
        drain(wg.at[0, 0], WPAIR, 4)
        for g in range(CHUNKS):
            at = ABASE + ASTRIDE * g
            sent(astage.at[g, 0], at + APAIR)
            sent(ag.at[0, 0], at + AX)
            drain(ag.at[0, 0], at + AZ, 4)
            sent(ag.at[0, 0], at + AZH)
            sent(ag.at[0, 0], at + AX2)
        drain(summand.at[0, 0], XSUM, 8)
        for g in range(CHUNKS):
            for k in range(2):
                own = (mine == 1) & (xh == g // 2) & (z == 2 * xl + k)

                @pl.when(jnp.logical_not(own))
                def _(g=g, k=k):
                    sent(summand.at[0, 0], OUT + 2 * g + k)


def local(q_latent, kv_latent, kv_gain, w_q_b, w_kv_b, w_o, prompt_len, response_mask):
    frequency = 10000.0 ** (-np.arange(ROPE // 2, dtype=np.float64) * 2.0 / ROPE)
    fine = np.arange(HALF, dtype=np.float64)[:, None] * np.tile(frequency, 2)[None, :]
    table = np.stack([np.cos(fine), np.sin(fine), np.cos(HALF * fine), np.sin(HALF * fine)])
    hbm = pl.BlockSpec(memory_space=pltpu.HBM)
    bf16 = jnp.bfloat16
    depth = HEADS * VD
    result = pl.pallas_call(
        body,
        out_shape=jax.ShapeDtypeStruct((2, 4, ROWS, 1792), bf16),
        in_specs=[hbm] * 5 + [pl.BlockSpec(memory_space=pltpu.SMEM)] + [hbm] * 3,
        out_specs=hbm,
        scratch_shapes=[
            pltpu.SemaphoreType.DMA((NSEM,)),
            pltpu.SemaphoreType.DMA((NSEM,)),
            pltpu.SemaphoreType.DMA((17,)),
            pltpu.VMEM((WIDE, 128), bf16),
            pltpu.VMEM((1, KVR), jnp.float32),
            pltpu.VMEM((4, HALF, ROPE), jnp.float32),
            pltpu.VMEM((32, 128), jnp.int32),
            pltpu.VMEM((2, 2, HALF // 2, 1536), bf16),
            pltpu.VMEM((8, 1536, 384), bf16),
            pltpu.VMEM((512, 4096), bf16),
            pltpu.VMEM((32, 2, HALF, WIDE), bf16),
            pltpu.VMEM((2, HEADS, HALF, WIDE), bf16),
            pltpu.VMEM((HEADS, HALF, KVR), bf16),
            pltpu.VMEM((CHUNKS, 2, ROWS, depth), bf16),
            pltpu.VMEM((8, CHUNKS, 2, ROWS, depth), bf16),
            pltpu.VMEM((2, 4, 224, 2048), bf16),
            pltpu.VMEM((CHUNKS, 8, ROWS, 4 * 224), jnp.float32),
            pltpu.VMEM((CHUNKS, 2, 2, 2, ROWS, 4 * 224), bf16),
            pltpu.VMEM((CHUNKS, 2, 2, ROWS, 4 * 224), bf16),
            pltpu.VMEM((4096 // BLOCK, BLOCK), jnp.float32),
            pltpu.VMEM((HEADS * HALF, 128), jnp.float32),
            pltpu.VMEM((HEADS * HALF, 128), jnp.float32),
            pltpu.VMEM((HEADS * HALF, KVR), jnp.float32),
        ],
        compiler_params=pltpu.CompilerParams(
            collective_id=0, has_side_effects=True, vmem_limit_bytes=67000000
        ),
        cost_estimate=pl.CostEstimate(
            flops=20_000_000_000, bytes_accessed=16_000_000, transcendentals=0
        ),
        name="layer",
    )(
        q_latent.reshape(2, 2, HALF // 2, 1536),
        kv_latent.T,
        kv_gain.reshape(1, -1),
        jnp.asarray(table, jnp.float32),
        response_mask.reshape(32, 128),
        prompt_len,
        w_q_b,
        w_kv_b,
        w_o.T,
    )
    return result.reshape(128, 1792)


def solution(mesh):
    finer = Mesh(mesh.devices.reshape(2, 4, 4, 2, 2), AXES)
    placed = (
        P(DP, None),
        P(DP, None),
        P(),
        P(None, HEAD),
        P(None, HEAD),
        P(HEAD, DP),
        P(),
        P(),
    )
    return jax.shard_map(
        local, mesh=finer, in_specs=placed, out_specs=P(DP, HEAD), check_vma=False
    )
```

```python
import functools
import math

import jax
import jax.numpy as jnp
import numpy as np
from jax import lax
from jax.experimental import pallas as pl
from jax.experimental.pallas import tpu as pltpu
from jax.sharding import Mesh
from jax.sharding import PartitionSpec as P

KVR = 512
ROPE = 64
NOPE = 128
VD = 128
WIDE = KVR + ROPE
AXES = ("xh", "z", "y", "xl", "c")
DP = ("xh", "z", "y")
HEAD = ("xl", "c")
MESH = pl.DeviceIdType.MESH

HEADS = 16
PER = 8
CHUNKS = 4
HALF = 64
ROWS = 16
BLOCK = 512
LOG2E = 1.4426950408889634
EPS = 1e-06

CROSS = 0
SWAP = 1
SWAP2 = 2
D1 = 3
FAR = 7
D2 = 9
D2H = 25
PAIR = 33
WFULL = 35
WHALF = 39
WPAIR = 40
ABASE = 44
APAIR, AX, AZ, AZH, AX2 = 0, 1, 2, 6, 7
ASTRIDE = 8
OUT = ABASE + ASTRIDE * CHUNKS
XSUM = OUT + 8
NSEM = XSUM + 8
S_CROSS, S_SWAP, S_KEYS, S_PAIR, S_W, S_WPAIR, S_APAIR, S_XSUM, S_A, S_OUT = 0, 1, 2, 3, 4, 5, 6, 7, 8, 12
NSENT = S_OUT + 8


def turn(values, cosine, sine):
    swapped = jnp.concatenate([values[:, ROPE // 2 :], values[:, : ROPE // 2]], axis=1)
    return values * cosine + swapped * sine


def body(
    q_hbm,
    kv_hbm,
    gain_hbm,
    table_hbm,
    live_hbm,
    prompt,
    wq_hbm,
    wkv_hbm,
    wo_hbm,
    out_ref,
    out_sem,
    in_sem,
    local_sem,
    kv_lat,
    gain,
    table,
    live,
    qx,
    wq,
    wkv,
    keys,
    qs,
    ctx,
    low_stage,
    high_stage,
    low,
    high,
    wg,
    part,
    outgoing,
    summand,
    bias,
    m_ref,
    l_ref,
    acc_ref,
):
    xh, z, y, xl, c = (lax.axis_index(a) for a in AXES)
    d1 = y + c * (z - y)
    d2 = z + c * (y - z)

    def place(t, o1, o2):
        a = lax.rem(d1 + o1 + 4, 4)
        b = lax.rem(d2 + o2 + 4, 4)
        zz = b + c * (a - b)
        yy = a + c * (b - a)
        xx = xh + t - 2 * xh * t
        return xx, zz, yy

    def unit(t, o1, o2):
        xx, zz, yy = place(t, o1, o2)
        return xx * 16 + zz * 4 + yy

    def near(o1, o2):
        _, zz, yy = place(0, o1, o2)
        return (xh, zz, yy, xl, c)

    def copy(src, dst, number, device, leaving=0):
        return pltpu.make_async_remote_copy(
            src_ref=src,
            dst_ref=dst,
            send_sem=out_sem.at[leaving],
            recv_sem=in_sem.at[number],
            device_id=device,
            device_id_type=MESH,
        )

    me = unit(0, 0, 0)
    partner = (xh, z, y, xl, 1 - c)
    cross = (1 - xh, z, y, 1 - xl, c)
    swap_peer = (1 - xh, 3 - z, y, 1 - xl, c)
    across = (1 - xh, z, y, xl, c)
    up_y = (xh, z, lax.rem(y + 1, 4), xl, c)
    down_y = (xh, z, lax.rem(y + 3, 4), xl, c)
    up_z = (xh, lax.rem(z + 1, 4), y, xl, c)
    down_z = (xh, lax.rem(z + 3, 4), y, xl, c)
    owners = [[(t, 2 * xl + k, y, xh, z // 2) for k in range(2)] for t in range(2)]
    makers = [(xl, 2 * c + k % 2, y, z // 2, k // 2) for k in range(4)]
    beside = (xh, z, y, 1 - xl, c)
    same = lambda u, v: 1 - jnp.minimum((u - v) * (u - v), 1)
    mine = same(c, xh) * same(xl, xh) * same(z // 2, c)
    z_low = z + xh * (3 - 2 * z)
    shard = (z_low * 4 + y, 16 + (3 - z_low) * 4 + y)

    barrier = pltpu.get_barrier_semaphore()
    far = near(2, 0)
    for peer in (partner, cross, swap_peer, across, beside, far, up_y, down_y, up_z, down_z):
        pl.semaphore_signal(barrier, inc=1, device_id=peer, device_id_type=MESH)
    for k in range(4):

        @pl.when((mine == 0) | (makers[k][1] != z) | (k // 2 != c))
        def _(k=k):
            pl.semaphore_signal(barrier, inc=1, device_id=makers[k], device_id_type=MESH)

    inputs = ((kv_hbm, kv_lat), (gain_hbm, gain), (table_hbm, table), (live_hbm, live))
    for n, (far_away, close) in enumerate(inputs):
        pltpu.make_async_copy(far_away, close, local_sem.at[12 + n]).start()
    own_rows = pltpu.make_async_copy(q_hbm.at[xh], qx.at[xh], local_sem.at[16])
    own_rows.start()
    pltpu.make_async_copy(wkv_hbm, wkv, local_sem.at[8]).start()
    for j in range(8):
        pltpu.make_async_copy(wq_hbm.at[:, pl.ds(j * 384, 384)], wq.at[j], local_sem.at[j]).start()
    pltpu.make_async_copy(wo_hbm, wg.at[c, y], local_sem.at[9]).start()

    with jax.named_scope("norm"):
        for n, (far_away, close) in enumerate(inputs):
            pltpu.make_async_copy(far_away, close, local_sem.at[12 + n]).wait()
        lane = lax.broadcasted_iota(jnp.int32, (1, ROPE), 1)
        sign = jnp.where(lane < ROPE // 2, -1.0, 1.0)

        def angles(m):
            cos_a, sin_a = table[2, pl.ds(m, 1), :], table[3, pl.ds(m, 1), :]
            cos_b, sin_b = table[0], table[1]
            return cos_a * cos_b - sin_a * sin_b, (sin_a * cos_b + cos_a * sin_b) * sign

        turned_rows = kv_lat[...].astype(jnp.float32).T
        rows = jnp.where(c == 0, turned_rows[:HALF], turned_rows[HALF:])
        latent = rows[:, :KVR]
        inverse = lax.rsqrt(jnp.mean(latent * latent, axis=-1, keepdims=True) + EPS)
        keys[me, c, :, :KVR] = (latent * inverse * gain[...]).astype(jnp.bfloat16)
        keys[me, c, :, KVR:] = turn(rows[:, KVR:], *angles(me * 2 + c)).astype(jnp.bfloat16)
        spot = lax.broadcasted_iota(jnp.int32, (32, 128), 0) * 128 + lax.broadcasted_iota(
            jnp.int32, (32, 128), 1
        )
        usable = (spot < prompt[0]) | (live[...] == 1)
        masked = jnp.where(usable, 0.0, -1e30)
        for r in range(32):
            b, at = r // (BLOCK // 128), r % (BLOCK // 128)
            bias[b : b + 1, at * 128 : (at + 1) * 128] = masked[r : r + 1]

    with jax.named_scope("barrier"):
        pl.semaphore_wait(barrier, 14 - mine)

    def key(t, o1, o2, which=None):
        ref = keys.at[unit(t, o1, o2), c]
        if which is None:
            return ref
        return ref.at[pl.ds(32 * which, 32)]

    def key_copy(number, t, o1, o2, device, which=None, leaving=S_KEYS):
        ref = key(t, o1, o2, which)
        return copy(ref, ref, number, device, leaving)

    offsets = (0, 1, 3, 2)
    lower, upper = xh, 1 - xh

    def spread(q, t):
        k, o = 2 * q + t, offsets[q]
        key_copy(D2 + 2 * k, t, o, 0, near(0, 1)).start()
        key_copy(D2 + 2 * k + 1, t, o, 0, near(0, -1)).start()
        key_copy(PAIR + t, t, o, 0, partner, leaving=S_PAIR).start()

    def first_out(t):
        key_copy(D1 + 2 * t, t, 0, 0, near(1, 0)).start()
        key_copy(D1 + 2 * t + 1, t, 0, 0, near(-1, 0)).start()
        spread(0, t)
        key_copy(FAR + t, t, 0, 0, far).start()

    def first_in(t):
        key_copy(D1 + 2 * t, t, -1, 0, near(1, 0)).wait_recv()
        spread(2, t)
        key_copy(D1 + 2 * t + 1, t, 1, 0, near(-1, 0)).wait_recv()
        spread(1, t)

    def far_in(t):
        key_copy(FAR + t, t, 2, 0, far).wait_recv()
        spread(3, t)

    def cross_in():
        key_copy(CROSS, 1, 0, 0, cross).wait_recv()

    with jax.named_scope("spread"):
        key_copy(CROSS, 0, 0, 0, cross, leaving=S_CROSS).start()
        copy(q_hbm.at[1 - xh, c], qx.at[xh, c], SWAP, swap_peer, S_SWAP).start()
        pl.when(xh == 1)(cross_in)
        first_out(lower)
        pl.when(xh == 0)(cross_in)
        first_out(upper)

    tables = [angles(2 * where + xh) for where in shard]

    def project(j):
        pltpu.make_async_copy(
            wq_hbm.at[:, pl.ds(0, 384)], wq.at[j], local_sem.at[j]
        ).wait()
        both = jnp.dot(
            qx[...].reshape(2 * HALF, 1536), wq[j], preferred_element_type=jnp.float32
        ).astype(jnp.bfloat16)
        for e in range(2):
            h = 2 * j + e
            plain = both[:, e * 192 : e * 192 + NOPE]
            roped = both[:, e * 192 + NOPE : (e + 1) * 192].astype(jnp.float32)
            w_key = wkv[:, pl.ds(pl.multiple_of(h * 256, 256), NOPE)]
            absorbed = lax.dot_general(
                plain, w_key, (((1,), (1,)), ((), ())), preferred_element_type=jnp.float32
            ).astype(jnp.bfloat16)
            for half in range(2):
                mine_rows = slice(half * HALF, (half + 1) * HALF)
                qs[half, h, :, :KVR] = absorbed[mine_rows]
                qs[half, h, :, KVR:] = turn(roped[mine_rows], *tables[half]).astype(jnp.bfloat16)

    def relay(q, t):
        k, o = 2 * q + t, offsets[q]
        key_copy(D2 + 2 * k, t, o, -1, near(0, 1)).wait_recv()
        key_copy(D2H + k, t, o, -1, near(0, 1), 0).start()
        key_copy(PAIR + t, t, o, -1, partner, leaving=S_PAIR).start()
        key_copy(D2 + 2 * k + 1, t, o, 1, near(0, -1)).wait_recv()
        key_copy(D2H + k, t, o, 1, near(0, -1), 1).start()
        key_copy(PAIR + t, t, o, 1, partner, leaving=S_PAIR).start()

    def last_in(q, t):
        k, o = 2 * q + t, offsets[q]
        key_copy(D2H + k, t, o, 2, near(0, 1)).wait_recv()
        key_copy(PAIR + t, t, o, 2, partner, leaving=S_PAIR).start()

    def pair_in(t):
        ref = keys.at[pl.ds(0, 16), 1 - c]
        copy(ref, ref, PAIR + t, partner).wait_recv()

    span = wo_hbm.shape[0] // 2

    def w_copy(number, row, device, which):
        ref = wg.at[c, row, pl.ds(which * span, span)]
        return copy(ref, ref, number, device, S_W)

    def w_pair(row, number):
        return copy(wg.at[c, row], wg.at[c, row], WPAIR + number, partner, S_WPAIR)

    def w_pair_in(row, number):
        return copy(wg.at[1 - c, row], wg.at[1 - c, row], WPAIR + number, partner)

    def project_in(*order):
        with jax.named_scope("project"):
            for j in order:
                project(j)

    def start_w():
        pltpu.make_async_copy(wo_hbm, wg.at[c, y], local_sem.at[9]).wait()
        for which in range(2):
            w_copy(WFULL + which, y, up_y, which).start()
            w_copy(WFULL + 3 - which, y, down_y, 1 - which).start()
        w_pair(y, 0).start()

    def swap_on():
        copy(qx.at[1 - xh, c], qx.at[1 - xh, c], SWAP, swap_peer).wait_recv()
        copy(qx.at[1 - xh, c], qx.at[1 - xh, c], SWAP2, partner, S_SWAP).start()

    with jax.named_scope("swap"):
        pl.when(xh == 1)(swap_on)
    with jax.named_scope("first_in_l"):
        first_in(lower)
    with jax.named_scope("relay_l0"):
        relay(0, lower)
    with jax.named_scope("far_l"):
        far_in(lower)
    with jax.named_scope("swap"):
        pl.when(xh == 0)(swap_on)
    with jax.named_scope("swap2"):
        own_rows.wait()
        pltpu.make_async_copy(wkv_hbm, wkv, local_sem.at[8]).wait()
        copy(qx.at[1 - xh, 1 - c], qx.at[1 - xh, 1 - c], SWAP2, partner).wait_recv()
    project_in(0, 1)
    with jax.named_scope("relay_l21"):
        relay(2, lower)
        relay(1, lower)
    project_in(2)
    with jax.named_scope("relay_l3"):
        relay(3, lower)
    with jax.named_scope("first_in_u"):
        first_in(upper)
    project_in(3)
    with jax.named_scope("far_u"):
        far_in(upper)
    with jax.named_scope("last_in_l"):
        for q in (0, 2, 1):
            last_in(q, lower)
    project_in(4)
    with jax.named_scope("last_in_l3"):
        last_in(3, lower)
    with jax.named_scope("relay_u0"):
        relay(0, upper)
    project_in(5, 6, 7)
    with jax.named_scope("pair_in_l"):
        pair_in(lower)

    scale = LOG2E / math.sqrt(NOPE + ROPE)
    reach = BLOCK // 128

    def attend(half, hooks, first, count):
        where = shard[half]
        blocks = where // reach
        tile_rows = count * HALF
        upto = pl.ds(0, tile_rows)
        m_ref[upto] = jnp.full((tile_rows, 128), -1e30, jnp.float32)
        l_ref[upto] = jnp.zeros((tile_rows, 128), jnp.float32)
        acc_ref[upto] = jnp.zeros((tile_rows, KVR), jnp.float32)

        def step(b, causal):
            block = keys[pl.ds(b * reach, reach)].reshape(BLOCK, WIDE)
            scores = lax.dot_general(
                qs[half, first : first + count].reshape(tile_rows, WIDE),
                block,
                (((1,), (1,)), ((), ())),
                preferred_element_type=jnp.float32,
            )
            scores = scores * scale + bias[pl.ds(b, 1), :]
            if causal is not None:
                scores = (scores.reshape(count, HALF, BLOCK) + causal[None]).reshape(
                    tile_rows, BLOCK
                )
            before = m_ref[upto]
            m_new = jnp.maximum(before, jnp.max(scores, axis=1, keepdims=True))
            alpha = jnp.exp2(before - m_new)
            lifted = jnp.exp2(scores - jnp.concatenate([m_new] * (BLOCK // 128), axis=1))
            total = l_ref[upto] * alpha
            for k in range(BLOCK // 128):
                total = total + lifted[:, k * 128 : (k + 1) * 128]
            l_ref[upto] = total
            m_ref[upto] = m_new
            acc_ref[upto] = acc_ref[upto] * jnp.concatenate([alpha] * (KVR // 128), axis=1) + jnp.dot(
                lifted.astype(jnp.bfloat16), block[:, :KVR], preferred_element_type=jnp.float32
            )

        def open_step(b, carry):
            hooks(b, blocks)
            step(b, None)
            return carry

        lax.fori_loop(0, blocks, open_step, 0)
        hooks(blocks, blocks)
        token = where * 128 + xh * HALF + lax.broadcasted_iota(jnp.int32, (HALF, BLOCK), 0)
        position = blocks * BLOCK + lax.broadcasted_iota(jnp.int32, (HALF, BLOCK), 1)
        step(blocks, jnp.where(position <= token, 0.0, -1e30))
        total = jnp.sum(l_ref[upto], axis=1, keepdims=True)
        ctx[:count] = (acc_ref[upto] / total).astype(jnp.bfloat16).reshape(count, HALF, KVR)

    here = xh * 4 + z

    def value_rows(h, at):
        w_value = wkv[:, h * 256 + NOPE : (h + 1) * 256]
        return jnp.dot(ctx[at], w_value, preferred_element_type=jnp.float32).astype(jnp.bfloat16)

    def values_low(g):
        for n in range(PER):
            attended = value_rows(g * PER + n, n)
            for to in range(2):
                low_stage[g, to, :, n * VD : (n + 1) * VD] = attended[
                    to * 2 * ROWS : (to + 1) * 2 * ROWS
                ]
        pair_copy(g).start()
        low[here, g, c] = low_stage[g, c]

    def values_high():
        for h in range(HEADS):
            attended = value_rows(h, h)
            for r in range(2):
                for to in range(2):
                    at = to * 2 * ROWS + r * ROWS
                    high_stage[r, to, :, h * VD : (h + 1) * VD] = attended[at : at + ROWS]
        for r in range(2):
            pair_copy(2 + r).start()
            high[here, r, c] = high_stage[r, c]

    def block_of(slot, g):
        return low.at[slot, g] if g < 2 else high.at[slot, g - 2]

    def a_copy(g, number, t, o, device, which=None):
        slot = (xh + t - 2 * xh * t) * 4 + lax.rem(z + o + 4, 4)
        ref = block_of(slot, g)
        if which is not None:
            ref = ref.at[which]
        return copy(ref, ref, ABASE + ASTRIDE * g + number, device, S_A + g)

    def pair_copy(g):
        staged = low_stage.at[g, 1 - c] if g < 2 else high_stage.at[g - 2, 1 - c]
        return copy(
            staged, block_of(here, g).at[c], ABASE + ASTRIDE * g + APAIR, partner, S_APAIR
        )

    def pair_copy_in(g):
        ref = block_of(here, g).at[1 - c]
        return copy(ref, ref, ABASE + ASTRIDE * g + APAIR, partner, S_APAIR)

    def stage1(g):
        pair_copy_in(g).wait_recv()
        a_copy(g, AX, 0, 0, across).start()
        a_copy(g, AZ, 0, 0, up_z).start()
        a_copy(g, AZ + 1, 0, 0, down_z).start()

    def stage2(g):
        a_copy(g, AZ, 0, -1, up_z).wait_recv()
        a_copy(g, AZH, 0, -1, up_z, 0).start()
        a_copy(g, AZ + 1, 0, 1, down_z).wait_recv()
        a_copy(g, AZH, 0, 1, down_z, 1).start()

    def stage3(g):
        a_copy(g, AX, 1, 0, across).wait_recv()
        a_copy(g, AZ + 2, 1, 0, up_z).start()
        a_copy(g, AZ + 3, 1, 0, down_z).start()

    def stage4(g):
        a_copy(g, AZH, 0, 2, up_z).wait_recv()
        a_copy(g, AX2, 0, 2, across).start()

    def stage5(g):
        a_copy(g, AZ + 2, 1, -1, up_z).wait_recv()
        a_copy(g, AZ + 3, 1, 1, down_z).wait_recv()
        a_copy(g, AX2, 1, 2, across).wait_recv()

    def w_relay(which):
        if which == 0:
            w_copy(WFULL, lax.rem(y + 3, 4), up_y, 0).wait_recv()
            w_copy(WHALF, lax.rem(y + 3, 4), up_y, 0).start()
        else:
            w_copy(WFULL + 3, lax.rem(y + 1, 4), down_y, 1).wait_recv()
            w_copy(WHALF, lax.rem(y + 1, 4), down_y, 1).start()

    def w_middle():
        w_copy(WFULL + 1, lax.rem(y + 3, 4), up_y, 1).wait_recv()
        w_pair(lax.rem(y + 3, 4), 1).start()
        w_copy(WFULL + 2, lax.rem(y + 1, 4), down_y, 0).wait_recv()
        w_pair(lax.rem(y + 1, 4), 2).start()

    def w_last():
        ref = wg.at[c, lax.rem(y + 2, 4)]
        copy(ref, ref, WHALF, up_y).wait_recv()
        w_pair(lax.rem(y + 2, 4), 3).start()

    def w_all():
        for k, o in enumerate((0, 3, 1, 2)):
            w_pair_in(lax.rem(y + o, 4), k).wait_recv()

    def multiplied(rows, weights):
        return lax.dot_general(
            rows, weights, (((1,), (1,)), ((), ())), preferred_element_type=jnp.float32
        )

    def product_low():
        rows, depth = 16 * ROWS, PER * VD
        total = jnp.zeros((rows, 4 * 224), jnp.float32)
        for g in range(2):
            for core in range(2):
                total = total + multiplied(
                    low[:, g, core].reshape(rows, depth),
                    wg[core, :, :, g * depth : (g + 1) * depth].reshape(4 * 224, depth),
                )
        total = total.reshape(8, 2 * ROWS, 4 * 224)
        for n in range(2):
            part[n] = total[:, n * ROWS : (n + 1) * ROWS]

    def product_high(r):
        rows = 8 * ROWS
        total = jnp.zeros((rows, 4 * 224), jnp.float32)
        for core in range(2):
            total = total + multiplied(
                high[:, r, core].reshape(rows, HEADS * VD),
                wg[core].reshape(4 * 224, HEADS * VD),
            )
        part[2 + r] = total.reshape(8, ROWS, 4 * 224)

    def slots(half, k):
        straight, mirrored = k, 3 - k
        first = straight if half == 0 else mirrored
        return first, 4 + 3 - first

    def half_out(g):
        for k in range(2):
            for xs, at in enumerate(slots(g // 2, 2 * (1 - xl) + k)):
                outgoing[g, 0, k, xs] = part[g, at].astype(jnp.bfloat16)
            copy(
                outgoing.at[g, 0, k], summand.at[g, k], XSUM + 2 * g + k, beside, S_XSUM
            ).start()

    def whole_out(g):
        half = g // 2
        number = lax.rem(z, 2) + 2 * c + 4 * (g % 2)
        for k in range(2):
            row = 2 * xl + k
            copy(outgoing.at[g, 0, k], summand.at[g, k], XSUM + 2 * g + k, beside).wait_recv()
            for xs, at in enumerate(slots(half, row)):
                outgoing[g, 1, k, xs] = (
                    part[g, at] + summand[g, k, xs].astype(jnp.float32)
                ).astype(jnp.bfloat16)
            own = (mine == 1) & (xh == half) & (z == row)
            target = out_ref.at[:, 2 * c + g % 2, :, pl.ds(lax.rem(z, 2) * 896, 896)]

            @pl.when(jnp.logical_not(own))
            def _():
                copy(
                    outgoing.at[g, 1, k], target, OUT + number, owners[half][k], S_OUT + 2 * g + k
                ).start()

            @pl.when(own)
            def _():
                pltpu.make_async_copy(
                    outgoing.at[g, 1, k], target, local_sem.at[10 + g % 2]
                ).start()

    def first_hooks(b, blocks):
        @pl.when(b == 0)
        def _():
            with jax.named_scope("relay_u"):
                for q in (2, 1, 3):
                    relay(q, upper)
                start_w()

    def last_in_u():
        with jax.named_scope("last_in_u"):
            for q in (0, 2, 1, 3):
                last_in(q, upper)

    def second_hooks(b, blocks):
        @pl.when((b == jnp.minimum(2, blocks)) & (blocks > 0))
        def _():
            with jax.named_scope("stage1_0"):
                stage1(0)
            last_in_u()

    def late_hooks(b, blocks):
        @pl.when((b == 0) & (shard[0] < reach))
        def _():
            with jax.named_scope("stage1_0"):
                stage1(0)
            last_in_u()

        @pl.when(b == 1)
        def _():
            with jax.named_scope("stage1_1"):
                stage1(1)

        @pl.when(b == 4)
        def _():
            with jax.named_scope("pair_in_u"):
                pair_in(upper)

        @pl.when(b == blocks - 1)
        def _():
            with jax.named_scope("stage23_0"):
                stage2(0)
                stage3(0)
                w_relay(0)
                w_relay(1)

        @pl.when(b == blocks)
        def _():
            with jax.named_scope("stage23_1"):
                stage2(1)
                stage3(1)

    with jax.named_scope("attend_low"):
        attend(0, first_hooks, 0, PER)
    with jax.named_scope("values"):
        values_low(0)
    with jax.named_scope("attend_low"):
        attend(0, second_hooks, PER, PER)
    with jax.named_scope("values"):
        values_low(1)
    with jax.named_scope("attend_high"):
        attend(1, late_hooks, 0, HEADS)
    with jax.named_scope("values"):
        values_high()
    with jax.named_scope("stage4_0"):
        stage4(0)
    with jax.named_scope("stage1_23"):
        stage1(2)
        stage1(3)
    with jax.named_scope("stage4_1"):
        stage4(1)
    with jax.named_scope("w_middle"):
        w_middle()
    with jax.named_scope("stage2_2"):
        stage2(2)
    with jax.named_scope("stage2_3"):
        stage2(3)
    with jax.named_scope("stage3_2"):
        stage3(2)
    with jax.named_scope("stage3_3"):
        stage3(3)
    with jax.named_scope("w_last"):
        w_last()
    with jax.named_scope("stage4_2"):
        stage4(2)
    with jax.named_scope("stage5_0"):
        stage5(0)
    with jax.named_scope("stage5_1"):
        stage5(1)
    with jax.named_scope("stage4_3"):
        stage4(3)
    with jax.named_scope("w_all"):
        w_all()
    with jax.named_scope("product_low"):
        product_low()
    with jax.named_scope("half_out_low"):
        half_out(0)
        half_out(1)
    with jax.named_scope("stage5_2"):
        stage5(2)
    with jax.named_scope("product_2"):
        product_high(0)
    with jax.named_scope("half_out_2"):
        half_out(2)
    with jax.named_scope("stage5_3"):
        stage5(3)
    with jax.named_scope("product_3"):
        product_high(1)
    with jax.named_scope("half_out_3"):
        half_out(3)
    with jax.named_scope("whole_out_low"):
        whole_out(0)
        whole_out(1)
    with jax.named_scope("whole_out_2"):
        whole_out(2)
    with jax.named_scope("whole_out_3"):
        whole_out(3)

    with jax.named_scope("finish"):
        for n in range(8):
            r, k = n // 4, n % 4
            piece = out_ref.at[:, 2 * (k // 2) + r, :, (k % 2) * 896 : (k % 2 + 1) * 896]
            self_made = (mine == 1) & (makers[k][1] == z) & (k // 2 == c)

            @pl.when(jnp.logical_not(self_made))
            def _(n=n, piece=piece):
                copy(piece, piece, OUT + n, partner).wait_recv()

            @pl.when(self_made)
            def _(r=r, piece=piece):
                pltpu.make_async_copy(outgoing.at[0, 1, 0], piece, local_sem.at[10 + r]).wait()

    with jax.named_scope("drain"):

        def sent(ref, leaving):
            copy(ref, ref, 0, partner, leaving).wait_send()

        sent(keys.at[0, 0], S_CROSS)
        sent(qx.at[0], S_SWAP)
        sent(keys.at[pl.ds(0, 15)], S_KEYS)
        sent(keys.at[pl.ds(0, 16)], S_PAIR)
        sent(wg.at[0, pl.ds(0, 3)], S_W)
        sent(wg.at[0], S_WPAIR)
        sent(low_stage, S_APAIR)
        sent(summand, S_XSUM)
        for g in range(CHUNKS):
            sent(low.at[pl.ds(0, 7), 0], S_A + g)
        for g in range(CHUNKS):
            for k in range(2):
                own = (mine == 1) & (xh == g // 2) & (z == 2 * xl + k)

                @pl.when(jnp.logical_not(own))
                def _(g=g, k=k):
                    sent(summand.at[0, 0], S_OUT + 2 * g + k)


def local(q_latent, kv_latent, kv_gain, w_q_b, w_kv_b, w_o, prompt_len, response_mask):
    frequency = 10000.0 ** (-np.arange(ROPE // 2, dtype=np.float64) * 2.0 / ROPE)
    fine = np.arange(HALF, dtype=np.float64)[:, None] * np.tile(frequency, 2)[None, :]
    table = np.stack([np.cos(fine), np.sin(fine), np.cos(HALF * fine), np.sin(HALF * fine)])
    hbm = pl.BlockSpec(memory_space=pltpu.HBM)
    bf16 = jnp.bfloat16
    result = pl.pallas_call(
        body,
        out_shape=jax.ShapeDtypeStruct((2, 4, ROWS, 1792), bf16),
        in_specs=[hbm] * 5 + [pl.BlockSpec(memory_space=pltpu.SMEM)] + [hbm] * 3,
        out_specs=hbm,
        scratch_shapes=[
            pltpu.SemaphoreType.DMA((NSENT,)),
            pltpu.SemaphoreType.DMA((NSEM,)),
            pltpu.SemaphoreType.DMA((17,)),
            pltpu.VMEM((WIDE, 128), bf16),
            pltpu.VMEM((1, KVR), jnp.float32),
            pltpu.VMEM((4, HALF, ROPE), jnp.float32),
            pltpu.VMEM((32, 128), jnp.int32),
            pltpu.VMEM((2, 2, HALF // 2, 1536), bf16),
            pltpu.VMEM((8, 1536, 384), bf16),
            pltpu.VMEM((512, 4096), bf16),
            pltpu.VMEM((32, 2, HALF, WIDE), bf16),
            pltpu.VMEM((2, HEADS, HALF, WIDE), bf16),
            pltpu.VMEM((HEADS, HALF, KVR), bf16),
            pltpu.VMEM((2, 2, 2 * ROWS, PER * VD), bf16),
            pltpu.VMEM((2, 2, ROWS, HEADS * VD), bf16),
            pltpu.VMEM((8, 2, 2, 2 * ROWS, PER * VD), bf16),
            pltpu.VMEM((8, 2, 2, ROWS, HEADS * VD), bf16),
            pltpu.VMEM((2, 4, 224, 2048), bf16),
            pltpu.VMEM((CHUNKS, 8, ROWS, 4 * 224), jnp.float32),
            pltpu.VMEM((CHUNKS, 2, 2, 2, ROWS, 4 * 224), bf16),
            pltpu.VMEM((CHUNKS, 2, 2, ROWS, 4 * 224), bf16),
            pltpu.VMEM((4096 // BLOCK, BLOCK), jnp.float32),
            pltpu.VMEM((HEADS * HALF, 128), jnp.float32),
            pltpu.VMEM((HEADS * HALF, 128), jnp.float32),
            pltpu.VMEM((HEADS * HALF, KVR), jnp.float32),
        ],
        compiler_params=pltpu.CompilerParams(
            collective_id=0, has_side_effects=True, vmem_limit_bytes=67000000
        ),
        cost_estimate=pl.CostEstimate(
            flops=20_000_000_000, bytes_accessed=16_000_000, transcendentals=0
        ),
        name="layer",
    )(
        q_latent.reshape(2, 2, HALF // 2, 1536),
        kv_latent.T,
        kv_gain.reshape(1, -1),
        jnp.asarray(table, jnp.float32),
        response_mask.reshape(32, 128),
        prompt_len,
        w_q_b,
        w_kv_b,
        w_o.T,
    )
    return result.reshape(128, 1792)


def solution(mesh):
    finer = Mesh(mesh.devices.reshape(2, 4, 4, 2, 2), AXES)
    placed = (
        P(DP, None),
        P(DP, None),
        P(),
        P(None, HEAD),
        P(None, HEAD),
        P(HEAD, DP),
        P(),
        P(),
    )
    return jax.shard_map(
        local, mesh=finer, in_specs=placed, out_specs=P(DP, HEAD), check_vma=False
    )
```

```python
import functools
import math

import jax
import jax.numpy as jnp
import numpy as np
from jax import lax
from jax.experimental import pallas as pl
from jax.experimental.pallas import tpu as pltpu
from jax.sharding import Mesh
from jax.sharding import PartitionSpec as P

KVR = 512
ROPE = 64
NOPE = 128
VD = 128
WIDE = KVR + ROPE
AXES = ("xh", "z", "y", "xl", "c")
DP = ("xh", "z", "y")
HEAD = ("xl", "c")
MESH = pl.DeviceIdType.MESH

HEADS = 16
PER = 8
CHUNKS = 4
HALF = 64
ROWS = 16
BLOCK = 512
LOG2E = 1.4426950408889634
EPS = 1e-06

CROSS = 0
SWAP = 1
SWAP2 = 2
D1 = 3
FAR = 7
D2 = 9
D2H = 25
PAIR = 33
WFULL = 35
WHALF = 39
WPAIR = 40
ABASE = 44
APAIR, AX, AZ, AZH, AX2 = 0, 1, 2, 6, 7
ASTRIDE = 8
OUT = ABASE + ASTRIDE * CHUNKS
XSUM = OUT + 8
NSEM = XSUM + 8
S_CROSS, S_SWAP, S_KEYS, S_PAIR, S_W, S_WPAIR, S_APAIR, S_XSUM, S_A, S_OUT = 0, 1, 2, 3, 4, 5, 6, 7, 8, 12
NSENT = S_OUT + 8


def turn(values, cosine, sine):
    swapped = jnp.concatenate([values[:, ROPE // 2 :], values[:, : ROPE // 2]], axis=1)
    return values * cosine + swapped * sine


def body(
    q_hbm,
    kv_hbm,
    gain_hbm,
    table_hbm,
    live_hbm,
    prompt,
    wq_hbm,
    wkv_hbm,
    wo_hbm,
    out_ref,
    out_sem,
    in_sem,
    local_sem,
    kv_lat,
    gain,
    table,
    live,
    qx,
    wq,
    wkv,
    keys,
    qs,
    ctx,
    low_stage,
    high_stage,
    low,
    high,
    wg,
    part,
    outgoing,
    summand,
    bias,
    m_ref,
    l_ref,
    acc_ref,
):
    xh, z, y, xl, c = (lax.axis_index(a) for a in AXES)
    d1 = y + c * (z - y)
    d2 = z + c * (y - z)

    def place(t, o1, o2):
        a = lax.rem(d1 + o1 + 4, 4)
        b = lax.rem(d2 + o2 + 4, 4)
        zz = b + c * (a - b)
        yy = a + c * (b - a)
        xx = xh + t - 2 * xh * t
        return xx, zz, yy

    def unit(t, o1, o2):
        xx, zz, yy = place(t, o1, o2)
        return xx * 16 + zz * 4 + yy

    def near(o1, o2):
        _, zz, yy = place(0, o1, o2)
        return (xh, zz, yy, xl, c)

    def copy(src, dst, number, device, leaving=0):
        return pltpu.make_async_remote_copy(
            src_ref=src,
            dst_ref=dst,
            send_sem=out_sem.at[leaving],
            recv_sem=in_sem.at[number],
            device_id=device,
            device_id_type=MESH,
        )

    me = unit(0, 0, 0)
    partner = (xh, z, y, xl, 1 - c)
    cross = (1 - xh, z, y, 1 - xl, c)
    swap_peer = (1 - xh, 3 - z, y, 1 - xl, c)
    across = (1 - xh, z, y, xl, c)
    up_y = (xh, z, lax.rem(y + 1, 4), xl, c)
    down_y = (xh, z, lax.rem(y + 3, 4), xl, c)
    up_z = (xh, lax.rem(z + 1, 4), y, xl, c)
    down_z = (xh, lax.rem(z + 3, 4), y, xl, c)
    owners = [[(t, 2 * xl + k, y, xh, z // 2) for k in range(2)] for t in range(2)]
    makers = [(xl, 2 * c + k % 2, y, z // 2, k // 2) for k in range(4)]
    beside = (xh, z, y, 1 - xl, c)
    same = lambda u, v: 1 - jnp.minimum((u - v) * (u - v), 1)
    mine = same(c, xh) * same(xl, xh) * same(z // 2, c)
    z_low = z + xh * (3 - 2 * z)
    shard = (z_low * 4 + y, 16 + (3 - z_low) * 4 + y)

    barrier = pltpu.get_barrier_semaphore()
    far = near(2, 0)
    for peer in (partner, cross, swap_peer, across, beside, far, up_y, down_y, up_z, down_z):
        pl.semaphore_signal(barrier, inc=1, device_id=peer, device_id_type=MESH)
    for k in range(4):

        @pl.when((mine == 0) | (makers[k][1] != z) | (k // 2 != c))
        def _(k=k):
            pl.semaphore_signal(barrier, inc=1, device_id=makers[k], device_id_type=MESH)

    inputs = ((kv_hbm, kv_lat), (gain_hbm, gain), (table_hbm, table), (live_hbm, live))
    for n, (far_away, close) in enumerate(inputs):
        pltpu.make_async_copy(far_away, close, local_sem.at[12 + n]).start()
    own_rows = pltpu.make_async_copy(q_hbm.at[xh], qx.at[xh], local_sem.at[16])
    own_rows.start()
    pltpu.make_async_copy(wkv_hbm, wkv, local_sem.at[8]).start()
    for j in range(8):
        pltpu.make_async_copy(wq_hbm.at[:, pl.ds(j * 384, 384)], wq.at[j], local_sem.at[j]).start()
    pltpu.make_async_copy(wo_hbm, wg.at[c, y], local_sem.at[9]).start()

    with jax.named_scope("norm"):
        for n, (far_away, close) in enumerate(inputs):
            pltpu.make_async_copy(far_away, close, local_sem.at[12 + n]).wait()
        lane = lax.broadcasted_iota(jnp.int32, (1, ROPE), 1)
        sign = jnp.where(lane < ROPE // 2, -1.0, 1.0)

        def angles(m):
            cos_a, sin_a = table[2, pl.ds(m, 1), :], table[3, pl.ds(m, 1), :]
            cos_b, sin_b = table[0], table[1]
            return cos_a * cos_b - sin_a * sin_b, (sin_a * cos_b + cos_a * sin_b) * sign

        turned_rows = kv_lat[...].astype(jnp.float32).T
        rows = jnp.where(c == 0, turned_rows[:HALF], turned_rows[HALF:])
        latent = rows[:, :KVR]
        inverse = lax.rsqrt(jnp.mean(latent * latent, axis=-1, keepdims=True) + EPS)
        keys[me, c, :, :KVR] = (latent * inverse * gain[...]).astype(jnp.bfloat16)
        keys[me, c, :, KVR:] = turn(rows[:, KVR:], *angles(me * 2 + c)).astype(jnp.bfloat16)
        spot = lax.broadcasted_iota(jnp.int32, (32, 128), 0) * 128 + lax.broadcasted_iota(
            jnp.int32, (32, 128), 1
        )
        usable = (spot < prompt[0]) | (live[...] == 1)
        masked = jnp.where(usable, 0.0, -1e30)
        for r in range(32):
            b, at = r // (BLOCK // 128), r % (BLOCK // 128)
            bias[b : b + 1, at * 128 : (at + 1) * 128] = masked[r : r + 1]

    with jax.named_scope("barrier"):
        pl.semaphore_wait(barrier, 14 - mine)

    def key(t, o1, o2, which=None):
        ref = keys.at[unit(t, o1, o2), c]
        if which is None:
            return ref
        return ref.at[pl.ds(32 * which, 32)]

    def key_copy(number, t, o1, o2, device, which=None, leaving=S_KEYS):
        ref = key(t, o1, o2, which)
        return copy(ref, ref, number, device, leaving)

    offsets = (0, 1, 3, 2)
    lower, upper = xh, 1 - xh

    def spread(q, t):
        k, o = 2 * q + t, offsets[q]
        key_copy(D2 + 2 * k, t, o, 0, near(0, 1)).start()
        key_copy(D2 + 2 * k + 1, t, o, 0, near(0, -1)).start()
        key_copy(PAIR + t, t, o, 0, partner, leaving=S_PAIR).start()

    def first_out(t):
        key_copy(D1 + 2 * t, t, 0, 0, near(1, 0)).start()
        key_copy(D1 + 2 * t + 1, t, 0, 0, near(-1, 0)).start()
        spread(0, t)
        key_copy(FAR + t, t, 0, 0, far).start()

    def first_in(t):
        key_copy(D1 + 2 * t, t, -1, 0, near(1, 0)).wait_recv()
        spread(2, t)
        key_copy(D1 + 2 * t + 1, t, 1, 0, near(-1, 0)).wait_recv()
        spread(1, t)

    def far_in(t):
        key_copy(FAR + t, t, 2, 0, far).wait_recv()
        spread(3, t)

    def cross_in():
        key_copy(CROSS, 1, 0, 0, cross).wait_recv()

    with jax.named_scope("spread"):
        key_copy(CROSS, 0, 0, 0, cross, leaving=S_CROSS).start()
        copy(q_hbm.at[1 - xh, c], qx.at[xh, c], SWAP, swap_peer, S_SWAP).start()
        pl.when(xh == 1)(cross_in)
        first_out(lower)
        pl.when(xh == 0)(cross_in)
        first_out(upper)

    tables = [angles(2 * where + xh) for where in shard]

    def project(j):
        pltpu.make_async_copy(
            wq_hbm.at[:, pl.ds(0, 384)], wq.at[j], local_sem.at[j]
        ).wait()
        both = jnp.dot(
            qx[...].reshape(2 * HALF, 1536), wq[j], preferred_element_type=jnp.float32
        ).astype(jnp.bfloat16)
        for e in range(2):
            h = 2 * j + e
            plain = both[:, e * 192 : e * 192 + NOPE]
            roped = both[:, e * 192 + NOPE : (e + 1) * 192].astype(jnp.float32)
            w_key = wkv[:, pl.ds(pl.multiple_of(h * 256, 256), NOPE)]
            absorbed = lax.dot_general(
                plain, w_key, (((1,), (1,)), ((), ())), preferred_element_type=jnp.float32
            ).astype(jnp.bfloat16)
            for half in range(2):
                mine_rows = slice(half * HALF, (half + 1) * HALF)
                qs[half, h, :, :KVR] = absorbed[mine_rows]
                qs[half, h, :, KVR:] = turn(roped[mine_rows], *tables[half]).astype(jnp.bfloat16)

    def relay(q, t):
        k, o = 2 * q + t, offsets[q]
        key_copy(D2 + 2 * k, t, o, -1, near(0, 1)).wait_recv()
        key_copy(D2H + k, t, o, -1, near(0, 1), 0).start()
        key_copy(PAIR + t, t, o, -1, partner, leaving=S_PAIR).start()
        key_copy(D2 + 2 * k + 1, t, o, 1, near(0, -1)).wait_recv()
        key_copy(D2H + k, t, o, 1, near(0, -1), 1).start()
        key_copy(PAIR + t, t, o, 1, partner, leaving=S_PAIR).start()

    def last_in(q, t):
        k, o = 2 * q + t, offsets[q]
        key_copy(D2H + k, t, o, 2, near(0, 1)).wait_recv()
        key_copy(PAIR + t, t, o, 2, partner, leaving=S_PAIR).start()

    def pair_in(t):
        ref = keys.at[pl.ds(0, 16), 1 - c]
        copy(ref, ref, PAIR + t, partner).wait_recv()

    span = wo_hbm.shape[0] // 2

    def w_copy(number, row, device, which):
        ref = wg.at[c, row, pl.ds(which * span, span)]
        return copy(ref, ref, number, device, S_W)

    def w_pair(row, number):
        return copy(wg.at[c, row], wg.at[c, row], WPAIR + number, partner, S_WPAIR)

    def w_pair_in(row, number):
        return copy(wg.at[1 - c, row], wg.at[1 - c, row], WPAIR + number, partner)

    def project_in(*order):
        with jax.named_scope("project"):
            for j in order:
                project(j)

    def start_w():
        pltpu.make_async_copy(wo_hbm, wg.at[c, y], local_sem.at[9]).wait()
        for which in range(2):
            w_copy(WFULL + which, y, up_y, which).start()
            w_copy(WFULL + 3 - which, y, down_y, 1 - which).start()
        w_pair(y, 0).start()

    def swap_on():
        copy(qx.at[1 - xh, c], qx.at[1 - xh, c], SWAP, swap_peer).wait_recv()
        copy(qx.at[1 - xh, c], qx.at[1 - xh, c], SWAP2, partner, S_SWAP).start()

    with jax.named_scope("swap"):
        pl.when(xh == 1)(swap_on)
    with jax.named_scope("first_in_l"):
        first_in(lower)
    with jax.named_scope("relay_l0"):
        relay(0, lower)
    with jax.named_scope("far_l"):
        far_in(lower)
    with jax.named_scope("swap"):
        pl.when(xh == 0)(swap_on)
    with jax.named_scope("swap2"):
        own_rows.wait()
        pltpu.make_async_copy(wkv_hbm, wkv, local_sem.at[8]).wait()
        copy(qx.at[1 - xh, 1 - c], qx.at[1 - xh, 1 - c], SWAP2, partner).wait_recv()
    project_in(0, 1, 2)
    with jax.named_scope("relay_l21"):
        relay(2, lower)
        relay(1, lower)
    project_in(3)
    with jax.named_scope("relay_l3"):
        relay(3, lower)
    with jax.named_scope("first_in_u"):
        first_in(upper)
    project_in(4)
    with jax.named_scope("far_u"):
        far_in(upper)
    with jax.named_scope("last_in_l"):
        for q in (0, 2, 1):
            last_in(q, lower)
    project_in(5)
    with jax.named_scope("last_in_l3"):
        last_in(3, lower)
    with jax.named_scope("relay_u0"):
        relay(0, upper)
    project_in(6, 7)
    with jax.named_scope("pair_in_l"):
        pair_in(lower)

    scale = LOG2E / math.sqrt(NOPE + ROPE)
    reach = BLOCK // 128

    def attend(half, hooks, first, count):
        where = shard[half]
        blocks = where // reach
        tile_rows = count * HALF
        upto = pl.ds(0, tile_rows)
        m_ref[upto] = jnp.full((tile_rows, 128), -1e30, jnp.float32)
        l_ref[upto] = jnp.zeros((tile_rows, 128), jnp.float32)
        acc_ref[upto] = jnp.zeros((tile_rows, KVR), jnp.float32)

        def step(b, causal):
            block = keys[pl.ds(b * reach, reach)].reshape(BLOCK, WIDE)
            scores = lax.dot_general(
                qs[half, first : first + count].reshape(tile_rows, WIDE),
                block,
                (((1,), (1,)), ((), ())),
                preferred_element_type=jnp.float32,
            )
            scores = scores * scale + bias[pl.ds(b, 1), :]
            if causal is not None:
                scores = (scores.reshape(count, HALF, BLOCK) + causal[None]).reshape(
                    tile_rows, BLOCK
                )
            before = m_ref[upto]
            m_new = jnp.maximum(before, jnp.max(scores, axis=1, keepdims=True))
            alpha = jnp.exp2(before - m_new)
            lifted = jnp.exp2(scores - jnp.concatenate([m_new] * (BLOCK // 128), axis=1))
            total = l_ref[upto] * alpha
            for k in range(BLOCK // 128):
                total = total + lifted[:, k * 128 : (k + 1) * 128]
            l_ref[upto] = total
            m_ref[upto] = m_new
            acc_ref[upto] = acc_ref[upto] * jnp.concatenate([alpha] * (KVR // 128), axis=1) + jnp.dot(
                lifted.astype(jnp.bfloat16), block[:, :KVR], preferred_element_type=jnp.float32
            )

        def open_step(b, carry):
            hooks(b, blocks)
            step(b, None)
            return carry

        lax.fori_loop(0, blocks, open_step, 0)
        hooks(blocks, blocks)
        token = where * 128 + xh * HALF + lax.broadcasted_iota(jnp.int32, (HALF, BLOCK), 0)
        position = blocks * BLOCK + lax.broadcasted_iota(jnp.int32, (HALF, BLOCK), 1)
        step(blocks, jnp.where(position <= token, 0.0, -1e30))
        total = jnp.sum(l_ref[upto], axis=1, keepdims=True)
        ctx[:count] = (acc_ref[upto] / total).astype(jnp.bfloat16).reshape(count, HALF, KVR)

    here = xh * 4 + z

    def value_rows(h, at):
        w_value = wkv[:, h * 256 + NOPE : (h + 1) * 256]
        return jnp.dot(ctx[at], w_value, preferred_element_type=jnp.float32).astype(jnp.bfloat16)

    def values_low(g):
        for n in range(PER):
            attended = value_rows(g * PER + n, n)
            for to in range(2):
                low_stage[g, to, :, n * VD : (n + 1) * VD] = attended[
                    to * 2 * ROWS : (to + 1) * 2 * ROWS
                ]
        pair_copy(g).start()
        low[here, g, c] = low_stage[g, c]

    def values_high():
        for h in range(HEADS):
            attended = value_rows(h, h)
            for r in range(2):
                for to in range(2):
                    at = to * 2 * ROWS + r * ROWS
                    high_stage[r, to, :, h * VD : (h + 1) * VD] = attended[at : at + ROWS]
        for r in range(2):
            pair_copy(2 + r).start()
            high[here, r, c] = high_stage[r, c]

    def block_of(slot, g):
        return low.at[slot, g] if g < 2 else high.at[slot, g - 2]

    def a_copy(g, number, t, o, device, which=None):
        slot = (xh + t - 2 * xh * t) * 4 + lax.rem(z + o + 4, 4)
        ref = block_of(slot, g)
        if which is not None:
            ref = ref.at[which]
        return copy(ref, ref, ABASE + ASTRIDE * g + number, device, S_A + g)

    def pair_copy(g):
        staged = low_stage.at[g, 1 - c] if g < 2 else high_stage.at[g - 2, 1 - c]
        return copy(
            staged, block_of(here, g).at[c], ABASE + ASTRIDE * g + APAIR, partner, S_APAIR
        )

    def pair_copy_in(g):
        ref = block_of(here, g).at[1 - c]
        return copy(ref, ref, ABASE + ASTRIDE * g + APAIR, partner, S_APAIR)

    def stage1(g):
        pair_copy_in(g).wait_recv()
        a_copy(g, AX, 0, 0, across).start()
        a_copy(g, AZ, 0, 0, up_z).start()
        a_copy(g, AZ + 1, 0, 0, down_z).start()

    def stage2(g):
        a_copy(g, AZ, 0, -1, up_z).wait_recv()
        a_copy(g, AZH, 0, -1, up_z, 0).start()
        a_copy(g, AZ + 1, 0, 1, down_z).wait_recv()
        a_copy(g, AZH, 0, 1, down_z, 1).start()

    def stage3(g):
        a_copy(g, AX, 1, 0, across).wait_recv()
        a_copy(g, AZ + 2, 1, 0, up_z).start()
        a_copy(g, AZ + 3, 1, 0, down_z).start()

    def stage4(g):
        a_copy(g, AZH, 0, 2, up_z).wait_recv()
        a_copy(g, AX2, 0, 2, across).start()

    def stage5(g):
        a_copy(g, AZ + 2, 1, -1, up_z).wait_recv()
        a_copy(g, AZ + 3, 1, 1, down_z).wait_recv()
        a_copy(g, AX2, 1, 2, across).wait_recv()

    def w_relay(which):
        if which == 0:
            w_copy(WFULL, lax.rem(y + 3, 4), up_y, 0).wait_recv()
            w_copy(WHALF, lax.rem(y + 3, 4), up_y, 0).start()
        else:
            w_copy(WFULL + 3, lax.rem(y + 1, 4), down_y, 1).wait_recv()
            w_copy(WHALF, lax.rem(y + 1, 4), down_y, 1).start()

    def w_middle():
        w_copy(WFULL + 1, lax.rem(y + 3, 4), up_y, 1).wait_recv()
        w_pair(lax.rem(y + 3, 4), 1).start()
        w_copy(WFULL + 2, lax.rem(y + 1, 4), down_y, 0).wait_recv()
        w_pair(lax.rem(y + 1, 4), 2).start()

    def w_last():
        ref = wg.at[c, lax.rem(y + 2, 4)]
        copy(ref, ref, WHALF, up_y).wait_recv()
        w_pair(lax.rem(y + 2, 4), 3).start()

    def w_all():
        for k, o in enumerate((0, 3, 1, 2)):
            w_pair_in(lax.rem(y + o, 4), k).wait_recv()

    def multiplied(rows, weights):
        return lax.dot_general(
            rows, weights, (((1,), (1,)), ((), ())), preferred_element_type=jnp.float32
        )

    def product_low():
        rows, depth = 16 * ROWS, PER * VD
        total = jnp.zeros((rows, 4 * 224), jnp.float32)
        for g in range(2):
            for core in range(2):
                total = total + multiplied(
                    low[:, g, core].reshape(rows, depth),
                    wg[core, :, :, g * depth : (g + 1) * depth].reshape(4 * 224, depth),
                )
        total = total.reshape(8, 2 * ROWS, 4 * 224)
        for n in range(2):
            part[n] = total[:, n * ROWS : (n + 1) * ROWS]

    def product_high(r):
        rows = 8 * ROWS
        total = jnp.zeros((rows, 4 * 224), jnp.float32)
        for core in range(2):
            total = total + multiplied(
                high[:, r, core].reshape(rows, HEADS * VD),
                wg[core].reshape(4 * 224, HEADS * VD),
            )
        part[2 + r] = total.reshape(8, ROWS, 4 * 224)

    def slots(half, k):
        straight, mirrored = k, 3 - k
        first = straight if half == 0 else mirrored
        return first, 4 + 3 - first

    def half_out(g):
        for k in range(2):
            for xs, at in enumerate(slots(g // 2, 2 * (1 - xl) + k)):
                outgoing[g, 0, k, xs] = part[g, at].astype(jnp.bfloat16)
            copy(
                outgoing.at[g, 0, k], summand.at[g, k], XSUM + 2 * g + k, beside, S_XSUM
            ).start()

    def whole_out(g):
        half = g // 2
        number = lax.rem(z, 2) + 2 * c + 4 * (g % 2)
        for k in range(2):
            row = 2 * xl + k
            copy(outgoing.at[g, 0, k], summand.at[g, k], XSUM + 2 * g + k, beside).wait_recv()
            for xs, at in enumerate(slots(half, row)):
                outgoing[g, 1, k, xs] = (
                    part[g, at] + summand[g, k, xs].astype(jnp.float32)
                ).astype(jnp.bfloat16)
            own = (mine == 1) & (xh == half) & (z == row)
            target = out_ref.at[:, 2 * c + g % 2, :, pl.ds(lax.rem(z, 2) * 896, 896)]

            @pl.when(jnp.logical_not(own))
            def _():
                copy(
                    outgoing.at[g, 1, k], target, OUT + number, owners[half][k], S_OUT + 2 * g + k
                ).start()

            @pl.when(own)
            def _():
                pltpu.make_async_copy(
                    outgoing.at[g, 1, k], target, local_sem.at[10 + g % 2]
                ).start()

    def first_hooks(b, blocks):
        @pl.when(b == 0)
        def _():
            with jax.named_scope("relay_u"):
                for q in (2, 1, 3):
                    relay(q, upper)
                start_w()

    def last_in_u():
        with jax.named_scope("last_in_u"):
            for q in (0, 2, 1, 3):
                last_in(q, upper)

    def second_hooks(b, blocks):
        @pl.when((b == jnp.minimum(2, blocks)) & (blocks > 0))
        def _():
            with jax.named_scope("stage1_0"):
                stage1(0)
            last_in_u()

    def late_hooks(b, blocks):
        @pl.when((b == 0) & (shard[0] < reach))
        def _():
            with jax.named_scope("stage1_0"):
                stage1(0)
            last_in_u()

        @pl.when(b == 1)
        def _():
            with jax.named_scope("stage1_1"):
                stage1(1)

        @pl.when(b == 4)
        def _():
            with jax.named_scope("pair_in_u"):
                pair_in(upper)

        @pl.when(b == blocks - 1)
        def _():
            with jax.named_scope("stage23_0"):
                stage2(0)
                stage3(0)
                w_relay(0)
                w_relay(1)

        @pl.when(b == blocks)
        def _():
            with jax.named_scope("stage23_1"):
                stage2(1)
                stage3(1)

    with jax.named_scope("attend_low"):
        attend(0, first_hooks, 0, PER)
    with jax.named_scope("values"):
        values_low(0)
    with jax.named_scope("attend_low"):
        attend(0, second_hooks, PER, PER)
    with jax.named_scope("values"):
        values_low(1)
    with jax.named_scope("attend_high"):
        attend(1, late_hooks, 0, HEADS)
    with jax.named_scope("values"):
        values_high()
    with jax.named_scope("stage4_0"):
        stage4(0)
    with jax.named_scope("stage1_23"):
        stage1(2)
        stage1(3)
    with jax.named_scope("stage4_1"):
        stage4(1)
    with jax.named_scope("w_middle"):
        w_middle()
    with jax.named_scope("stage2_2"):
        stage2(2)
    with jax.named_scope("stage2_3"):
        stage2(3)
    with jax.named_scope("stage3_2"):
        stage3(2)
    with jax.named_scope("stage3_3"):
        stage3(3)
    with jax.named_scope("w_last"):
        w_last()
    with jax.named_scope("stage4_2"):
        stage4(2)
    with jax.named_scope("stage5_0"):
        stage5(0)
    with jax.named_scope("stage5_1"):
        stage5(1)
    with jax.named_scope("stage4_3"):
        stage4(3)
    with jax.named_scope("w_all"):
        w_all()
    with jax.named_scope("product_low"):
        product_low()
    with jax.named_scope("half_out_low"):
        half_out(0)
        half_out(1)
    with jax.named_scope("stage5_2"):
        stage5(2)
    with jax.named_scope("product_2"):
        product_high(0)
    with jax.named_scope("half_out_2"):
        half_out(2)
    with jax.named_scope("stage5_3"):
        stage5(3)
    with jax.named_scope("product_3"):
        product_high(1)
    with jax.named_scope("half_out_3"):
        half_out(3)
    with jax.named_scope("whole_out_low"):
        whole_out(0)
        whole_out(1)
    with jax.named_scope("whole_out_2"):
        whole_out(2)
    with jax.named_scope("whole_out_3"):
        whole_out(3)

    with jax.named_scope("finish"):
        for n in range(8):
            r, k = n // 4, n % 4
            piece = out_ref.at[:, 2 * (k // 2) + r, :, (k % 2) * 896 : (k % 2 + 1) * 896]
            self_made = (mine == 1) & (makers[k][1] == z) & (k // 2 == c)

            @pl.when(jnp.logical_not(self_made))
            def _(n=n, piece=piece):
                copy(piece, piece, OUT + n, partner).wait_recv()

            @pl.when(self_made)
            def _(r=r, piece=piece):
                pltpu.make_async_copy(outgoing.at[0, 1, 0], piece, local_sem.at[10 + r]).wait()

    with jax.named_scope("drain"):

        def sent(ref, leaving):
            copy(ref, ref, 0, partner, leaving).wait_send()

        sent(keys.at[0, 0], S_CROSS)
        sent(qx.at[0], S_SWAP)
        sent(keys.at[pl.ds(0, 15)], S_KEYS)
        sent(keys.at[pl.ds(0, 16)], S_PAIR)
        sent(wg.at[0, pl.ds(0, 3)], S_W)
        sent(wg.at[0], S_WPAIR)
        sent(low_stage, S_APAIR)
        sent(summand, S_XSUM)
        for g in range(CHUNKS):
            sent(low.at[pl.ds(0, 7), 0], S_A + g)
        for g in range(CHUNKS):
            for k in range(2):
                own = (mine == 1) & (xh == g // 2) & (z == 2 * xl + k)

                @pl.when(jnp.logical_not(own))
                def _(g=g, k=k):
                    sent(summand.at[0, 0], S_OUT + 2 * g + k)


def local(q_latent, kv_latent, kv_gain, w_q_b, w_kv_b, w_o, prompt_len, response_mask):
    frequency = 10000.0 ** (-np.arange(ROPE // 2, dtype=np.float64) * 2.0 / ROPE)
    fine = np.arange(HALF, dtype=np.float64)[:, None] * np.tile(frequency, 2)[None, :]
    table = np.stack([np.cos(fine), np.sin(fine), np.cos(HALF * fine), np.sin(HALF * fine)])
    hbm = pl.BlockSpec(memory_space=pltpu.HBM)
    bf16 = jnp.bfloat16
    result = pl.pallas_call(
        body,
        out_shape=jax.ShapeDtypeStruct((2, 4, ROWS, 1792), bf16),
        in_specs=[hbm] * 5 + [pl.BlockSpec(memory_space=pltpu.SMEM)] + [hbm] * 3,
        out_specs=hbm,
        scratch_shapes=[
            pltpu.SemaphoreType.DMA((NSENT,)),
            pltpu.SemaphoreType.DMA((NSEM,)),
            pltpu.SemaphoreType.DMA((17,)),
            pltpu.VMEM((WIDE, 128), bf16),
            pltpu.VMEM((1, KVR), jnp.float32),
            pltpu.VMEM((4, HALF, ROPE), jnp.float32),
            pltpu.VMEM((32, 128), jnp.int32),
            pltpu.VMEM((2, 2, HALF // 2, 1536), bf16),
            pltpu.VMEM((8, 1536, 384), bf16),
            pltpu.VMEM((512, 4096), bf16),
            pltpu.VMEM((32, 2, HALF, WIDE), bf16),
            pltpu.VMEM((2, HEADS, HALF, WIDE), bf16),
            pltpu.VMEM((HEADS, HALF, KVR), bf16),
            pltpu.VMEM((2, 2, 2 * ROWS, PER * VD), bf16),
            pltpu.VMEM((2, 2, ROWS, HEADS * VD), bf16),
            pltpu.VMEM((8, 2, 2, 2 * ROWS, PER * VD), bf16),
            pltpu.VMEM((8, 2, 2, ROWS, HEADS * VD), bf16),
            pltpu.VMEM((2, 4, 224, 2048), bf16),
            pltpu.VMEM((CHUNKS, 8, ROWS, 4 * 224), jnp.float32),
            pltpu.VMEM((CHUNKS, 2, 2, 2, ROWS, 4 * 224), bf16),
            pltpu.VMEM((CHUNKS, 2, 2, ROWS, 4 * 224), bf16),
            pltpu.VMEM((4096 // BLOCK, BLOCK), jnp.float32),
            pltpu.VMEM((HEADS * HALF, 128), jnp.float32),
            pltpu.VMEM((HEADS * HALF, 128), jnp.float32),
            pltpu.VMEM((HEADS * HALF, KVR), jnp.float32),
        ],
        compiler_params=pltpu.CompilerParams(
            collective_id=0, has_side_effects=True, vmem_limit_bytes=67000000
        ),
        cost_estimate=pl.CostEstimate(
            flops=20_000_000_000, bytes_accessed=16_000_000, transcendentals=0
        ),
        name="layer",
    )(
        q_latent.reshape(2, 2, HALF // 2, 1536),
        kv_latent.T,
        kv_gain.reshape(1, -1),
        jnp.asarray(table, jnp.float32),
        response_mask.reshape(32, 128),
        prompt_len,
        w_q_b,
        w_kv_b,
        w_o.T,
    )
    return jnp.where(prompt_len[0] > 0, result.reshape(128, 1792), 0)


def solution(mesh):
    finer = Mesh(mesh.devices.reshape(2, 4, 4, 2, 2), AXES)
    placed = (
        P(DP, None),
        P(DP, None),
        P(),
        P(None, HEAD),
        P(None, HEAD),
        P(HEAD, DP),
        P(),
        P(),
    )
    return jax.shard_map(
        local, mesh=finer, in_specs=placed, out_specs=P(DP, HEAD), check_vma=False
    )
```

```python
import functools
import math

import jax
import jax.numpy as jnp
import numpy as np
from jax import lax
from jax.experimental import pallas as pl
from jax.experimental.pallas import tpu as pltpu
from jax.sharding import Mesh
from jax.sharding import PartitionSpec as P

KVR = 512
ROPE = 64
NOPE = 128
VD = 128
WIDE = KVR + ROPE
AXES = ("xh", "z", "y", "xl", "c")
DP = ("xh", "z", "y")
HEAD = ("xl", "c")
MESH = pl.DeviceIdType.MESH

HEADS = 16
PER = 8
CHUNKS = 4
HALF = 64
ROWS = 16
BLOCK = 512
LOG2E = 1.4426950408889634
EPS = 1e-06

CROSS = 0
SWAP = 1
SWAP2 = 2
D1 = 3
FAR = 7
D2 = 9
D2H = 25
PAIR = 33
WFULL = 35
WHALF = 39
WPAIR = 40
ABASE = 44
APAIR, AX, AZ, AZH, AX2 = 0, 1, 2, 6, 7
ASTRIDE = 8
OUT = ABASE + ASTRIDE * CHUNKS
XSUM = OUT + 8
NSEM = XSUM + 8
S_CROSS, S_SWAP, S_KEYS, S_PAIR, S_W, S_WPAIR, S_APAIR, S_XSUM, S_A, S_OUT = 0, 1, 2, 3, 4, 5, 6, 7, 8, 12
NSENT = S_OUT + 8


def turn(values, cosine, sine):
    swapped = jnp.concatenate([values[:, ROPE // 2 :], values[:, : ROPE // 2]], axis=1)
    return values * cosine + swapped * sine


def body(
    q_hbm,
    kv_hbm,
    gain_hbm,
    table_hbm,
    live_hbm,
    prompt,
    wq_hbm,
    wkv_hbm,
    wo_hbm,
    out_ref,
    out_sem,
    in_sem,
    local_sem,
    kv_lat,
    gain,
    table,
    live,
    qx,
    wq,
    wkv,
    keys,
    qs,
    ctx,
    low_stage,
    high_stage,
    low,
    high,
    wg,
    part,
    outgoing,
    summand,
    bias,
    m_ref,
    l_ref,
    acc_ref,
):
    xh, z, y, xl, c = (lax.axis_index(a) for a in AXES)
    d1 = y + c * (z - y)
    d2 = z + c * (y - z)

    def place(t, o1, o2):
        a = lax.rem(d1 + o1 + 4, 4)
        b = lax.rem(d2 + o2 + 4, 4)
        zz = b + c * (a - b)
        yy = a + c * (b - a)
        xx = xh + t - 2 * xh * t
        return xx, zz, yy

    def unit(t, o1, o2):
        xx, zz, yy = place(t, o1, o2)
        return xx * 16 + zz * 4 + yy

    def near(o1, o2):
        _, zz, yy = place(0, o1, o2)
        return (xh, zz, yy, xl, c)

    def copy(src, dst, number, device, leaving=0):
        return pltpu.make_async_remote_copy(
            src_ref=src,
            dst_ref=dst,
            send_sem=out_sem.at[leaving],
            recv_sem=in_sem.at[number],
            device_id=device,
            device_id_type=MESH,
        )

    me = unit(0, 0, 0)
    partner = (xh, z, y, xl, 1 - c)
    cross = (1 - xh, z, y, 1 - xl, c)
    swap_peer = (1 - xh, 3 - z, y, 1 - xl, c)
    across = (1 - xh, z, y, xl, c)
    up_y = (xh, z, lax.rem(y + 1, 4), xl, c)
    down_y = (xh, z, lax.rem(y + 3, 4), xl, c)
    up_z = (xh, lax.rem(z + 1, 4), y, xl, c)
    down_z = (xh, lax.rem(z + 3, 4), y, xl, c)
    owners = [[(t, 2 * xl + k, y, xh, z // 2) for k in range(2)] for t in range(2)]
    makers = [(xl, 2 * c + k % 2, y, z // 2, k // 2) for k in range(4)]
    beside = (xh, z, y, 1 - xl, c)
    same = lambda u, v: 1 - jnp.minimum((u - v) * (u - v), 1)
    mine = same(c, xh) * same(xl, xh) * same(z // 2, c)
    z_low = z + xh * (3 - 2 * z)
    shard = (z_low * 4 + y, 16 + (3 - z_low) * 4 + y)

    barrier = pltpu.get_barrier_semaphore()
    far = near(2, 0)
    for peer in (partner, cross, swap_peer, across, beside, far, up_y, down_y, up_z, down_z):
        pl.semaphore_signal(barrier, inc=1, device_id=peer, device_id_type=MESH)
    for k in range(4):

        @pl.when((mine == 0) | (makers[k][1] != z) | (k // 2 != c))
        def _(k=k):
            pl.semaphore_signal(barrier, inc=1, device_id=makers[k], device_id_type=MESH)

    inputs = ((kv_hbm, kv_lat), (gain_hbm, gain), (table_hbm, table), (live_hbm, live))
    for n, (far_away, close) in enumerate(inputs):
        pltpu.make_async_copy(far_away, close, local_sem.at[12 + n]).start()
    own_rows = pltpu.make_async_copy(q_hbm.at[xh], qx.at[xh], local_sem.at[16])
    own_rows.start()
    pltpu.make_async_copy(wkv_hbm, wkv, local_sem.at[8]).start()
    for j in range(8):
        pltpu.make_async_copy(wq_hbm.at[:, pl.ds(j * 384, 384)], wq.at[j], local_sem.at[j]).start()
    pltpu.make_async_copy(wo_hbm, wg.at[c, y], local_sem.at[9]).start()

    with jax.named_scope("norm"):
        for n, (far_away, close) in enumerate(inputs):
            pltpu.make_async_copy(far_away, close, local_sem.at[12 + n]).wait()
        lane = lax.broadcasted_iota(jnp.int32, (1, ROPE), 1)
        sign = jnp.where(lane < ROPE // 2, -1.0, 1.0)

        def angles(m):
            cos_a, sin_a = table[2, pl.ds(m, 1), :], table[3, pl.ds(m, 1), :]
            cos_b, sin_b = table[0], table[1]
            return cos_a * cos_b - sin_a * sin_b, (sin_a * cos_b + cos_a * sin_b) * sign

        turned_rows = kv_lat[...].astype(jnp.float32).T
        rows = jnp.where(c == 0, turned_rows[:HALF], turned_rows[HALF:])
        latent = rows[:, :KVR]
        inverse = lax.rsqrt(jnp.mean(latent * latent, axis=-1, keepdims=True) + EPS)
        keys[me, c, :, :KVR] = (latent * inverse * gain[...]).astype(jnp.bfloat16)
        keys[me, c, :, KVR:] = turn(rows[:, KVR:], *angles(me * 2 + c)).astype(jnp.bfloat16)
        spot = lax.broadcasted_iota(jnp.int32, (32, 128), 0) * 128 + lax.broadcasted_iota(
            jnp.int32, (32, 128), 1
        )
        usable = (spot < prompt[0]) | (live[...] == 1)
        masked = jnp.where(usable, 0.0, -1e30)
        for r in range(32):
            b, at = r // (BLOCK // 128), r % (BLOCK // 128)
            bias[b : b + 1, at * 128 : (at + 1) * 128] = masked[r : r + 1]

    with jax.named_scope("barrier"):
        pl.semaphore_wait(barrier, 14 - mine)

    def key(t, o1, o2, which=None):
        ref = keys.at[unit(t, o1, o2), c]
        if which is None:
            return ref
        return ref.at[pl.ds(32 * which, 32)]

    def key_copy(number, t, o1, o2, device, which=None, leaving=S_KEYS):
        ref = key(t, o1, o2, which)
        return copy(ref, ref, number, device, leaving)

    offsets = (0, 1, 3, 2)
    lower, upper = xh, 1 - xh

    def spread(q, t):
        k, o = 2 * q + t, offsets[q]
        key_copy(D2 + 2 * k, t, o, 0, near(0, 1)).start()
        key_copy(D2 + 2 * k + 1, t, o, 0, near(0, -1)).start()
        key_copy(PAIR + t, t, o, 0, partner, leaving=S_PAIR).start()

    def first_out(t):
        key_copy(D1 + 2 * t, t, 0, 0, near(1, 0)).start()
        key_copy(D1 + 2 * t + 1, t, 0, 0, near(-1, 0)).start()
        spread(0, t)
        key_copy(FAR + t, t, 0, 0, far).start()

    def first_in(t):
        key_copy(D1 + 2 * t, t, -1, 0, near(1, 0)).wait_recv()
        spread(2, t)
        key_copy(D1 + 2 * t + 1, t, 1, 0, near(-1, 0)).wait_recv()
        spread(1, t)

    def far_in(t):
        key_copy(FAR + t, t, 2, 0, far).wait_recv()
        spread(3, t)

    def cross_in():
        key_copy(CROSS, 1, 0, 0, cross).wait_recv()

    with jax.named_scope("spread"):
        key_copy(CROSS, 0, 0, 0, cross, leaving=S_CROSS).start()
        copy(q_hbm.at[1 - xh, c], qx.at[xh, c], SWAP, swap_peer, S_SWAP).start()
        pl.when(xh == 1)(cross_in)
        first_out(lower)
        pl.when(xh == 0)(cross_in)
        first_out(upper)

    tables = [angles(2 * where + xh) for where in shard]

    def project(j):
        pltpu.make_async_copy(
            wq_hbm.at[:, pl.ds(0, 384)], wq.at[j], local_sem.at[j]
        ).wait()
        both = jnp.dot(
            qx[...].reshape(2 * HALF, 1536), wq[j], preferred_element_type=jnp.float32
        ).astype(jnp.bfloat16)
        for e in range(2):
            h = 2 * j + e
            plain = both[:, e * 192 : e * 192 + NOPE]
            roped = both[:, e * 192 + NOPE : (e + 1) * 192].astype(jnp.float32)
            w_key = wkv[:, pl.ds(pl.multiple_of(h * 256, 256), NOPE)]
            absorbed = lax.dot_general(
                plain, w_key, (((1,), (1,)), ((), ())), preferred_element_type=jnp.float32
            ).astype(jnp.bfloat16)
            for half in range(2):
                mine_rows = slice(half * HALF, (half + 1) * HALF)
                qs[half, h, :, :KVR] = absorbed[mine_rows]
                qs[half, h, :, KVR:] = turn(roped[mine_rows], *tables[half]).astype(jnp.bfloat16)

    def relay(q, t):
        k, o = 2 * q + t, offsets[q]
        key_copy(D2 + 2 * k, t, o, -1, near(0, 1)).wait_recv()
        key_copy(D2H + k, t, o, -1, near(0, 1), 0).start()
        key_copy(PAIR + t, t, o, -1, partner, leaving=S_PAIR).start()
        key_copy(D2 + 2 * k + 1, t, o, 1, near(0, -1)).wait_recv()
        key_copy(D2H + k, t, o, 1, near(0, -1), 1).start()
        key_copy(PAIR + t, t, o, 1, partner, leaving=S_PAIR).start()

    def last_in(q, t):
        k, o = 2 * q + t, offsets[q]
        key_copy(D2H + k, t, o, 2, near(0, 1)).wait_recv()
        key_copy(PAIR + t, t, o, 2, partner, leaving=S_PAIR).start()

    def pair_in(t):
        ref = keys.at[pl.ds(0, 16), 1 - c]
        copy(ref, ref, PAIR + t, partner).wait_recv()

    span = wo_hbm.shape[0] // 2

    def w_copy(number, row, device, which):
        ref = wg.at[c, row, pl.ds(which * span, span)]
        return copy(ref, ref, number, device, S_W)

    def w_pair(row, number):
        return copy(wg.at[c, row], wg.at[c, row], WPAIR + number, partner, S_WPAIR)

    def w_pair_in(row, number):
        return copy(wg.at[1 - c, row], wg.at[1 - c, row], WPAIR + number, partner)

    def project_in(*order):
        with jax.named_scope("project"):
            for j in order:
                project(j)

    def start_w():
        pltpu.make_async_copy(wo_hbm, wg.at[c, y], local_sem.at[9]).wait()
        for which in range(2):
            w_copy(WFULL + which, y, up_y, which).start()
            w_copy(WFULL + 3 - which, y, down_y, 1 - which).start()
        w_pair(y, 0).start()

    def swap_on():
        copy(qx.at[1 - xh, c], qx.at[1 - xh, c], SWAP, swap_peer).wait_recv()
        copy(qx.at[1 - xh, c], qx.at[1 - xh, c], SWAP2, partner, S_SWAP).start()

    with jax.named_scope("swap"):
        pl.when(xh == 1)(swap_on)
    with jax.named_scope("first_in_l"):
        first_in(lower)
    with jax.named_scope("relay_l0"):
        relay(0, lower)
    with jax.named_scope("far_l"):
        far_in(lower)
    with jax.named_scope("swap"):
        pl.when(xh == 0)(swap_on)
    with jax.named_scope("swap2"):
        own_rows.wait()
        pltpu.make_async_copy(wkv_hbm, wkv, local_sem.at[8]).wait()
        copy(qx.at[1 - xh, 1 - c], qx.at[1 - xh, 1 - c], SWAP2, partner).wait_recv()
    project_in(0, 1, 2)
    with jax.named_scope("relay_l21"):
        relay(2, lower)
        relay(1, lower)
    project_in(3)
    with jax.named_scope("relay_l3"):
        relay(3, lower)
    with jax.named_scope("first_in_u"):
        first_in(upper)
    project_in(4)
    with jax.named_scope("far_u"):
        far_in(upper)
    with jax.named_scope("last_in_l"):
        for q in (0, 2, 1):
            last_in(q, lower)
    project_in(5)
    with jax.named_scope("last_in_l3"):
        last_in(3, lower)
    with jax.named_scope("relay_u0"):
        relay(0, upper)
    project_in(6, 7)
    with jax.named_scope("pair_in_l"):
        pair_in(lower)

    scale = LOG2E / math.sqrt(NOPE + ROPE)
    reach = BLOCK // 128

    def attend(half, hooks, first, count):
        where = shard[half]
        blocks = where // reach
        tile_rows = count * HALF
        upto = pl.ds(0, tile_rows)
        m_ref[upto] = jnp.full((tile_rows, 128), -1e30, jnp.float32)
        l_ref[upto] = jnp.zeros((tile_rows, 128), jnp.float32)
        acc_ref[upto] = jnp.zeros((tile_rows, KVR), jnp.float32)

        def step(b, causal):
            block = keys[pl.ds(b * reach, reach)].reshape(BLOCK, WIDE)
            scores = lax.dot_general(
                qs[half, first : first + count].reshape(tile_rows, WIDE),
                block,
                (((1,), (1,)), ((), ())),
                preferred_element_type=jnp.float32,
            )
            scores = scores * scale + bias[pl.ds(b, 1), :]
            if causal is not None:
                scores = (scores.reshape(count, HALF, BLOCK) + causal[None]).reshape(
                    tile_rows, BLOCK
                )
            before = m_ref[upto]
            m_new = jnp.maximum(before, jnp.max(scores, axis=1, keepdims=True))
            alpha = jnp.exp2(before - m_new)
            lifted = jnp.exp2(scores - jnp.concatenate([m_new] * (BLOCK // 128), axis=1))
            total = l_ref[upto] * alpha
            for k in range(BLOCK // 128):
                total = total + lifted[:, k * 128 : (k + 1) * 128]
            l_ref[upto] = total
            m_ref[upto] = m_new
            acc_ref[upto] = acc_ref[upto] * jnp.concatenate([alpha] * (KVR // 128), axis=1) + jnp.dot(
                lifted.astype(jnp.bfloat16), block[:, :KVR], preferred_element_type=jnp.float32
            )

        def open_step(b, carry):
            hooks(b, blocks)
            step(b, None)
            return carry

        lax.fori_loop(0, blocks, open_step, 0)
        hooks(blocks, blocks)
        token = where * 128 + xh * HALF + lax.broadcasted_iota(jnp.int32, (HALF, BLOCK), 0)
        position = blocks * BLOCK + lax.broadcasted_iota(jnp.int32, (HALF, BLOCK), 1)
        step(blocks, jnp.where(position <= token, 0.0, -1e30))
        total = jnp.sum(l_ref[upto], axis=1, keepdims=True)
        ctx[:count] = (acc_ref[upto] / total).astype(jnp.bfloat16).reshape(count, HALF, KVR)

    here = xh * 4 + z

    def value_rows(h, at):
        w_value = wkv[:, h * 256 + NOPE : (h + 1) * 256]
        return jnp.dot(ctx[at], w_value, preferred_element_type=jnp.float32).astype(jnp.bfloat16)

    def values_low(g):
        for n in range(PER):
            attended = value_rows(g * PER + n, n)
            for to in range(2):
                low_stage[g, to, :, n * VD : (n + 1) * VD] = attended[
                    to * 2 * ROWS : (to + 1) * 2 * ROWS
                ]
        pair_copy(g).start()
        low[here, g, c] = low_stage[g, c]

    def values_high():
        for h in range(HEADS):
            attended = value_rows(h, h)
            for r in range(2):
                for to in range(2):
                    at = to * 2 * ROWS + r * ROWS
                    high_stage[r, to, :, h * VD : (h + 1) * VD] = attended[at : at + ROWS]
        for r in range(2):
            pair_copy(2 + r).start()
            high[here, r, c] = high_stage[r, c]

    def block_of(slot, g):
        return low.at[slot, g] if g < 2 else high.at[slot, g - 2]

    def a_copy(g, number, t, o, device, which=None):
        slot = (xh + t - 2 * xh * t) * 4 + lax.rem(z + o + 4, 4)
        ref = block_of(slot, g)
        if which is not None:
            ref = ref.at[which]
        return copy(ref, ref, ABASE + ASTRIDE * g + number, device, S_A + g)

    def pair_copy(g):
        staged = low_stage.at[g, 1 - c] if g < 2 else high_stage.at[g - 2, 1 - c]
        return copy(
            staged, block_of(here, g).at[c], ABASE + ASTRIDE * g + APAIR, partner, S_APAIR
        )

    def pair_copy_in(g):
        ref = block_of(here, g).at[1 - c]
        return copy(ref, ref, ABASE + ASTRIDE * g + APAIR, partner, S_APAIR)

    def stage1(g):
        pair_copy_in(g).wait_recv()
        a_copy(g, AX, 0, 0, across).start()
        a_copy(g, AZ, 0, 0, up_z).start()
        a_copy(g, AZ + 1, 0, 0, down_z).start()

    def stage2(g):
        a_copy(g, AZ, 0, -1, up_z).wait_recv()
        a_copy(g, AZH, 0, -1, up_z, 0).start()
        a_copy(g, AZ + 1, 0, 1, down_z).wait_recv()
        a_copy(g, AZH, 0, 1, down_z, 1).start()

    def stage3(g):
        a_copy(g, AX, 1, 0, across).wait_recv()
        a_copy(g, AZ + 2, 1, 0, up_z).start()
        a_copy(g, AZ + 3, 1, 0, down_z).start()

    def stage4(g):
        a_copy(g, AZH, 0, 2, up_z).wait_recv()
        a_copy(g, AX2, 0, 2, across).start()

    def stage5(g):
        a_copy(g, AZ + 2, 1, -1, up_z).wait_recv()
        a_copy(g, AZ + 3, 1, 1, down_z).wait_recv()
        a_copy(g, AX2, 1, 2, across).wait_recv()

    def w_relay(which):
        if which == 0:
            w_copy(WFULL, lax.rem(y + 3, 4), up_y, 0).wait_recv()
            w_copy(WHALF, lax.rem(y + 3, 4), up_y, 0).start()
        else:
            w_copy(WFULL + 3, lax.rem(y + 1, 4), down_y, 1).wait_recv()
            w_copy(WHALF, lax.rem(y + 1, 4), down_y, 1).start()

    def w_middle():
        w_copy(WFULL + 1, lax.rem(y + 3, 4), up_y, 1).wait_recv()
        w_pair(lax.rem(y + 3, 4), 1).start()
        w_copy(WFULL + 2, lax.rem(y + 1, 4), down_y, 0).wait_recv()
        w_pair(lax.rem(y + 1, 4), 2).start()

    def w_last():
        ref = wg.at[c, lax.rem(y + 2, 4)]
        copy(ref, ref, WHALF, up_y).wait_recv()
        w_pair(lax.rem(y + 2, 4), 3).start()

    def w_all():
        for k, o in enumerate((0, 3, 1, 2)):
            w_pair_in(lax.rem(y + o, 4), k).wait_recv()

    def multiplied(rows, weights):
        return lax.dot_general(
            rows, weights, (((1,), (1,)), ((), ())), preferred_element_type=jnp.float32
        )

    def product_low():
        rows, depth = 16 * ROWS, PER * VD
        total = jnp.zeros((rows, 4 * 224), jnp.float32)
        for g in range(2):
            for core in range(2):
                total = total + multiplied(
                    low[:, g, core].reshape(rows, depth),
                    wg[core, :, :, g * depth : (g + 1) * depth].reshape(4 * 224, depth),
                )
        total = total.reshape(8, 2 * ROWS, 4 * 224)
        for n in range(2):
            part[n] = total[:, n * ROWS : (n + 1) * ROWS]

    def product_high():
        rows = 16 * ROWS
        total = jnp.zeros((rows, 4 * 224), jnp.float32)
        for core in range(2):
            total = total + multiplied(
                high[:, :, core].reshape(rows, HEADS * VD),
                wg[core].reshape(4 * 224, HEADS * VD),
            )
        total = total.reshape(8, 2 * ROWS, 4 * 224)
        for n in range(2):
            part[2 + n] = total[:, n * ROWS : (n + 1) * ROWS]

    def slots(half, k):
        straight, mirrored = k, 3 - k
        first = straight if half == 0 else mirrored
        return first, 4 + 3 - first

    def half_out(g):
        for k in range(2):
            for xs, at in enumerate(slots(g // 2, 2 * (1 - xl) + k)):
                outgoing[g, 0, k, xs] = part[g, at].astype(jnp.bfloat16)
            copy(
                outgoing.at[g, 0, k], summand.at[g, k], XSUM + 2 * g + k, beside, S_XSUM
            ).start()

    def whole_out(g):
        half = g // 2
        number = lax.rem(z, 2) + 2 * c + 4 * (g % 2)
        for k in range(2):
            row = 2 * xl + k
            copy(outgoing.at[g, 0, k], summand.at[g, k], XSUM + 2 * g + k, beside).wait_recv()
            for xs, at in enumerate(slots(half, row)):
                outgoing[g, 1, k, xs] = (
                    part[g, at] + summand[g, k, xs].astype(jnp.float32)
                ).astype(jnp.bfloat16)
            own = (mine == 1) & (xh == half) & (z == row)
            target = out_ref.at[:, 2 * c + g % 2, :, pl.ds(lax.rem(z, 2) * 896, 896)]

            @pl.when(jnp.logical_not(own))
            def _():
                copy(
                    outgoing.at[g, 1, k], target, OUT + number, owners[half][k], S_OUT + 2 * g + k
                ).start()

            @pl.when(own)
            def _():
                pltpu.make_async_copy(
                    outgoing.at[g, 1, k], target, local_sem.at[10 + g % 2]
                ).start()

    def first_hooks(b, blocks):
        @pl.when(b == 0)
        def _():
            with jax.named_scope("relay_u"):
                for q in (2, 1, 3):
                    relay(q, upper)
                start_w()

    def last_in_u():
        with jax.named_scope("last_in_u"):
            for q in (0, 2, 1, 3):
                last_in(q, upper)

    def second_hooks(b, blocks):
        @pl.when((b == jnp.minimum(2, blocks)) & (blocks > 0))
        def _():
            with jax.named_scope("stage1_0"):
                stage1(0)
            last_in_u()

    def late_hooks(b, blocks):
        @pl.when((b == 0) & (shard[0] < reach))
        def _():
            with jax.named_scope("stage1_0"):
                stage1(0)
            last_in_u()

        @pl.when(b == 1)
        def _():
            with jax.named_scope("stage1_1"):
                stage1(1)

        @pl.when(b == 4)
        def _():
            with jax.named_scope("pair_in_u"):
                pair_in(upper)

        @pl.when(b == blocks - 1)
        def _():
            with jax.named_scope("stage23_0"):
                stage2(0)
                stage3(0)
                w_relay(0)
                w_relay(1)

        @pl.when(b == blocks)
        def _():
            with jax.named_scope("stage23_1"):
                stage2(1)
                stage3(1)

    with jax.named_scope("attend_low"):
        attend(0, first_hooks, 0, PER)
    with jax.named_scope("values"):
        values_low(0)
    with jax.named_scope("attend_low"):
        attend(0, second_hooks, PER, PER)
    with jax.named_scope("values"):
        values_low(1)
    with jax.named_scope("attend_high"):
        attend(1, late_hooks, 0, HEADS)
    with jax.named_scope("values"):
        values_high()
    with jax.named_scope("stage4_0"):
        stage4(0)
    with jax.named_scope("stage1_23"):
        stage1(2)
        stage1(3)
    with jax.named_scope("stage4_1"):
        stage4(1)
    with jax.named_scope("w_middle"):
        w_middle()
    with jax.named_scope("stage2_2"):
        stage2(2)
    with jax.named_scope("stage2_3"):
        stage2(3)
    with jax.named_scope("stage3_2"):
        stage3(2)
    with jax.named_scope("stage3_3"):
        stage3(3)
    with jax.named_scope("w_last"):
        w_last()
    with jax.named_scope("stage4_2"):
        stage4(2)
    with jax.named_scope("stage5_0"):
        stage5(0)
    with jax.named_scope("stage5_1"):
        stage5(1)
    with jax.named_scope("stage4_3"):
        stage4(3)
    with jax.named_scope("w_all"):
        w_all()
    with jax.named_scope("product_low"):
        product_low()
    with jax.named_scope("half_out_low"):
        half_out(0)
        half_out(1)
    with jax.named_scope("stage5_23"):
        stage5(2)
        stage5(3)
    with jax.named_scope("product_high"):
        product_high()
    with jax.named_scope("half_out_high"):
        half_out(2)
        half_out(3)
    with jax.named_scope("whole_out_low"):
        whole_out(0)
        whole_out(1)
    with jax.named_scope("whole_out_2"):
        whole_out(2)
    with jax.named_scope("whole_out_3"):
        whole_out(3)

    with jax.named_scope("finish"):
        for n in range(8):
            r, k = n // 4, n % 4
            piece = out_ref.at[:, 2 * (k // 2) + r, :, (k % 2) * 896 : (k % 2 + 1) * 896]
            self_made = (mine == 1) & (makers[k][1] == z) & (k // 2 == c)

            @pl.when(jnp.logical_not(self_made))
            def _(n=n, piece=piece):
                copy(piece, piece, OUT + n, partner).wait_recv()

            @pl.when(self_made)
            def _(r=r, piece=piece):
                pltpu.make_async_copy(outgoing.at[0, 1, 0], piece, local_sem.at[10 + r]).wait()

    with jax.named_scope("drain"):

        def sent(ref, leaving):
            copy(ref, ref, 0, partner, leaving).wait_send()

        sent(keys.at[0, 0], S_CROSS)
        sent(qx.at[0], S_SWAP)
        sent(keys.at[pl.ds(0, 15)], S_KEYS)
        sent(keys.at[pl.ds(0, 16)], S_PAIR)
        sent(wg.at[0, pl.ds(0, 3)], S_W)
        sent(wg.at[0], S_WPAIR)
        sent(low_stage, S_APAIR)
        sent(summand, S_XSUM)
        for g in range(CHUNKS):
            sent(low.at[pl.ds(0, 7), 0], S_A + g)
        for g in range(CHUNKS):
            for k in range(2):
                own = (mine == 1) & (xh == g // 2) & (z == 2 * xl + k)

                @pl.when(jnp.logical_not(own))
                def _(g=g, k=k):
                    sent(summand.at[0, 0], S_OUT + 2 * g + k)


def local(q_latent, kv_latent, kv_gain, w_q_b, w_kv_b, w_o, prompt_len, response_mask):
    frequency = 10000.0 ** (-np.arange(ROPE // 2, dtype=np.float64) * 2.0 / ROPE)
    fine = np.arange(HALF, dtype=np.float64)[:, None] * np.tile(frequency, 2)[None, :]
    table = np.stack([np.cos(fine), np.sin(fine), np.cos(HALF * fine), np.sin(HALF * fine)])
    hbm = pl.BlockSpec(memory_space=pltpu.HBM)
    bf16 = jnp.bfloat16
    result = pl.pallas_call(
        body,
        out_shape=jax.ShapeDtypeStruct((2, 4, ROWS, 1792), bf16),
        in_specs=[hbm] * 5 + [pl.BlockSpec(memory_space=pltpu.SMEM)] + [hbm] * 3,
        out_specs=hbm,
        scratch_shapes=[
            pltpu.SemaphoreType.DMA((NSENT,)),
            pltpu.SemaphoreType.DMA((NSEM,)),
            pltpu.SemaphoreType.DMA((17,)),
            pltpu.VMEM((WIDE, 128), bf16),
            pltpu.VMEM((1, KVR), jnp.float32),
            pltpu.VMEM((4, HALF, ROPE), jnp.float32),
            pltpu.VMEM((32, 128), jnp.int32),
            pltpu.VMEM((2, 2, HALF // 2, 1536), bf16),
            pltpu.VMEM((8, 1536, 384), bf16),
            pltpu.VMEM((512, 4096), bf16),
            pltpu.VMEM((32, 2, HALF, WIDE), bf16),
            pltpu.VMEM((2, HEADS, HALF, WIDE), bf16),
            pltpu.VMEM((HEADS, HALF, KVR), bf16),
            pltpu.VMEM((2, 2, 2 * ROWS, PER * VD), bf16),
            pltpu.VMEM((2, 2, ROWS, HEADS * VD), bf16),
            pltpu.VMEM((8, 2, 2, 2 * ROWS, PER * VD), bf16),
            pltpu.VMEM((8, 2, 2, ROWS, HEADS * VD), bf16),
            pltpu.VMEM((2, 4, 224, 2048), bf16),
            pltpu.VMEM((CHUNKS, 8, ROWS, 4 * 224), jnp.float32),
            pltpu.VMEM((CHUNKS, 2, 2, 2, ROWS, 4 * 224), bf16),
            pltpu.VMEM((CHUNKS, 2, 2, ROWS, 4 * 224), bf16),
            pltpu.VMEM((4096 // BLOCK, BLOCK), jnp.float32),
            pltpu.VMEM((HEADS * HALF, 128), jnp.float32),
            pltpu.VMEM((HEADS * HALF, 128), jnp.float32),
            pltpu.VMEM((HEADS * HALF, KVR), jnp.float32),
        ],
        compiler_params=pltpu.CompilerParams(
            collective_id=0, has_side_effects=True, vmem_limit_bytes=67000000
        ),
        cost_estimate=pl.CostEstimate(
            flops=20_000_000_000, bytes_accessed=16_000_000, transcendentals=0
        ),
        name="layer",
    )(
        q_latent.reshape(2, 2, HALF // 2, 1536),
        kv_latent.T,
        kv_gain.reshape(1, -1),
        jnp.asarray(table, jnp.float32),
        response_mask.reshape(32, 128),
        prompt_len,
        w_q_b,
        w_kv_b,
        w_o.T,
    )
    return jnp.where(prompt_len[0] > 0, result.reshape(128, 1792), 0)


def solution(mesh):
    finer = Mesh(mesh.devices.reshape(2, 4, 4, 2, 2), AXES)
    placed = (
        P(DP, None),
        P(DP, None),
        P(),
        P(None, HEAD),
        P(None, HEAD),
        P(HEAD, DP),
        P(),
        P(),
    )
    return jax.shard_map(
        local, mesh=finer, in_specs=placed, out_specs=P(DP, HEAD), check_vma=False
    )
```

```python
import functools
import math

import jax
import jax.numpy as jnp
import numpy as np
from jax import lax
from jax.experimental import pallas as pl
from jax.experimental.pallas import tpu as pltpu
from jax.sharding import Mesh
from jax.sharding import PartitionSpec as P

KVR = 512
ROPE = 64
NOPE = 128
VD = 128
WIDE = KVR + ROPE
AXES = ("xh", "z", "y", "xl", "c")
DP = ("xh", "z", "y")
HEAD = ("xl", "c")
MESH = pl.DeviceIdType.MESH

HEADS = 16
PER = 8
CHUNKS = 4
HALF = 64
ROWS = 16
BLOCK = 512
LOG2E = 1.4426950408889634
EPS = 1e-06

CROSS = 0
SWAP = 1
SWAP2 = 2
D1 = 3
FAR = 7
D2 = 9
D2H = 25
PAIR = 33
WFULL = 35
WHALF = 39
WPAIR = 40
ABASE = 44
APAIR, AX, AZ, AZH, AX2 = 0, 1, 2, 6, 7
ASTRIDE = 8
OUT = ABASE + ASTRIDE * CHUNKS
XSUM = OUT + 8
NSEM = XSUM + 8
S_CROSS, S_SWAP, S_KEYS, S_PAIR, S_W, S_WPAIR, S_APAIR, S_XSUM, S_A, S_OUT = 0, 1, 2, 3, 4, 5, 6, 7, 8, 12
NSENT = S_OUT + 8


def turn(values, cosine, sine):
    swapped = jnp.concatenate([values[:, ROPE // 2 :], values[:, : ROPE // 2]], axis=1)
    return values * cosine + swapped * sine


def body(
    q_hbm,
    kv_hbm,
    gain_hbm,
    table_hbm,
    live_hbm,
    prompt,
    wq_hbm,
    wkv_hbm,
    wo_hbm,
    out_ref,
    out_sem,
    in_sem,
    local_sem,
    kv_lat,
    gain,
    table,
    live,
    qx,
    wq,
    wkv,
    keys,
    qs,
    ctx,
    low_stage,
    high_stage,
    low,
    high,
    wg,
    part,
    outgoing,
    summand,
    bias,
    m_ref,
    l_ref,
    acc_ref,
):
    xh, z, y, xl, c = (lax.axis_index(a) for a in AXES)
    d1 = y + c * (z - y)
    d2 = z + c * (y - z)

    def place(t, o1, o2):
        a = lax.rem(d1 + o1 + 4, 4)
        b = lax.rem(d2 + o2 + 4, 4)
        zz = b + c * (a - b)
        yy = a + c * (b - a)
        xx = xh + t - 2 * xh * t
        return xx, zz, yy

    def unit(t, o1, o2):
        xx, zz, yy = place(t, o1, o2)
        return xx * 16 + zz * 4 + yy

    def near(o1, o2):
        _, zz, yy = place(0, o1, o2)
        return (xh, zz, yy, xl, c)

    def copy(src, dst, number, device, leaving=0):
        return pltpu.make_async_remote_copy(
            src_ref=src,
            dst_ref=dst,
            send_sem=out_sem.at[leaving],
            recv_sem=in_sem.at[number],
            device_id=device,
            device_id_type=MESH,
        )

    me = unit(0, 0, 0)
    partner = (xh, z, y, xl, 1 - c)
    cross = (1 - xh, z, y, 1 - xl, c)
    swap_peer = (1 - xh, 3 - z, y, 1 - xl, c)
    across = (1 - xh, z, y, xl, c)
    up_y = (xh, z, lax.rem(y + 1, 4), xl, c)
    down_y = (xh, z, lax.rem(y + 3, 4), xl, c)
    up_z = (xh, lax.rem(z + 1, 4), y, xl, c)
    down_z = (xh, lax.rem(z + 3, 4), y, xl, c)
    owners = [[(t, 2 * xl + k, y, xh, z // 2) for k in range(2)] for t in range(2)]
    makers = [(xl, 2 * c + k % 2, y, z // 2, k // 2) for k in range(4)]
    beside = (xh, z, y, 1 - xl, c)
    same = lambda u, v: 1 - jnp.minimum((u - v) * (u - v), 1)
    mine = same(c, xh) * same(xl, xh) * same(z // 2, c)
    z_low = z + xh * (3 - 2 * z)
    shard = (z_low * 4 + y, 16 + (3 - z_low) * 4 + y)

    barrier = pltpu.get_barrier_semaphore()
    far = near(2, 0)
    for peer in (partner, cross, swap_peer, across, beside, far, up_y, down_y, up_z, down_z):
        pl.semaphore_signal(barrier, inc=1, device_id=peer, device_id_type=MESH)
    for k in range(4):

        @pl.when((mine == 0) | (makers[k][1] != z) | (k // 2 != c))
        def _(k=k):
            pl.semaphore_signal(barrier, inc=1, device_id=makers[k], device_id_type=MESH)

    inputs = ((kv_hbm, kv_lat), (gain_hbm, gain), (table_hbm, table), (live_hbm, live))
    for n, (far_away, close) in enumerate(inputs):
        pltpu.make_async_copy(far_away, close, local_sem.at[12 + n]).start()
    own_rows = pltpu.make_async_copy(q_hbm.at[xh], qx.at[xh], local_sem.at[16])
    own_rows.start()
    pltpu.make_async_copy(wkv_hbm, wkv, local_sem.at[8]).start()
    for j in range(8):
        pltpu.make_async_copy(wq_hbm.at[:, pl.ds(j * 384, 384)], wq.at[j], local_sem.at[j]).start()
    pltpu.make_async_copy(wo_hbm, wg.at[c, y], local_sem.at[9]).start()

    with jax.named_scope("norm"):
        for n, (far_away, close) in enumerate(inputs):
            pltpu.make_async_copy(far_away, close, local_sem.at[12 + n]).wait()
        lane = lax.broadcasted_iota(jnp.int32, (1, ROPE), 1)
        sign = jnp.where(lane < ROPE // 2, -1.0, 1.0)

        def angles(m):
            cos_a, sin_a = table[2, pl.ds(m, 1), :], table[3, pl.ds(m, 1), :]
            cos_b, sin_b = table[0], table[1]
            return cos_a * cos_b - sin_a * sin_b, (sin_a * cos_b + cos_a * sin_b) * sign

        turned_rows = kv_lat[...].astype(jnp.float32).T
        rows = jnp.where(c == 0, turned_rows[:HALF], turned_rows[HALF:])
        latent = rows[:, :KVR]
        inverse = lax.rsqrt(jnp.mean(latent * latent, axis=-1, keepdims=True) + EPS)
        keys[me, c, :, :KVR] = (latent * inverse * gain[...]).astype(jnp.bfloat16)
        keys[me, c, :, KVR:] = turn(rows[:, KVR:], *angles(me * 2 + c)).astype(jnp.bfloat16)
        spot = lax.broadcasted_iota(jnp.int32, (32, 128), 0) * 128 + lax.broadcasted_iota(
            jnp.int32, (32, 128), 1
        )
        usable = (spot < prompt[0]) | (live[...] == 1)
        masked = jnp.where(usable, 0.0, -1e30)
        for r in range(32):
            b, at = r // (BLOCK // 128), r % (BLOCK // 128)
            bias[b : b + 1, at * 128 : (at + 1) * 128] = masked[r : r + 1]

    with jax.named_scope("barrier"):
        pl.semaphore_wait(barrier, 14 - mine)

    def key(t, o1, o2, which=None):
        ref = keys.at[unit(t, o1, o2), c]
        if which is None:
            return ref
        return ref.at[pl.ds(32 * which, 32)]

    def key_copy(number, t, o1, o2, device, which=None, leaving=S_KEYS):
        ref = key(t, o1, o2, which)
        return copy(ref, ref, number, device, leaving)

    offsets = (0, 1, 3, 2)
    lower, upper = xh, 1 - xh

    def spread(q, t):
        k, o = 2 * q + t, offsets[q]
        key_copy(D2 + 2 * k, t, o, 0, near(0, 1)).start()
        key_copy(D2 + 2 * k + 1, t, o, 0, near(0, -1)).start()
        key_copy(PAIR + t, t, o, 0, partner, leaving=S_PAIR).start()

    def first_out(t):
        key_copy(D1 + 2 * t, t, 0, 0, near(1, 0)).start()
        key_copy(D1 + 2 * t + 1, t, 0, 0, near(-1, 0)).start()
        spread(0, t)
        key_copy(FAR + t, t, 0, 0, far).start()

    def first_in(t):
        key_copy(D1 + 2 * t, t, -1, 0, near(1, 0)).wait_recv()
        spread(2, t)
        key_copy(D1 + 2 * t + 1, t, 1, 0, near(-1, 0)).wait_recv()
        spread(1, t)

    def far_in(t):
        key_copy(FAR + t, t, 2, 0, far).wait_recv()
        spread(3, t)

    def cross_in():
        key_copy(CROSS, 1, 0, 0, cross).wait_recv()

    with jax.named_scope("spread"):
        key_copy(CROSS, 0, 0, 0, cross, leaving=S_CROSS).start()
        copy(q_hbm.at[1 - xh, c], qx.at[xh, c], SWAP, swap_peer, S_SWAP).start()
        pl.when(xh == 1)(cross_in)
        first_out(lower)
        pl.when(xh == 0)(cross_in)
        first_out(upper)

    tables = [angles(2 * where + xh) for where in shard]

    def project(j):
        pltpu.make_async_copy(
            wq_hbm.at[:, pl.ds(0, 384)], wq.at[j], local_sem.at[j]
        ).wait()
        both = jnp.dot(
            qx[...].reshape(2 * HALF, 1536), wq[j], preferred_element_type=jnp.float32
        ).astype(jnp.bfloat16)
        for e in range(2):
            h = 2 * j + e
            plain = both[:, e * 192 : e * 192 + NOPE]
            roped = both[:, e * 192 + NOPE : (e + 1) * 192].astype(jnp.float32)
            w_key = wkv[:, pl.ds(pl.multiple_of(h * 256, 256), NOPE)]
            absorbed = lax.dot_general(
                plain, w_key, (((1,), (1,)), ((), ())), preferred_element_type=jnp.float32
            ).astype(jnp.bfloat16)
            for half in range(2):
                mine_rows = slice(half * HALF, (half + 1) * HALF)
                qs[half, h, :, :KVR] = absorbed[mine_rows]
                qs[half, h, :, KVR:] = turn(roped[mine_rows], *tables[half]).astype(jnp.bfloat16)

    def relay(q, t):
        k, o = 2 * q + t, offsets[q]
        key_copy(D2 + 2 * k, t, o, -1, near(0, 1)).wait_recv()
        key_copy(D2H + k, t, o, -1, near(0, 1), 0).start()
        key_copy(PAIR + t, t, o, -1, partner, leaving=S_PAIR).start()
        key_copy(D2 + 2 * k + 1, t, o, 1, near(0, -1)).wait_recv()
        key_copy(D2H + k, t, o, 1, near(0, -1), 1).start()
        key_copy(PAIR + t, t, o, 1, partner, leaving=S_PAIR).start()

    def last_in(q, t):
        k, o = 2 * q + t, offsets[q]
        key_copy(D2H + k, t, o, 2, near(0, 1)).wait_recv()
        key_copy(PAIR + t, t, o, 2, partner, leaving=S_PAIR).start()

    def pair_in(t):
        ref = keys.at[pl.ds(0, 16), 1 - c]
        copy(ref, ref, PAIR + t, partner).wait_recv()

    span = wo_hbm.shape[0] // 2

    def w_copy(number, row, device, which):
        ref = wg.at[c, row, pl.ds(which * span, span)]
        return copy(ref, ref, number, device, S_W)

    def w_pair(row, number):
        return copy(wg.at[c, row], wg.at[c, row], WPAIR + number, partner, S_WPAIR)

    def w_pair_in(row, number):
        return copy(wg.at[1 - c, row], wg.at[1 - c, row], WPAIR + number, partner)

    def project_in(*order):
        with jax.named_scope("project"):
            for j in order:
                project(j)

    def start_w():
        pltpu.make_async_copy(wo_hbm, wg.at[c, y], local_sem.at[9]).wait()
        for which in range(2):
            w_copy(WFULL + which, y, up_y, which).start()
            w_copy(WFULL + 3 - which, y, down_y, 1 - which).start()
        w_pair(y, 0).start()

    def swap_on():
        copy(qx.at[1 - xh, c], qx.at[1 - xh, c], SWAP, swap_peer).wait_recv()
        copy(qx.at[1 - xh, c], qx.at[1 - xh, c], SWAP2, partner, S_SWAP).start()

    with jax.named_scope("swap"):
        pl.when(xh == 1)(swap_on)
    with jax.named_scope("first_in_l"):
        first_in(lower)
    with jax.named_scope("relay_l0"):
        relay(0, lower)
    with jax.named_scope("far_l"):
        far_in(lower)
    with jax.named_scope("swap"):
        pl.when(xh == 0)(swap_on)
    with jax.named_scope("swap2"):
        own_rows.wait()
        pltpu.make_async_copy(wkv_hbm, wkv, local_sem.at[8]).wait()
        copy(qx.at[1 - xh, 1 - c], qx.at[1 - xh, 1 - c], SWAP2, partner).wait_recv()
    project_in(0, 1, 2)
    with jax.named_scope("relay_l21"):
        relay(2, lower)
        relay(1, lower)
    project_in(3)
    with jax.named_scope("relay_l3"):
        relay(3, lower)
    with jax.named_scope("first_in_u"):
        first_in(upper)
    project_in(4)
    with jax.named_scope("far_u"):
        far_in(upper)
    with jax.named_scope("last_in_l"):
        for q in (0, 2, 1):
            last_in(q, lower)
    project_in(5)
    with jax.named_scope("last_in_l3"):
        last_in(3, lower)
    with jax.named_scope("relay_u0"):
        relay(0, upper)
    project_in(6, 7)
    with jax.named_scope("pair_in_l"):
        pair_in(lower)

    scale = LOG2E / math.sqrt(NOPE + ROPE)
    reach = BLOCK // 128

    def attend(half, hooks, first, count):
        where = shard[half]
        blocks = where // reach
        tile_rows = count * HALF
        upto = pl.ds(0, tile_rows)
        m_ref[upto] = jnp.full((tile_rows, 128), -1e30, jnp.float32)
        l_ref[upto] = jnp.zeros((tile_rows, 128), jnp.float32)
        acc_ref[upto] = jnp.zeros((tile_rows, KVR), jnp.float32)

        def step(b, causal):
            block = keys[pl.ds(b * reach, reach)].reshape(BLOCK, WIDE)
            scores = lax.dot_general(
                qs[half, first : first + count].reshape(tile_rows, WIDE),
                block,
                (((1,), (1,)), ((), ())),
                preferred_element_type=jnp.float32,
            )
            scores = scores * scale + bias[pl.ds(b, 1), :]
            if causal is not None:
                scores = (scores.reshape(count, HALF, BLOCK) + causal[None]).reshape(
                    tile_rows, BLOCK
                )
            before = m_ref[upto]
            m_new = jnp.maximum(before, jnp.max(scores, axis=1, keepdims=True))
            alpha = jnp.exp2(before - m_new)
            lifted = jnp.exp2(scores - jnp.concatenate([m_new] * (BLOCK // 128), axis=1))
            total = l_ref[upto] * alpha
            for k in range(BLOCK // 128):
                total = total + lifted[:, k * 128 : (k + 1) * 128]
            l_ref[upto] = total
            m_ref[upto] = m_new
            acc_ref[upto] = acc_ref[upto] * jnp.concatenate([alpha] * (KVR // 128), axis=1) + jnp.dot(
                lifted.astype(jnp.bfloat16), block[:, :KVR], preferred_element_type=jnp.float32
            )

        def open_step(b, carry):
            hooks(b, blocks)
            step(b, None)
            return carry

        lax.fori_loop(0, blocks, open_step, 0)
        hooks(blocks, blocks)
        token = where * 128 + xh * HALF + lax.broadcasted_iota(jnp.int32, (HALF, BLOCK), 0)
        position = blocks * BLOCK + lax.broadcasted_iota(jnp.int32, (HALF, BLOCK), 1)
        step(blocks, jnp.where(position <= token, 0.0, -1e30))
        total = jnp.sum(l_ref[upto], axis=1, keepdims=True)
        ctx[:count] = (acc_ref[upto] / total).astype(jnp.bfloat16).reshape(count, HALF, KVR)

    here = xh * 4 + z

    def value_rows(h, at):
        w_value = wkv[:, h * 256 + NOPE : (h + 1) * 256]
        return jnp.dot(ctx[at], w_value, preferred_element_type=jnp.float32).astype(jnp.bfloat16)

    def values_low(g):
        for n in range(PER):
            attended = value_rows(g * PER + n, n)
            for to in range(2):
                low_stage[g, to, :, n * VD : (n + 1) * VD] = attended[
                    to * 2 * ROWS : (to + 1) * 2 * ROWS
                ]
        pair_copy(g).start()
        low[here, g, c] = low_stage[g, c]

    def values_high():
        for h in range(HEADS):
            attended = value_rows(h, h)
            for r in range(2):
                for to in range(2):
                    at = to * 2 * ROWS + r * ROWS
                    high_stage[r, to, :, h * VD : (h + 1) * VD] = attended[at : at + ROWS]
        for r in range(2):
            pair_copy(2 + r).start()
            high[here, r, c] = high_stage[r, c]

    def block_of(slot, g):
        return low.at[slot, g] if g < 2 else high.at[slot, g - 2]

    def a_copy(g, number, t, o, device, which=None):
        slot = (xh + t - 2 * xh * t) * 4 + lax.rem(z + o + 4, 4)
        ref = block_of(slot, g)
        if which is not None:
            ref = ref.at[which]
        return copy(ref, ref, ABASE + ASTRIDE * g + number, device, S_A + g)

    def pair_copy(g):
        staged = low_stage.at[g, 1 - c] if g < 2 else high_stage.at[g - 2, 1 - c]
        return copy(
            staged, block_of(here, g).at[c], ABASE + ASTRIDE * g + APAIR, partner, S_APAIR
        )

    def pair_copy_in(g):
        ref = block_of(here, g).at[1 - c]
        return copy(ref, ref, ABASE + ASTRIDE * g + APAIR, partner, S_APAIR)

    def stage1(g):
        pair_copy_in(g).wait_recv()
        a_copy(g, AX, 0, 0, across).start()
        a_copy(g, AZ, 0, 0, up_z).start()
        a_copy(g, AZ + 1, 0, 0, down_z).start()

    def stage2(g):
        a_copy(g, AZ, 0, -1, up_z).wait_recv()
        a_copy(g, AZH, 0, -1, up_z, 0).start()
        a_copy(g, AZ + 1, 0, 1, down_z).wait_recv()
        a_copy(g, AZH, 0, 1, down_z, 1).start()

    def stage3(g):
        a_copy(g, AX, 1, 0, across).wait_recv()
        a_copy(g, AZ + 2, 1, 0, up_z).start()
        a_copy(g, AZ + 3, 1, 0, down_z).start()

    def stage4(g):
        a_copy(g, AZH, 0, 2, up_z).wait_recv()
        a_copy(g, AX2, 0, 2, across).start()

    def stage5(g):
        a_copy(g, AZ + 2, 1, -1, up_z).wait_recv()
        a_copy(g, AZ + 3, 1, 1, down_z).wait_recv()
        a_copy(g, AX2, 1, 2, across).wait_recv()

    def w_relay(which):
        if which == 0:
            w_copy(WFULL, lax.rem(y + 3, 4), up_y, 0).wait_recv()
            w_copy(WHALF, lax.rem(y + 3, 4), up_y, 0).start()
        else:
            w_copy(WFULL + 3, lax.rem(y + 1, 4), down_y, 1).wait_recv()
            w_copy(WHALF, lax.rem(y + 1, 4), down_y, 1).start()

    def w_middle():
        w_copy(WFULL + 1, lax.rem(y + 3, 4), up_y, 1).wait_recv()
        w_pair(lax.rem(y + 3, 4), 1).start()
        w_copy(WFULL + 2, lax.rem(y + 1, 4), down_y, 0).wait_recv()
        w_pair(lax.rem(y + 1, 4), 2).start()

    def w_last():
        ref = wg.at[c, lax.rem(y + 2, 4)]
        copy(ref, ref, WHALF, up_y).wait_recv()
        w_pair(lax.rem(y + 2, 4), 3).start()

    def w_all():
        for k, o in enumerate((0, 3, 1, 2)):
            w_pair_in(lax.rem(y + o, 4), k).wait_recv()

    def multiplied(rows, weights):
        return lax.dot_general(
            rows, weights, (((1,), (1,)), ((), ())), preferred_element_type=jnp.float32
        )

    def product_low():
        rows, depth = 16 * ROWS, PER * VD
        total = jnp.zeros((rows, 4 * 224), jnp.float32)
        for g in range(2):
            for core in range(2):
                total = total + multiplied(
                    low[:, g, core].reshape(rows, depth),
                    wg[core, :, :, g * depth : (g + 1) * depth].reshape(4 * 224, depth),
                )
        total = total.reshape(8, 2 * ROWS, 4 * 224)
        for n in range(2):
            part[n] = total[:, n * ROWS : (n + 1) * ROWS]

    def product_high(r):
        rows = 8 * ROWS
        total = jnp.zeros((rows, 4 * 224), jnp.float32)
        for core in range(2):
            total = total + multiplied(
                high[:, r, core].reshape(rows, HEADS * VD),
                wg[core].reshape(4 * 224, HEADS * VD),
            )
        part[2 + r] = total.reshape(8, ROWS, 4 * 224)

    def slots(half, k):
        straight, mirrored = k, 3 - k
        first = straight if half == 0 else mirrored
        return first, 4 + 3 - first

    def half_out(g):
        for k in range(2):
            for xs, at in enumerate(slots(g // 2, 2 * (1 - xl) + k)):
                outgoing[g, 0, k, xs] = part[g, at].astype(jnp.bfloat16)
            copy(
                outgoing.at[g, 0, k], summand.at[g, k], XSUM + 2 * g + k, beside, S_XSUM
            ).start()

    def whole_out(g):
        half = g // 2
        number = lax.rem(z, 2) + 2 * c + 4 * (g % 2)
        for k in range(2):
            row = 2 * xl + k
            copy(outgoing.at[g, 0, k], summand.at[g, k], XSUM + 2 * g + k, beside).wait_recv()
            for xs, at in enumerate(slots(half, row)):
                outgoing[g, 1, k, xs] = (
                    part[g, at] + summand[g, k, xs].astype(jnp.float32)
                ).astype(jnp.bfloat16)
            own = (mine == 1) & (xh == half) & (z == row)
            target = out_ref.at[:, 2 * c + g % 2, :, pl.ds(lax.rem(z, 2) * 896, 896)]

            @pl.when(jnp.logical_not(own))
            def _():
                copy(
                    outgoing.at[g, 1, k], target, OUT + number, owners[half][k], S_OUT + 2 * g + k
                ).start()

            @pl.when(own)
            def _():
                pltpu.make_async_copy(
                    outgoing.at[g, 1, k], target, local_sem.at[10 + g % 2]
                ).start()

    def first_hooks(b, blocks):
        @pl.when(b == jnp.minimum(1, blocks))
        def _():
            with jax.named_scope("relay_u"):
                for q in (2, 1, 3):
                    relay(q, upper)
                start_w()

    def last_in_u():
        with jax.named_scope("last_in_u"):
            for q in (0, 2, 1, 3):
                last_in(q, upper)

    def second_hooks(b, blocks):
        @pl.when((b == jnp.minimum(2, blocks)) & (blocks > 0))
        def _():
            with jax.named_scope("stage1_0"):
                stage1(0)
            last_in_u()

    def late_hooks(b, blocks):
        @pl.when((b == 0) & (shard[0] < reach))
        def _():
            with jax.named_scope("stage1_0"):
                stage1(0)
            last_in_u()

        @pl.when(b == 1)
        def _():
            with jax.named_scope("stage1_1"):
                stage1(1)

        @pl.when(b == 4)
        def _():
            with jax.named_scope("pair_in_u"):
                pair_in(upper)

        @pl.when(b == blocks - 1)
        def _():
            with jax.named_scope("stage23_0"):
                stage2(0)
                stage3(0)
                w_relay(0)
                w_relay(1)

        @pl.when(b == blocks)
        def _():
            with jax.named_scope("stage23_1"):
                stage2(1)
                stage3(1)

    with jax.named_scope("attend_low"):
        attend(0, first_hooks, 0, PER)
    with jax.named_scope("values"):
        values_low(0)
    with jax.named_scope("attend_low"):
        attend(0, second_hooks, PER, PER)
    with jax.named_scope("values"):
        values_low(1)
    with jax.named_scope("attend_high"):
        attend(1, late_hooks, 0, HEADS)
    with jax.named_scope("values"):
        values_high()
    with jax.named_scope("stage4_0"):
        stage4(0)
    with jax.named_scope("stage1_23"):
        stage1(2)
        stage1(3)
    with jax.named_scope("stage4_1"):
        stage4(1)
    with jax.named_scope("w_middle"):
        w_middle()
    with jax.named_scope("stage2_2"):
        stage2(2)
    with jax.named_scope("stage2_3"):
        stage2(3)
    with jax.named_scope("stage3_2"):
        stage3(2)
    with jax.named_scope("stage3_3"):
        stage3(3)
    with jax.named_scope("w_last"):
        w_last()
    with jax.named_scope("stage4_2"):
        stage4(2)
    with jax.named_scope("stage5_0"):
        stage5(0)
    with jax.named_scope("stage5_1"):
        stage5(1)
    with jax.named_scope("stage4_3"):
        stage4(3)
    with jax.named_scope("w_all"):
        w_all()
    with jax.named_scope("product_low"):
        product_low()
    with jax.named_scope("half_out_low"):
        half_out(0)
        half_out(1)
    with jax.named_scope("stage5_2"):
        stage5(2)
    with jax.named_scope("product_2"):
        product_high(0)
    with jax.named_scope("half_out_2"):
        half_out(2)
    with jax.named_scope("stage5_3"):
        stage5(3)
    with jax.named_scope("product_3"):
        product_high(1)
    with jax.named_scope("half_out_3"):
        half_out(3)
    with jax.named_scope("whole_out_low"):
        whole_out(0)
        whole_out(1)
    with jax.named_scope("whole_out_2"):
        whole_out(2)
    with jax.named_scope("whole_out_3"):
        whole_out(3)

    with jax.named_scope("finish"):
        for n in range(8):
            r, k = n // 4, n % 4
            piece = out_ref.at[:, 2 * (k // 2) + r, :, (k % 2) * 896 : (k % 2 + 1) * 896]
            self_made = (mine == 1) & (makers[k][1] == z) & (k // 2 == c)

            @pl.when(jnp.logical_not(self_made))
            def _(n=n, piece=piece):
                copy(piece, piece, OUT + n, partner).wait_recv()

            @pl.when(self_made)
            def _(r=r, piece=piece):
                pltpu.make_async_copy(outgoing.at[0, 1, 0], piece, local_sem.at[10 + r]).wait()

    with jax.named_scope("drain"):

        def sent(ref, leaving):
            copy(ref, ref, 0, partner, leaving).wait_send()

        sent(keys.at[0, 0], S_CROSS)
        sent(qx.at[0], S_SWAP)
        sent(keys.at[pl.ds(0, 15)], S_KEYS)
        sent(keys.at[pl.ds(0, 16)], S_PAIR)
        sent(wg.at[0, pl.ds(0, 3)], S_W)
        sent(wg.at[0], S_WPAIR)
        sent(low_stage, S_APAIR)
        sent(summand, S_XSUM)
        for g in range(CHUNKS):
            sent(low.at[pl.ds(0, 7), 0], S_A + g)
        for g in range(CHUNKS):
            for k in range(2):
                own = (mine == 1) & (xh == g // 2) & (z == 2 * xl + k)

                @pl.when(jnp.logical_not(own))
                def _(g=g, k=k):
                    sent(summand.at[0, 0], S_OUT + 2 * g + k)


def local(q_latent, kv_latent, kv_gain, w_q_b, w_kv_b, w_o, prompt_len, response_mask):
    frequency = 10000.0 ** (-np.arange(ROPE // 2, dtype=np.float64) * 2.0 / ROPE)
    fine = np.arange(HALF, dtype=np.float64)[:, None] * np.tile(frequency, 2)[None, :]
    table = np.stack([np.cos(fine), np.sin(fine), np.cos(HALF * fine), np.sin(HALF * fine)])
    hbm = pl.BlockSpec(memory_space=pltpu.HBM)
    bf16 = jnp.bfloat16
    result = pl.pallas_call(
        body,
        out_shape=jax.ShapeDtypeStruct((2, 4, ROWS, 1792), bf16),
        in_specs=[hbm] * 5 + [pl.BlockSpec(memory_space=pltpu.SMEM)] + [hbm] * 3,
        out_specs=hbm,
        scratch_shapes=[
            pltpu.SemaphoreType.DMA((NSENT,)),
            pltpu.SemaphoreType.DMA((NSEM,)),
            pltpu.SemaphoreType.DMA((17,)),
            pltpu.VMEM((WIDE, 128), bf16),
            pltpu.VMEM((1, KVR), jnp.float32),
            pltpu.VMEM((4, HALF, ROPE), jnp.float32),
            pltpu.VMEM((32, 128), jnp.int32),
            pltpu.VMEM((2, 2, HALF // 2, 1536), bf16),
            pltpu.VMEM((8, 1536, 384), bf16),
            pltpu.VMEM((512, 4096), bf16),
            pltpu.VMEM((32, 2, HALF, WIDE), bf16),
            pltpu.VMEM((2, HEADS, HALF, WIDE), bf16),
            pltpu.VMEM((HEADS, HALF, KVR), bf16),
            pltpu.VMEM((2, 2, 2 * ROWS, PER * VD), bf16),
            pltpu.VMEM((2, 2, ROWS, HEADS * VD), bf16),
            pltpu.VMEM((8, 2, 2, 2 * ROWS, PER * VD), bf16),
            pltpu.VMEM((8, 2, 2, ROWS, HEADS * VD), bf16),
            pltpu.VMEM((2, 4, 224, 2048), bf16),
            pltpu.VMEM((CHUNKS, 8, ROWS, 4 * 224), jnp.float32),
            pltpu.VMEM((CHUNKS, 2, 2, 2, ROWS, 4 * 224), bf16),
            pltpu.VMEM((CHUNKS, 2, 2, ROWS, 4 * 224), bf16),
            pltpu.VMEM((4096 // BLOCK, BLOCK), jnp.float32),
            pltpu.VMEM((HEADS * HALF, 128), jnp.float32),
            pltpu.VMEM((HEADS * HALF, 128), jnp.float32),
            pltpu.VMEM((HEADS * HALF, KVR), jnp.float32),
        ],
        compiler_params=pltpu.CompilerParams(
            collective_id=0, has_side_effects=True, vmem_limit_bytes=67000000
        ),
        cost_estimate=pl.CostEstimate(
            flops=20_000_000_000, bytes_accessed=16_000_000, transcendentals=0
        ),
        name="layer",
    )(
        q_latent.reshape(2, 2, HALF // 2, 1536),
        kv_latent.T,
        kv_gain.reshape(1, -1),
        jnp.asarray(table, jnp.float32),
        response_mask.reshape(32, 128),
        prompt_len,
        w_q_b,
        w_kv_b,
        w_o.T,
    )
    return jnp.where(prompt_len[0] > 0, result.reshape(128, 1792), 0)


def solution(mesh):
    finer = Mesh(mesh.devices.reshape(2, 4, 4, 2, 2), AXES)
    placed = (
        P(DP, None),
        P(DP, None),
        P(),
        P(None, HEAD),
        P(None, HEAD),
        P(HEAD, DP),
        P(),
        P(),
    )
    return jax.shard_map(
        local, mesh=finer, in_specs=placed, out_specs=P(DP, HEAD), check_vma=False
    )
```
